8 devices in a mesh: data: 2 (over z, y), dap: 4 (over x, core).
Axes of the slice: x: 2, y: 2, z: 1, core: 2. Of those that a mesh axis runs over, the one named last changes fastest.
Arguments:
- pair_z: float32 [24, 256, 256, 64], P('data', 'dap'), parts along dimension 0
- pair_mask: int32 [24, 256, 256], P('data', 'dap'), parts along dimension 0
- out_norm_gain: float32 [64], replicated
- out_norm_bias: float32 [64], replicated
- out_w_a: bfloat16 [64, 64], replicated
- out_w_agate: bfloat16 [64, 64], replicated
- out_w_b: bfloat16 [64, 64], replicated
- out_w_bgate: bfloat16 [64, 64], replicated
- out_w_gate: bfloat16 [64, 64], replicated
- out_x_gain: float32 [64], replicated
- out_x_bias: float32 [64], replicated
- out_w_proj: bfloat16 [64, 64], replicated
- in_norm_gain: float32 [64], replicated
- in_norm_bias: float32 [64], replicated
- in_w_a: bfloat16 [64, 64], replicated
- in_w_agate: bfloat16 [64, 64], replicated
- in_w_b: bfloat16 [64, 64], replicated
- in_w_bgate: bfloat16 [64, 64], replicated
- in_w_gate: bfloat16 [64, 64], replicated
- in_x_gain: float32 [64], replicated
- in_x_bias: float32 [64], replicated
- in_w_proj: bfloat16 [64, 64], replicated
- att_norm_gain: float32 [64], replicated
- att_norm_bias: float32 [64], replicated
- att_w_q: bfloat16 [64, 64], replicated
- att_w_k: bfloat16 [64, 64], replicated
- att_w_v: bfloat16 [64, 64], replicated
- att_w_bias: bfloat16 [64, 4], replicated
- att_w_gate: bfloat16 [64, 64], replicated
- att_w_proj: bfloat16 [64, 64], replicated
Outputs:
- output: float32 [24, 256, 256, 64], P('data', 'dap'), parts along dimension 0
There are 2 independent parts. The reference program is written for one: setup_inputs(seed, part) draws one part's arguments, and reference() takes and returns one part's arrays. A program takes and returns all parts, laid end to end along the dimension named above; an argument that names none is the same for every part.
All inputs are finite; a program needn't handle non-finite values.
Results may differ from the reference program's by a relative error of at most 0.00913572.
Values are sent between devices in bfloat16 or wider.
A program may use at most 1 GiB of HBM per device.

```python
import jax
import jax.numpy as jnp
from jax import lax

BATCH = 12
N = 256
C_Z = 64
C = 64
HEADS = 4
HEAD = 16

LN_EPS = 1e-5
MASK_FILL = -1e9
WEIGHT_NAMES = (
    'out_norm_gain', 'out_norm_bias', 'out_w_a', 'out_w_agate', 'out_w_b', 'out_w_bgate',
    'out_w_gate', 'out_x_gain', 'out_x_bias', 'out_w_proj',
    'in_norm_gain', 'in_norm_bias', 'in_w_a', 'in_w_agate', 'in_w_b', 'in_w_bgate',
    'in_w_gate', 'in_x_gain', 'in_x_bias', 'in_w_proj',
    'att_norm_gain', 'att_norm_bias', 'att_w_q', 'att_w_k', 'att_w_v', 'att_w_bias',
    'att_w_gate', 'att_w_proj',
)


def layer_norm(values, norm_gain, norm_shift):
    ch_mean = jnp.mean(values, axis=-1, keepdims=True)
    ch_var = jnp.mean(jnp.square(values - ch_mean), axis=-1, keepdims=True)
    return (values - ch_mean) * lax.rsqrt(ch_var + LN_EPS) * norm_gain + norm_shift


def draw_mask(mask_key):
    lengths = jax.random.randint(mask_key, (BATCH,), N - N // 8, N - N // 16 + 1)
    valid_rows = (jnp.arange(N)[None, :] < lengths[:, None]).astype(jnp.int32)
    return valid_rows[:, :, None] * valid_rows[:, None, :]


def gaussian(rand_key, arr_shape, w_scale):
    return w_scale * jax.random.normal(rand_key, arr_shape, jnp.float32)


def draw_update(upd_key):
    sub_keys = jax.random.split(upd_key, 10)
    scale_z = C_Z ** -0.5
    return [
        1.0 + gaussian(sub_keys[0], (C_Z,), 0.3),
        gaussian(sub_keys[1], (C_Z,), 0.3),
        gaussian(sub_keys[2], (C_Z, C), scale_z).astype(jnp.bfloat16),
        gaussian(sub_keys[3], (C_Z, C), scale_z).astype(jnp.bfloat16),
        gaussian(sub_keys[4], (C_Z, C), scale_z).astype(jnp.bfloat16),
        gaussian(sub_keys[5], (C_Z, C), scale_z).astype(jnp.bfloat16),
        gaussian(sub_keys[6], (C_Z, C_Z), scale_z).astype(jnp.bfloat16),
        1.0 + gaussian(sub_keys[7], (C,), 0.3),
        gaussian(sub_keys[8], (C,), 0.3),
        gaussian(sub_keys[9], (C, C_Z), C ** -0.5).astype(jnp.bfloat16),
    ]


def draw_attention(att_key):
    sub_keys = jax.random.split(att_key, 8)
    scale_z = C_Z ** -0.5
    att_width = HEADS * HEAD
    return [
        1.0 + gaussian(sub_keys[0], (C_Z,), 0.3),
        gaussian(sub_keys[1], (C_Z,), 0.3),
        gaussian(sub_keys[2], (C_Z, att_width), scale_z).astype(jnp.bfloat16),
        gaussian(sub_keys[3], (C_Z, att_width), scale_z).astype(jnp.bfloat16),
        gaussian(sub_keys[4], (C_Z, att_width), scale_z).astype(jnp.bfloat16),
        gaussian(sub_keys[5], (C_Z, HEADS), 1.5 * scale_z).astype(jnp.bfloat16),
        gaussian(sub_keys[6], (C_Z, att_width), scale_z).astype(jnp.bfloat16),
        gaussian(sub_keys[7], (att_width, C_Z), N ** 0.25 * att_width ** -0.5).astype(jnp.bfloat16),
    ]


def setup_inputs(seed: int = 0, part: int = 0) -> dict:
    base_key = jax.random.key(seed)
    pair_key, mask_key = jax.random.split(jax.random.fold_in(base_key, part))
    shared_keys = jax.random.split(jax.random.key(seed + 7919), 3)
    weights = draw_update(shared_keys[0]) + draw_update(shared_keys[1]) + draw_attention(shared_keys[2])
    inputs = {
        'pair_z': jax.random.normal(pair_key, (BATCH, N, N, C_Z), jnp.float32),
        'pair_mask': draw_mask(mask_key),
    }
    inputs.update(dict(zip(WEIGHT_NAMES, weights)))
    return inputs


def tri_update(pair_z, mask_flat, params, incoming):
    norm_gain, norm_bias, w_a, w_agate, w_b, w_bgate, w_gate, x_gain, x_bias, w_proj = params
    normed = layer_norm(pair_z, norm_gain, norm_bias).astype(jnp.bfloat16).reshape(N * N, C_Z)
    left_proj = (mask_flat * jax.nn.sigmoid(jnp.dot(normed, w_agate, preferred_element_type=jnp.float32))
                 * jnp.dot(normed, w_a, preferred_element_type=jnp.float32)).astype(jnp.bfloat16)
    right_proj = (mask_flat * jax.nn.sigmoid(jnp.dot(normed, w_bgate, preferred_element_type=jnp.float32))
                  * jnp.dot(normed, w_b, preferred_element_type=jnp.float32)).astype(jnp.bfloat16)
    gate_val = jax.nn.sigmoid(jnp.dot(normed, w_gate, preferred_element_type=jnp.float32))

    def chan_out(chan_pair):
        lhs_chan, rhs_chan = chan_pair
        return jnp.dot(lhs_chan.astype(jnp.float32), rhs_chan.astype(jnp.float32).T)

    def chan_in(chan_pair):
        lhs_chan, rhs_chan = chan_pair
        return jnp.dot(lhs_chan.astype(jnp.float32).T, rhs_chan.astype(jnp.float32))

    x_sum = lax.map(chan_in if incoming else chan_out,
                    (left_proj.T.reshape(C, N, N), right_proj.T.reshape(C, N, N)))
    x_norm = layer_norm(x_sum.reshape(C, N * N).T, x_gain, x_bias).astype(jnp.bfloat16)
    update = gate_val * jnp.dot(x_norm, w_proj, preferred_element_type=jnp.float32)
    return pair_z + update.reshape(N, N, C_Z)


def tri_attention(pair_z, pair_mask, params):
    norm_gain, norm_bias, w_q, w_k, w_v, w_bias, w_gate, w_proj = params
    normed = layer_norm(pair_z, norm_gain, norm_bias).astype(jnp.bfloat16).reshape(N * N, C_Z)
    q_heads = jnp.dot(normed, w_q, preferred_element_type=jnp.float32).astype(jnp.bfloat16).reshape(N, N, HEADS, HEAD)
    k_heads = jnp.dot(normed, w_k, preferred_element_type=jnp.float32).astype(jnp.bfloat16).reshape(N, N, HEADS, HEAD)
    v_heads = jnp.dot(normed, w_v, preferred_element_type=jnp.float32).astype(jnp.bfloat16).reshape(N, N, HEADS, HEAD)
    pair_bias = jnp.dot(normed, w_bias, preferred_element_type=jnp.float32).astype(jnp.bfloat16)
    pair_bias = pair_bias.astype(jnp.float32).reshape(N, N, HEADS).transpose(2, 0, 1)
    gate_val = jax.nn.sigmoid(jnp.dot(normed, w_gate, preferred_element_type=jnp.float32))

    def one_row(row_in):
        q_row, k_row, v_row, m_row = row_in
        logits = jnp.einsum('jhd,khd->hjk', q_row.astype(jnp.float32), k_row.astype(jnp.float32)) * HEAD ** -0.5 + pair_bias
        logits = jnp.where(m_row[None, None, :] > 0, logits, MASK_FILL)
        att_probs = jax.nn.softmax(logits, axis=-1).astype(jnp.bfloat16)
        return jnp.einsum('hjk,khd->jhd', att_probs.astype(jnp.float32), v_row.astype(jnp.float32))

    attended = lax.map(one_row, (q_heads, k_heads, v_heads, pair_mask)).reshape(N * N, HEADS * HEAD)
    gated_o = (attended * gate_val).astype(jnp.bfloat16)
    return pair_z + jnp.dot(gated_o, w_proj, preferred_element_type=jnp.float32).reshape(N, N, C_Z)


def reference(pair_z, pair_mask, out_norm_gain, out_norm_bias, out_w_a, out_w_agate, out_w_b, out_w_bgate,
              out_w_gate, out_x_gain, out_x_bias, out_w_proj, in_norm_gain, in_norm_bias, in_w_a, in_w_agate,
              in_w_b, in_w_bgate, in_w_gate, in_x_gain, in_x_bias, in_w_proj, att_norm_gain, att_norm_bias,
              att_w_q, att_w_k, att_w_v, att_w_bias, att_w_gate, att_w_proj):
    out_params = (out_norm_gain, out_norm_bias, out_w_a, out_w_agate, out_w_b, out_w_bgate,
                  out_w_gate, out_x_gain, out_x_bias, out_w_proj)
    in_params = (in_norm_gain, in_norm_bias, in_w_a, in_w_agate, in_w_b, in_w_bgate,
                 in_w_gate, in_x_gain, in_x_bias, in_w_proj)
    att_params = (att_norm_gain, att_norm_bias, att_w_q, att_w_k, att_w_v, att_w_bias, att_w_gate, att_w_proj)

    def one_sample(sample_in):
        sample_z, sample_mask = sample_in
        mask_flat = sample_mask.reshape(N * N, 1).astype(jnp.float32)
        z_one = tri_update(sample_z, mask_flat, out_params, False)
        z_two = tri_update(z_one, mask_flat, in_params, True)
        return tri_attention(z_two, sample_mask, att_params)

    return lax.map(one_sample, (pair_z, pair_mask))
```

```python
import jax
import jax.numpy as jnp
from jax import lax
from jax.experimental import pallas as pl
from jax.experimental.pallas import tpu as pltpu
from jax.sharding import PartitionSpec as P


LN_EPS = 1e-5
F32, BF16 = jnp.float32, jnp.bfloat16
ROWS, CH, COLS = 64, 64, 256
TILE = 16


def channel_norm(vals, gain, shift, axis_id):
    ch_mean = jnp.mean(vals, axis=axis_id, keepdims=True)
    ch_var = jnp.mean(jnp.square(vals - ch_mean), axis=axis_id, keepdims=True)
    return (vals - ch_mean) * lax.rsqrt(ch_var + LN_EPS) * gain + shift


def sigmoid(vals):
    return 1.0 / (1.0 + jnp.exp(-vals))


def mm(lhs, rhs):
    return jnp.dot(lhs, rhs, preferred_element_type=F32)


def ab_row(z_row, m_row, norm, w_ab, tile_a, tile_b, slot):
    normed = channel_norm(z_row, norm[0], norm[1], 0).astype(BF16)
    proj = mm(w_ab, normed)
    tile_a[slot] = (m_row * sigmoid(proj[CH:2 * CH]) * proj[:CH]).astype(BF16)
    tile_b[slot] = (m_row * sigmoid(proj[3 * CH:]) * proj[2 * CH:3 * CH]).astype(BF16)


def x_norm_tile(x_s, tile_x, base, xg, xb):
    parts = [(sub, half) for sub in range(2) for half in range(2)]

    def load(c, part):
        return x_s[c, pl.ds(pl.multiple_of(base + 8 * part[0], 8), 8), 128 * part[1]:128 * part[1] + 128]

    means = [sum(load(c, p) for c in range(CH)) * (1.0 / CH) for p in parts]
    scales = [lax.rsqrt(sum(jnp.square(load(c, p) - means[n]) for c in range(CH)) * (1.0 / CH) + LN_EPS)
              for n, p in enumerate(parts)]
    for c in range(CH):
        rows = []
        for sub in range(2):
            rows.append(jnp.concatenate(
                [(load(c, (sub, half)) - means[2 * sub + half]) * scales[2 * sub + half] * xg[c] + xb[c]
                 for half in range(2)], axis=1))
        tile_x[c] = jnp.concatenate(rows, axis=0).astype(BF16)


def gated_update(z_row, xn_row, norm, w_gate, w_proj):
    normed = channel_norm(z_row, norm[0], norm[1], 0).astype(BF16)
    return z_row + sigmoid(mm(w_gate, normed)) * mm(w_proj, xn_row)


def u_kernel(sc, zt, zr1, zr2, zr3, mask, norms, xgs, w_ab, w_sq, w_bias, z2_out, bias_out,
             z_s, a_s, b_s, x_s, tile_a, tile_b, tile_x, tile_c, tile_d, in_sem, out_sem):
    me, sample = sc[0], sc[1]
    srcs = (zt.at[sample], zr1, zr2, zr3)

    def z_copy(r):
        start = pl.multiple_of(64 * (me ^ r), 64)
        return pltpu.make_async_copy(srcs[r], z_s.at[pl.ds(start, 64)], in_sem.at[r])

    for r in range(4):
        z_copy(r).start()
    out_norm = (norms[0], norms[1])
    in_norm = (norms[2], norms[3])
    att_norm = (norms[4], norms[5])

    def flush(base):
        a_s[:, pl.ds(base, TILE), :] = jnp.swapaxes(tile_a[...], 0, 1)
        b_s[:, pl.ds(base, TILE), :] = jnp.swapaxes(tile_b[...], 0, 1)

    for r in range(4):
        z_copy(r).wait()

        @pl.loop(0, 4)
        def _(t):
            base = pl.multiple_of(64 * (me ^ r) + TILE * t, TILE)

            @pl.loop(0, TILE, unroll=4)
            def _(i):
                ab_row(z_s[base + i], mask[pl.ds(base + i, 1), :], out_norm, w_ab[0], tile_a, tile_b, i)
            flush(base)

    @pl.loop(0, CH, unroll=2)
    def _(c):
        x_s[c] = lax.dot_general(a_s[c], b_s[c], (((1,), (1,)), ((), ())), preferred_element_type=F32)

    @pl.loop(0, COLS // TILE)
    def _(t):
        base = pl.multiple_of(TILE * t, TILE)
        x_norm_tile(x_s, tile_x, base, xgs.at[0], xgs.at[1])
        tile_c[...] = jnp.swapaxes(tile_x[...], 0, 1)

        @pl.loop(0, TILE, unroll=4)
        def _(i):
            z_one = gated_update(z_s[base + i], tile_c[i], out_norm, w_sq[0], w_sq[1])
            z_s[base + i] = z_one
            ab_row(z_one, mask[pl.ds(base + i, 1), :], in_norm, w_ab[1], tile_a, tile_b, i)
        flush(base)

    @pl.loop(0, CH, unroll=2)
    def _(c):
        x_s[c] = lax.dot_general(a_s[c], b_s[c], (((0,), (0,)), ((), ())), preferred_element_type=F32)

    def z2_copy(t):
        base = pl.multiple_of(TILE * t, TILE)
        return pltpu.make_async_copy(z_s.at[pl.ds(base, TILE)], z2_out.at[pl.ds(base, TILE)], out_sem)

    @pl.loop(0, COLS // TILE)
    def _(t):
        base = pl.multiple_of(TILE * t, TILE)
        x_norm_tile(x_s, tile_x, base, xgs.at[2], xgs.at[3])
        tile_c[...] = jnp.swapaxes(tile_x[...], 0, 1)

        @pl.loop(0, TILE, unroll=4)
        def _(i):
            z_two = gated_update(z_s[base + i], tile_c[i], in_norm, w_sq[2], w_sq[3])
            z_s[base + i] = z_two
            normed = channel_norm(z_two, att_norm[0], att_norm[1], 0).astype(BF16)
            tile_d[i] = mm(w_bias[...], normed)
        bias_out[:, pl.ds(base, TILE), :] = jnp.swapaxes(tile_d[...], 0, 1)[:4].astype(BF16)
        z2_copy(t).start()

    @pl.loop(0, COLS // TILE)
    def _(t):
        z2_copy(t).wait()


def u_call(sc, zt, zr, mask, norms, xgs, w_ab, w_sq, w_bias):
    vm = pl.BlockSpec(memory_space=pltpu.VMEM)
    hb = pl.BlockSpec(memory_space=pl.ANY)
    return pl.pallas_call(
        u_kernel,
        out_shape=(jax.ShapeDtypeStruct((256, CH, COLS), F32), jax.ShapeDtypeStruct((4, 256, 256), BF16)),
        in_specs=[pl.BlockSpec(memory_space=pltpu.SMEM), hb, hb, hb, hb] + [vm] * 6,
        out_specs=(hb, vm),
        scratch_shapes=[
            pltpu.VMEM((256, CH, COLS), F32), pltpu.VMEM((CH, 256, COLS), BF16), pltpu.VMEM((CH, 256, COLS), BF16),
            pltpu.VMEM((CH, 256, COLS), F32), pltpu.VMEM((TILE, CH, COLS), BF16), pltpu.VMEM((TILE, CH, COLS), BF16),
            pltpu.VMEM((CH, TILE, COLS), BF16), pltpu.VMEM((TILE, CH, COLS), BF16), pltpu.VMEM((TILE, 8, COLS), F32),
            pltpu.SemaphoreType.DMA((4,)), pltpu.SemaphoreType.DMA,
        ],
        compiler_params=pltpu.CompilerParams(vmem_limit_bytes=62 << 20),
        name="pair_updates",
    )(sc, zt, *zr, mask, norms, xgs, w_ab, w_sq, w_bias)

HEADS, HEAD = 4, 16
MASK_FILL = -1e9
CHUNK = 32
SLOTS = 2


def a_kernel(z_in, mask, bias, norms, w_all, w_proj, z_out, bias_t, q_s, k_s, v_s, g_s, keep_s, s_buf, e_buf, top_s, inv_s, o_s):
    for h in range(HEADS):
        bias_t[h] = bias[h].astype(F32).T
    n_rows = z_in.shape[0]

    def project(row, slot):
        row = jnp.clip(row, 0, n_rows - 1)
        normed = channel_norm(z_in[row], norms[0], norms[1], 0).astype(BF16)
        proj = mm(w_all[...], normed)
        k_s[slot] = proj[CH:2 * CH].T.astype(BF16)
        q = proj[:CH].astype(BF16)
        for h in range(HEADS):
            q_s[slot, h, HEAD * h:HEAD * h + HEAD] = q[HEAD * h:HEAD * h + HEAD]
        v_s[slot] = proj[2 * CH:3 * CH].astype(BF16)
        g_s[slot] = sigmoid(proj[3 * CH:])
        keep_s[slot] = jnp.broadcast_to(mask[pl.ds(row, 1), :], (128, COLS)).T

    def fold(part, op):
        out = part[:8]
        for n in range(1, part.shape[0] // 8):
            out = op(out, part[8 * n:8 * n + 8])
        return out

    def scores(slot, h):
        return mm(k_s[slot], q_s[slot, h])

    def step(slot, h, logits):
        buf, prev = h % 2, (h + 1) % 2
        h2 = (h - 2) % HEADS
        slot2 = 1 - slot if h < 2 else slot
        top, total, probs = None, None, []
        for c in range(COLS // CHUNK):
            rows = slice(CHUNK * c, CHUNK * c + CHUNK)
            scale = (e_buf[buf, rows] * jnp.concatenate([inv_s[buf]] * (CHUNK // 8), axis=0)).astype(BF16)
            probs.append(scale)
            exps = jnp.exp(s_buf[prev, rows] - jnp.concatenate([top_s[prev]] * (CHUNK // 8), axis=0))
            e_buf[prev, rows] = exps
            part = fold(exps, jnp.add)
            total = part if total is None else total + part
            keep = keep_s[slot, rows]
            keep = jnp.concatenate([keep, keep], axis=1) > 0
            vals = jnp.where(keep, logits[rows] + bias_t[h, rows], MASK_FILL)
            s_buf[buf, rows] = vals
            part = fold(vals, jnp.maximum)
            top = part if top is None else jnp.maximum(top, part)
        top_s[buf] = jnp.broadcast_to(jnp.max(top, axis=0, keepdims=True), (8, COLS))
        inv_s[prev] = jnp.broadcast_to(1.0 / jnp.sum(total, axis=0, keepdims=True), (8, COLS))
        heads = slice(HEAD * h2, HEAD * h2 + HEAD)
        o_s[slot2, heads] = mm(v_s[slot2, heads], jnp.concatenate(probs, axis=0))

    def finish(row, slot):
        row = jnp.clip(row, 0, n_rows - 1)
        gated = (g_s[slot] * o_s[slot]).astype(BF16)
        z_out[row] = z_in[row] + mm(w_proj[...], gated)

    q_s[...] = jnp.zeros_like(q_s)

    @pl.loop(0, n_rows // 2 + 1)
    def _(pair):
        first = 2 * pair - 1
        lg = scores(1, 0)
        for slot in (1, 0):
            row = first + 1 - slot
            for h in range(HEADS):
                nxt = scores(slot, h + 1) if h < HEADS - 1 else (scores(0, 0) if slot else None)
                step(slot, h, lg)
                lg = nxt
                if h == 1:
                    finish(row - 1, 1 - slot)
                    project(row + 1, 1 - slot)


def a_call(z_in, mask, bias, norms, w_all, w_proj, n_rows=64):
    rows = z_in.shape[0]
    row_spec = pl.BlockSpec((n_rows, CH, COLS), lambda i: (i, 0, 0))
    full = lambda a: pl.BlockSpec(a.shape, lambda i: (0,) * a.ndim)
    return pl.pallas_call(
        a_kernel,
        grid=(rows // n_rows,),
        out_shape=jax.ShapeDtypeStruct((rows, CH, COLS), F32),
        in_specs=[row_spec, pl.BlockSpec((n_rows, COLS), lambda i: (i, 0)), full(bias), full(norms), full(w_all), full(w_proj)],
        out_specs=row_spec,
        scratch_shapes=[
            pltpu.VMEM((HEADS, COLS, COLS), F32), pltpu.VMEM((SLOTS, HEADS, CH, COLS), BF16), pltpu.VMEM((SLOTS, COLS, CH), BF16),
            pltpu.VMEM((SLOTS, CH, COLS), BF16), pltpu.VMEM((SLOTS, CH, COLS), F32), pltpu.VMEM((SLOTS, COLS, 128), F32),
            pltpu.VMEM((2, COLS, COLS), F32), pltpu.VMEM((2, COLS, COLS), F32), pltpu.VMEM((2, 8, COLS), F32),
            pltpu.VMEM((2, 8, COLS), F32), pltpu.VMEM((SLOTS, CH, COLS), F32),
        ],
        compiler_params=pltpu.CompilerParams(vmem_limit_bytes=48 << 20, dimension_semantics=("arbitrary",)),
        name="triangle_attention",
    )(z_in, mask, bias, norms, w_all, w_proj)


def exchange(values, r):
    return lax.ppermute(values, 'dap', [(i, i ^ r) for i in range(4)])


def update_weights(params):
    norm_gain, norm_bias, w_a, w_agate, w_b, w_bgate, w_gate, x_gain, x_bias, w_proj = params
    wide = lambda v: jnp.broadcast_to(v[:, None], (CH, COLS))
    deep = lambda v: jnp.broadcast_to(v[:, None, None], (CH, 8, 128))
    return ([wide(norm_gain), wide(norm_bias)], [deep(x_gain), deep(x_bias)],
            jnp.concatenate([w_a.T, w_agate.T, w_b.T, w_bgate.T], axis=0), [w_gate.T, w_proj.T])


def solution(mesh):
    def local_block(pair_z, pair_mask, *weights):
        out_n, out_x, out_ab, out_sq = update_weights(weights[:10])
        in_n, in_x, in_ab, in_sq = update_weights(weights[10:20])
        att_gain, att_shift, w_q, w_k, w_v, w_bias, w_gate, w_proj = weights[20:]
        att_n = [jnp.broadcast_to(v[:, None], (CH, COLS)) for v in (att_gain, att_shift)]
        norms = jnp.stack(out_n + in_n + att_n)
        xgs = jnp.stack(out_x + in_x)
        w_ab = jnp.stack([out_ab, in_ab])
        w_sq = jnp.stack(out_sq + in_sq)
        w_bias8 = jnp.concatenate([w_bias.T, jnp.zeros((4, CH), BF16)], axis=0)
        w_all = jnp.concatenate([w_q.T * jnp.bfloat16(HEAD ** -0.5), w_k.T, w_v.T, w_gate.T], axis=0)

        me = lax.axis_index('dap')
        zt = jnp.transpose(pair_z, (0, 1, 3, 2))
        n_own = zt.shape[0] // 4
        mask_bf = pair_mask.astype(BF16)
        mask_parts = jnp.stack([exchange(lax.dynamic_slice_in_dim(mask_bf, n_own * (me ^ r), n_own, axis=0), r) if r
                                else lax.dynamic_slice_in_dim(mask_bf, n_own * me, n_own, axis=0) for r in range(4)])
        mask_own = jnp.concatenate([lax.dynamic_index_in_dim(mask_parts, p ^ me, 0, keepdims=False) for p in range(4)],
                                   axis=1).astype(F32)
        arrived = [[exchange(lax.dynamic_index_in_dim(zt, n_own * (me ^ r) + t, 0, keepdims=False), r) for r in (1, 2, 3)]
                   for t in range(n_own)]
        out = jnp.zeros_like(zt)
        for t in range(n_own):
            sc = jnp.stack([me, n_own * me + t]).astype(jnp.int32)
            z_two, bias = u_call(sc, zt, arrived[t], mask_own[t], norms, xgs, w_ab, w_sq, w_bias8)
            z_three = a_call(z_two, mask_own[t], bias, norms[4:], w_all, w_proj.T)
            for r in range(4):
                part = lax.dynamic_slice_in_dim(z_three, ROWS * (me ^ r), ROWS, axis=0)
                if r:
                    part = exchange(part, r)
                out = lax.dynamic_update_index_in_dim(out, part, n_own * (me ^ r) + t, 0)
        return jnp.transpose(out, (0, 1, 3, 2))

    pair_spec = P('data', 'dap')
    return jax.shard_map(local_block, mesh=mesh, in_specs=(pair_spec, pair_spec) + (P(),) * 28,
                         out_specs=pair_spec, check_vma=False)
```

```python
import jax
import jax.numpy as jnp
from jax import lax
from jax.experimental import pallas as pl
from jax.experimental.pallas import tpu as pltpu
from jax.sharding import PartitionSpec as P


LN_EPS = 1e-5
F32, BF16 = jnp.float32, jnp.bfloat16
ROWS, CH, COLS = 64, 64, 256
TILE = 16


def channel_norm(vals, gain, shift, axis_id):
    ch_mean = jnp.mean(vals, axis=axis_id, keepdims=True)
    ch_var = jnp.mean(jnp.square(vals - ch_mean), axis=axis_id, keepdims=True)
    return (vals - ch_mean) * lax.rsqrt(ch_var + LN_EPS) * gain + shift


def sigmoid(vals):
    return 0.5 * jnp.tanh(0.5 * vals) + 0.5


def mm(lhs, rhs):
    return jnp.dot(lhs, rhs, preferred_element_type=F32)


def masked_norm(z_row, m_row, norm):
    return (m_row * channel_norm(z_row, norm[0], norm[1], 0)).astype(BF16)


def ab_row(proj, tile_a, tile_b, slot):
    tile_a[slot] = ((jnp.tanh(proj[CH:2 * CH]) + 1.0) * proj[:CH]).astype(BF16)
    tile_b[slot] = ((jnp.tanh(proj[3 * CH:]) + 1.0) * proj[2 * CH:3 * CH]).astype(BF16)


def x_norm_tile(x_s, tile_x, base, xg, xb):
    parts = [(sub, half) for sub in range(2) for half in range(2)]

    def load(c, part):
        return x_s[c, pl.ds(pl.multiple_of(base + 8 * part[0], 8), 8), 128 * part[1]:128 * part[1] + 128]

    means = [sum(load(c, p) for c in range(CH)) * (1.0 / CH) for p in parts]
    scales = [lax.rsqrt(sum(jnp.square(load(c, p) - means[n]) for c in range(CH)) * (1.0 / CH) + LN_EPS)
              for n, p in enumerate(parts)]
    for c in range(CH):
        rows = []
        for sub in range(2):
            rows.append(jnp.concatenate(
                [(load(c, (sub, half)) - means[2 * sub + half]) * scales[2 * sub + half] * xg[c] + xb[c]
                 for half in range(2)], axis=1))
        tile_x[c] = jnp.concatenate(rows, axis=0).astype(BF16)


LAG = 3


def staggered(count, *stages):
    held = [{} for _ in stages]
    for tick in range(count + LAG * (len(stages) - 1)):
        for k, stage in enumerate(stages):
            i = tick - LAG * k
            if 0 <= i < count:
                held[k][i] = stage(i, held[k - 1].pop(i) if k else None)


def u_kernel(sc, zt, zr1, zr2, zr3, mask0, mask1, mask2, mask3, norms, xgs, w_ab, w_sq, w_bias,
             z2_own, z2_par, bias_out, xo2, xo3, xi2, xi3,
             z_s, a_s, b_s, x_s, mask, tile_a, tile_b, tile_x, tile_c, tile_d, tile_z, in_sem, z_sem, x_sem):
    me, sample = sc[0], sc[1]
    srcs = (zt.at[sample], zr1, zr2, zr3)
    lanes = pl.ds(pl.multiple_of(128 * (me // 2), 128), 128)
    out_norm = (norms[0], norms[1])
    in_norm = (norms[2], norms[3])
    att_norm = (norms[4], norms[5])
    n_tiles = COLS // TILE

    def z_copy(r):
        start = pl.multiple_of(ROWS * (me ^ r), ROWS)
        return pltpu.make_async_copy(srcs[r], z_s.at[pl.ds(start, ROWS)], in_sem.at[r])

    for r in range(4):
        z_copy(r).start()
    for r, part in enumerate((mask0, mask1, mask2, mask3)):
        mask[pl.ds(pl.multiple_of(ROWS * (me ^ r), ROWS), ROWS), :] = part[...].astype(F32)

    def flush(base):
        a_s[:, pl.ds(base, TILE), :] = jnp.swapaxes(tile_a[...], 0, 1)
        b_s[:, pl.ds(base, TILE), :] = jnp.swapaxes(tile_b[...], 0, 1)

    def part_of(t):
        return (t * TILE // ROWS) ^ me, pl.ds(pl.multiple_of(t * TILE % ROWS, TILE), TILE)

    def export(t, start, own, par, far2, far3, sem):
        r, rows = part_of(t)
        act = (lambda cp: cp.start()) if start else (lambda cp: cp.wait())
        src = tile_c.at[t % 2] if far2.shape[-1] == COLS else tile_c.at[t % 2, :, :, lanes]
        for k, dst in ((0, own), (1, par), (2, far2), (3, far3)):
            if dst is not None:
                @pl.when(r == k)
                def _():
                    act(pltpu.make_async_copy(tile_z.at[t % 2] if k < 2 else src, dst.at[rows], sem.at[t % 2]))

    @pl.loop(0, n_tiles)
    def _(v):
        r = v * TILE // ROWS

        @pl.when(v * TILE % ROWS == 0)
        def _():
            pltpu.make_async_copy(zr1, z_s.at[pl.ds(0, ROWS)], in_sem.at[r]).wait()

        base = pl.multiple_of(ROWS * (me ^ r) + v * TILE % ROWS, TILE)
        staggered(
            TILE,
            lambda i, _: mm(w_ab[0], masked_norm(z_s[base + i], mask[pl.ds(base + i, 1), :], out_norm)),
            lambda i, proj: ab_row(proj, tile_a, tile_b, i))
        flush(base)

    @pl.loop(0, CH, unroll=4)
    def _(c):
        x_s[c] = lax.dot_general(a_s[c], b_s[c], (((1,), (1,)), ((), ())), preferred_element_type=F32)

    @pl.loop(0, n_tiles)
    def _(t):
        base = pl.multiple_of(TILE * t, TILE)

        @pl.when(t >= 2)
        def _():
            export(t - 2, False, None, None, xo2, xo3, x_sem)

        x_norm_tile(x_s, tile_x, base, xgs.at[0], xgs.at[1])
        tile_c[t % 2] = jnp.swapaxes(tile_x[...], 0, 1)

        def gate_and_update(i, _):
            normed = channel_norm(z_s[base + i], out_norm[0], out_norm[1], 0).astype(BF16)
            return mm(w_sq[0], normed), mm(w_sq[1], tile_c[t % 2, i])

        def next_norm(i, parts):
            z_one = z_s[base + i] + (jnp.tanh(parts[0]) + 1.0) * parts[1]
            tile_z[0, i] = z_one
            return masked_norm(z_one, mask[pl.ds(base + i, 1), :], in_norm)

        staggered(TILE, gate_and_update, next_norm, lambda i, normed: mm(w_ab[1], normed),
                  lambda i, proj: ab_row(proj, tile_a, tile_b, i))
        flush(base)
        z_s[pl.ds(base, TILE)] = tile_z[0]
        export(t, True, None, None, xo2, xo3, x_sem)

    for t in (n_tiles - 2, n_tiles - 1):
        export(t, False, None, None, xo2, xo3, x_sem)

    @pl.loop(0, CH, unroll=4)
    def _(c):
        x_s[c] = lax.dot_general(a_s[c], b_s[c], (((0,), (0,)), ((), ())), preferred_element_type=F32)

    @pl.loop(0, n_tiles)
    def _(t):
        base = pl.multiple_of(TILE * t, TILE)

        @pl.when(t >= 2)
        def _():
            export(t - 2, False, z2_own, z2_par, xi2, xi3, z_sem)

        x_norm_tile(x_s, tile_x, base, xgs.at[2], xgs.at[3])
        tile_c[t % 2] = jnp.swapaxes(tile_x[...], 0, 1)

        def gate_and_update(i, _):
            normed = channel_norm(z_s[base + i], in_norm[0], in_norm[1], 0).astype(BF16)
            return mm(w_sq[2], normed), mm(w_sq[3], tile_c[t % 2, i])

        def next_norm(i, parts):
            z_two = z_s[base + i] + (jnp.tanh(parts[0]) + 1.0) * parts[1]
            tile_z[t % 2, i] = z_two
            return channel_norm(z_two, att_norm[0], att_norm[1], 0).astype(BF16)

        def bias_row(i, normed):
            tile_d[i] = mm(w_bias[...], normed)

        staggered(TILE, gate_and_update, next_norm, bias_row)
        rows = pl.ds(pl.multiple_of(t * TILE % ROWS, TILE), TILE)
        bias_out[t * TILE // ROWS, :, rows, :] = jnp.swapaxes(tile_d[...], 0, 1)[:4].astype(BF16)
        export(t, True, z2_own, z2_par, xi2, xi3, z_sem)

    for t in (n_tiles - 2, n_tiles - 1):
        export(t, False, z2_own, z2_par, xi2, xi3, z_sem)


LANES = 128
VM = pl.BlockSpec(memory_space=pltpu.VMEM)
HB = pl.BlockSpec(memory_space=pl.ANY)
SM = pl.BlockSpec(memory_space=pltpu.SMEM)
PARAMS = pltpu.CompilerParams(vmem_limit_bytes=40 << 20, dimension_semantics=("arbitrary",))
AB_TILE = pltpu.VMEM((TILE, CH, COLS), BF16)
DMA2 = pltpu.SemaphoreType.DMA((2,))
ROW_HALF = jax.ShapeDtypeStruct((ROWS, CH, LANES), BF16)
ROW_FULL = jax.ShapeDtypeStruct((ROWS, CH, COLS), BF16)
ROW_WIDE = jax.ShapeDtypeStruct((ROWS, CH, COLS), F32)
SAMPLE_BF = pltpu.VMEM((CH, COLS, COLS), BF16)


def u_call(sc, zt, zr, masks, norms, xgs, w_ab, w_sq, w_bias):
    return pl.pallas_call(
        u_kernel,
        out_shape=(ROW_WIDE, ROW_WIDE, jax.ShapeDtypeStruct((4, 4, ROWS, COLS), BF16), ROW_HALF, ROW_HALF, ROW_FULL, ROW_FULL),
        in_specs=[SM] + [HB] * 4 + [VM] * 9,
        out_specs=(HB, HB, VM, HB, HB, HB, HB),
        scratch_shapes=[
            pltpu.VMEM((COLS, CH, COLS), F32), SAMPLE_BF, SAMPLE_BF,
            pltpu.VMEM((CH, COLS, COLS), F32), pltpu.VMEM((COLS, COLS), F32), AB_TILE, AB_TILE, pltpu.VMEM((CH, TILE, COLS), BF16), pltpu.VMEM((2, TILE, CH, COLS), BF16),
            pltpu.VMEM((TILE, 8, COLS), F32), pltpu.VMEM((2, TILE, CH, COLS), F32),
            pltpu.SemaphoreType.DMA((4,)), DMA2, DMA2,
        ],
        compiler_params=pltpu.CompilerParams(vmem_limit_bytes=62 << 20),
        name="pair_updates",
    )(sc, zt, *zr, *masks, norms, xgs, w_ab, w_sq, w_bias)


def l1_kernel(ids, z_in, mask_in, norms, w_ab, a_out, b_out, mask, tile_a, tile_b):
    out_norm = (norms[0], norms[1])
    mask[...] = mask_in[0].astype(F32)

    @pl.loop(0, ROWS // TILE)
    def _(t):
        base = pl.multiple_of(TILE * t, TILE)
        staggered(
            TILE,
            lambda i, _: mm(w_ab[0], masked_norm(z_in[0, base + i], mask[pl.ds(base + i, 1), :], out_norm)),
            lambda i, proj: ab_row(proj, tile_a, tile_b, i))
        a_out[0, :, pl.ds(base, TILE), :] = jnp.swapaxes(tile_a[...], 0, 1)
        b_out[0, :, pl.ds(base, TILE), :] = jnp.swapaxes(tile_b[...], 0, 1)


def l1_call(ids, zt, mask, norms, w_ab):
    n = ids.shape[0]
    ab = jax.ShapeDtypeStruct((n, CH, ROWS, COLS), BF16)
    ab_spec = pl.BlockSpec((1, CH, ROWS, COLS), lambda i, ids: (i, 0, 0, 0))
    return pl.pallas_call(
        l1_kernel,
        out_shape=(ab, ab),
        grid_spec=pltpu.PrefetchScalarGridSpec(
            num_scalar_prefetch=1, grid=(n,),
            in_specs=[pl.BlockSpec((1, ROWS, CH, COLS), lambda i, ids: (ids[i], 0, 0, 0)),
                      pl.BlockSpec((1, ROWS, COLS), lambda i, ids: (ids[i], 0, 0)), VM, VM],
            out_specs=(ab_spec, ab_spec),
            scratch_shapes=[pltpu.VMEM((ROWS, COLS), F32), AB_TILE, AB_TILE]),
        compiler_params=PARAMS,
        name="near_projections",
    )(ids, zt, mask, norms, w_ab)


def l2_kernel(sc, a_in, b_own, b_par, xgs, x_out, x_s, tile_x):
    odd = sc[0] % 2 == 1

    @pl.loop(0, CH, unroll=2)
    def _(c):
        for n in range(2):
            own, par = b_own[n, c].astype(F32), b_par[1 - n, c].astype(F32)
            pair = jnp.concatenate([jnp.where(odd, par, own), jnp.where(odd, own, par)], axis=0).astype(BF16)
            x_s[c, :, LANES * n:LANES * n + LANES] = lax.dot_general(
                a_in[n, c], pair, (((1,), (1,)), ((), ())), preferred_element_type=F32)

    @pl.loop(0, ROWS // TILE)
    def _(t):
        base = pl.multiple_of(TILE * t, TILE)
        x_norm_tile(x_s, tile_x, base, xgs.at[0], xgs.at[1])
        both = jnp.swapaxes(tile_x[...], 0, 1)
        for n in range(2):
            x_out[n, pl.ds(base, TILE)] = both[:, :, LANES * n:LANES * n + LANES]


def l2_call(sc, a_all, b_own, b_par, xgs):
    n = a_all.shape[0]
    ab_spec = pl.BlockSpec((2, CH, ROWS, COLS), lambda i: (i, 0, 0, 0))
    return pl.pallas_call(
        l2_kernel,
        grid=(n // 2,),
        out_shape=jax.ShapeDtypeStruct((n, ROWS, CH, LANES), BF16),
        in_specs=[SM, ab_spec, ab_spec, ab_spec, VM],
        out_specs=pl.BlockSpec((2, ROWS, CH, LANES), lambda i: (i, 0, 0, 0)),
        scratch_shapes=[pltpu.VMEM((CH, ROWS, COLS), F32), pltpu.VMEM((CH, TILE, COLS), BF16)],
        compiler_params=PARAMS,
        name="near_product",
    )(sc, a_all, b_own, b_par, xgs)


def r_kernel(sc, z_in, x_near, x_far, xi, norms, w_sq, w_bias, z_out, bias_out, tile_d):
    first = sc[0] < 2
    out_norm = (norms[0], norms[1])
    in_norm = (norms[2], norms[3])
    att_norm = (norms[4], norms[5])

    def outgoing(i, _):
        near, far = x_near[0, i].astype(F32), x_far[i].astype(F32)
        xn = jnp.concatenate([jnp.where(first, near, far), jnp.where(first, far, near)], axis=1).astype(BF16)
        normed = channel_norm(z_in[0, i], out_norm[0], out_norm[1], 0).astype(BF16)
        return mm(w_sq[0], normed), mm(w_sq[1], xn)

    def norm_one(i, parts):
        z_one = z_in[0, i] + (jnp.tanh(parts[0]) + 1.0) * parts[1]
        z_out[i] = z_one
        return channel_norm(z_one, in_norm[0], in_norm[1], 0).astype(BF16)

    def incoming(i, normed):
        return mm(w_sq[2], normed), mm(w_sq[3], xi[i])

    def norm_two(i, parts):
        z_two = z_out[i] + (jnp.tanh(parts[0]) + 1.0) * parts[1]
        z_out[i] = z_two
        return channel_norm(z_two, att_norm[0], att_norm[1], 0).astype(BF16)

    def bias_row(i, normed):
        tile_d[i] = mm(w_bias[...], normed)

    staggered(TILE, outgoing, norm_one, incoming, norm_two, bias_row)
    bias_out[...] = jnp.swapaxes(tile_d[...], 0, 1)[:4].astype(BF16)


def r_call(sc, zt, x_near, x_far, xi, norms, w_sq, w_bias):
    return pl.pallas_call(
        r_kernel,
        out_shape=(ROW_WIDE, jax.ShapeDtypeStruct((4, ROWS, COLS), BF16)),
        grid_spec=pltpu.PrefetchScalarGridSpec(
            num_scalar_prefetch=1, grid=(ROWS // TILE,),
            in_specs=[pl.BlockSpec((1, TILE, CH, COLS), lambda i, sc: (sc[1], i, 0, 0)),
                      pl.BlockSpec((1, TILE, CH, 128), lambda i, sc: (sc[2], i, 0, 0)),
                      pl.BlockSpec((TILE, CH, 128), lambda i, sc: (i, 0, 0)),
                      pl.BlockSpec((TILE, CH, COLS), lambda i, sc: (i, 0, 0)), VM, VM, VM],
            out_specs=(pl.BlockSpec((TILE, CH, COLS), lambda i, sc: (i, 0, 0)),
                       pl.BlockSpec((4, TILE, COLS), lambda i, sc: (0, i, 0))),
            scratch_shapes=[pltpu.VMEM((TILE, 8, COLS), F32)]),
        compiler_params=PARAMS,
        name="row_updates",
    )(sc, zt, x_near, x_far, xi, norms, w_sq, w_bias)


HEADS, HEAD = 4, 16
MASK_FILL = -1e9
CHUNK = 32
SLOTS = 2


def a_kernel(sc, z_in, mask_in, bias, norms, w_all, w_proj, out_in, out_ref, mask, bias_rows, bias_t, q_s, k_s, v_s, g_s, vn_s, gn_s, keep_s, s_buf, e_buf, p_s, top_s, inv_s, o_s):
    z_out = out_ref.at[0]
    mask[...] = mask_in[0].astype(F32)
    for r in range(4):
        bias_rows[:, pl.ds(pl.multiple_of(ROWS * (sc[1] ^ r), ROWS), ROWS), :] = bias[r].astype(F32)
    for h in range(HEADS):
        bias_t[h] = bias_rows[h].T
    n_rows = z_in.shape[0]

    def project(row, slot):
        row = jnp.clip(row, 0, n_rows - 1)
        normed = channel_norm(z_in[row], norms[0], norms[1], 0).astype(BF16)
        proj = mm(w_all[...], normed)
        k_s[slot] = proj[CH:2 * CH].T.astype(BF16)
        q = proj[:CH].astype(BF16)
        for h in range(HEADS):
            q_s[slot, h, HEAD * h:HEAD * h + HEAD] = q[HEAD * h:HEAD * h + HEAD]
        vn_s[slot] = proj[2 * CH:3 * CH].astype(BF16)
        gn_s[slot] = sigmoid(proj[3 * CH:])

    def keep_mask(row, slot):
        row = jnp.clip(row, 0, n_rows - 1)
        keep_s[slot] = jnp.broadcast_to(mask[pl.ds(row, 1), :], (128, COLS)).T

    def fold(part, op):
        out = part[:8]
        for n in range(1, part.shape[0] // 8):
            out = op(out, part[8 * n:8 * n + 8])
        return out

    def scores(slot, h):
        return mm(k_s[slot], q_s[slot, h])

    def weigh(slot, h, probs):
        heads = slice(HEAD * h, HEAD * h + HEAD)
        o_s[slot, heads] = mm(v_s[slot, heads], probs)

    def step(slot, h, logits, defer=False):
        buf, prev = h % 2, (h + 1) % 2
        top, total, probs = None, None, []
        for c in range(COLS // CHUNK):
            rows = slice(CHUNK * c, CHUNK * c + CHUNK)
            scale = (e_buf[buf, rows] * jnp.concatenate([inv_s[buf]] * (CHUNK // 8), axis=0)).astype(BF16)
            probs.append(scale)
            exps = jnp.exp(s_buf[prev, rows] - jnp.concatenate([top_s[prev]] * (CHUNK // 8), axis=0))
            e_buf[prev, rows] = exps
            part = fold(exps, jnp.add)
            total = part if total is None else total + part
            keep = keep_s[slot, rows]
            keep = jnp.concatenate([keep, keep], axis=1) > 0
            vals = jnp.where(keep, logits[rows] + bias_t[h, rows], MASK_FILL)
            s_buf[buf, rows] = vals
            part = fold(vals, jnp.maximum)
            top = part if top is None else jnp.maximum(top, part)
        top_s[buf] = jnp.broadcast_to(jnp.max(top, axis=0, keepdims=True), (8, COLS))
        inv_s[prev] = jnp.broadcast_to(1.0 / jnp.sum(total, axis=0, keepdims=True), (8, COLS))
        if defer:
            p_s[...] = jnp.concatenate(probs, axis=0)
        else:
            weigh(1 - slot if h < 2 else slot, (h - 2) % HEADS, jnp.concatenate(probs, axis=0))

    def finish(row, slot):
        row = jnp.clip(row, 0, n_rows - 1)
        gated = (g_s[slot] * o_s[slot]).astype(BF16)
        z_out[row] = z_in[row] + mm(w_proj[...], gated)

    q_s[...] = jnp.zeros_like(q_s)
    project(0, 0)
    keep_mask(0, 0)

    @pl.loop(0, n_rows // 2 + 1)
    def _(pair):
        first = 2 * pair - 1
        lg = scores(1, 0)
        weigh(0, 1, p_s[...])
        for slot in (1, 0):
            row = first + 1 - slot
            for h in range(HEADS):
                nxt = scores(slot, h + 1) if h < HEADS - 1 else (scores(0, 0) if slot else None)
                if h == 2:
                    project(row + 2, slot)
                step(slot, h, lg, defer=slot == 0 and h == 3)
                lg = nxt
                if h == 2:
                    finish(row - 1, 1 - slot)
                    v_s[1 - slot] = vn_s[1 - slot]
                    g_s[1 - slot] = gn_s[1 - slot]
            keep_mask(row + 2, slot)


def a_call(sc, z_in, mask, bias, norms, w_all, w_proj, out):
    full = lambda a: pl.BlockSpec(a.shape, lambda i, sc: (0,) * a.ndim)
    fresh = out is None
    call = pl.pallas_call(
        a_first if fresh else a_kernel,
        out_shape=jax.ShapeDtypeStruct((mask.shape[0], ROWS, CH, COLS), F32),
        grid_spec=pltpu.PrefetchScalarGridSpec(
            num_scalar_prefetch=1, grid=(1,),
            in_specs=[full(z_in), pl.BlockSpec((1, ROWS, COLS), lambda i, sc: (sc[0], 0, 0)),
                      full(bias), full(norms), full(w_all), full(w_proj)] + ([] if fresh else [HB]),
            out_specs=pl.BlockSpec((1, ROWS, CH, COLS), lambda i, sc: (sc[0], 0, 0, 0)),
            scratch_shapes=[
                pltpu.VMEM((ROWS, COLS), F32), pltpu.VMEM((HEADS, COLS, COLS), F32), pltpu.VMEM((HEADS, COLS, COLS), F32),
                pltpu.VMEM((SLOTS, HEADS, CH, COLS), BF16), pltpu.VMEM((SLOTS, COLS, CH), BF16),
                pltpu.VMEM((SLOTS, CH, COLS), BF16), pltpu.VMEM((SLOTS, CH, COLS), F32), pltpu.VMEM((SLOTS, CH, COLS), BF16),
                pltpu.VMEM((SLOTS, CH, COLS), F32), pltpu.VMEM((SLOTS, COLS, 128), F32), pltpu.VMEM((2, COLS, COLS), F32),
                pltpu.VMEM((2, COLS, COLS), F32), pltpu.VMEM((COLS, COLS), BF16), pltpu.VMEM((2, 8, COLS), F32),
                pltpu.VMEM((2, 8, COLS), F32), pltpu.VMEM((SLOTS, CH, COLS), F32),
            ]),
        compiler_params=pltpu.CompilerParams(vmem_limit_bytes=48 << 20, dimension_semantics=("arbitrary",)),
        input_output_aliases={} if fresh else {7: 0},
        name="triangle_attention",
    )
    args = (sc, z_in, mask, bias, norms, w_all, w_proj)
    return call(*args) if fresh else call(*args, out)


def a_first(sc, z_in, mask_in, bias, norms, w_all, w_proj, out_ref, *scratch):
    a_kernel(sc, z_in, mask_in, bias, norms, w_all, w_proj, None, out_ref, *scratch)


def exchange(values, r):
    return lax.ppermute(values, 'dap', [(i, i ^ r) for i in range(4)])


def update_weights(params):
    norm_gain, norm_bias, w_a, w_agate, w_b, w_bgate, w_gate, x_gain, x_bias, w_proj = params
    half = jnp.bfloat16(0.5)
    wide = lambda v: jnp.broadcast_to(v[:, None], (CH, COLS))
    deep = lambda v: jnp.broadcast_to(v[:, None, None], (CH, 8, 128))
    return ([wide(norm_gain), wide(norm_bias)], [deep(x_gain), deep(x_bias)],
            half * jnp.concatenate([w_a.T, w_agate.T, w_b.T, w_bgate.T], axis=0), [half * w_gate.T, half * w_proj.T])


def solution(mesh):
    def local_block(pair_z, pair_mask, *weights):
        me = lax.axis_index('dap')
        zt = jnp.transpose(pair_z, (0, 1, 3, 2))
        n_own = zt.shape[0] // 4
        mask_bf = pair_mask.astype(BF16)
        masks = [lax.dynamic_slice_in_dim(mask_bf, n_own * (me ^ r), n_own, axis=0) for r in range(4)]
        arrived, zt_t = [], zt
        for t in range(n_own):
            sends = [lax.dynamic_index_in_dim(zt_t, n_own * (me ^ r) + t, 0, keepdims=False) for r in (2, 3, 1)]
            *sends, zt_t = lax.optimization_barrier((*sends, zt))
            if t == 0:
                weights, masks = lax.optimization_barrier((weights, masks, sends[0]))[:2]
            got = [exchange(v, r) for v, r in zip(sends, (2, 3, 1))]
            arrived.append((got[2], got[0], got[1]))
        masks = [exchange(m, r) if r else m for r, m in enumerate(masks)]

        out_n, out_x, out_ab, out_sq = update_weights(weights[:10])
        in_n, in_x, in_ab, in_sq = update_weights(weights[10:20])
        att_gain, att_shift, w_q, w_k, w_v, w_bias, w_gate, w_proj = weights[20:]
        att_n = [jnp.broadcast_to(v[:, None], (CH, COLS)) for v in (att_gain, att_shift)]
        norms = jnp.stack(out_n + in_n + att_n)
        xgs = jnp.stack(out_x + in_x)
        w_ab = jnp.stack([out_ab, in_ab])
        w_sq = jnp.stack(out_sq + in_sq)
        w_bias8 = jnp.concatenate([w_bias.T, jnp.zeros((4, CH), BF16)], axis=0)
        w_all = jnp.concatenate([w_q.T * jnp.bfloat16(HEAD ** -0.5), w_k.T, w_v.T, w_gate.T], axis=0)
        w_out = w_proj.T
        att_norms = norms[4:]

        token = [None]

        def ordered(call, sc, *args):
            sc = jnp.stack([jnp.asarray(v, jnp.int32) for v in sc])
            if token[0] is not None:
                sc = lax.optimization_barrier((sc, token[0]))[0]
            res = call(sc, *args)
            token[0] = jax.tree.leaves(res)[-1]
            return res

        far = [(t, r) for t in range(n_own) for r in (2, 3)]
        a_far, b_far = ordered(l1_call, [n_own * (me ^ r) + t for t, r in far], zt, pair_mask, norms, w_ab)
        b_par = exchange(b_far, 1)
        x_near = ordered(l2_call, [me], a_far, b_far, b_par, xgs)

        out = None
        held = []
        for t in range(n_own):
            z_own, z_par, bias, *far_x = ordered(u_call, [me, n_own * me + t], zt, arrived[t], [m[t] for m in masks],
                                                 norms, xgs, w_ab, w_sq, w_bias8)
            got = {}
            bias_blk = {2: lax.dynamic_index_in_dim(bias, me, 0, keepdims=False),
                        3: lax.dynamic_index_in_dim(bias, me ^ 1, 0, keepdims=False)}
            z_near, bias_near = exchange(z_par, 1), exchange(bias, 1)
            for r in (2, 3):
                got[r] = [exchange(v, r) for v in (bias_blk[r], far_x[r - 2], far_x[r])]
            held.append(got)
            out = ordered(a_call, [n_own * me + t, 0], z_own, pair_mask, bias, att_norms, w_all, w_out, out)
            out = ordered(a_call, [n_own * (me ^ 1) + t, 0], z_near, pair_mask, bias_near, att_norms, w_all, w_out, out)
        for t in range(n_own):
            mine, z_two = {}, {}
            for r in (2, 3):
                bias_far, x_far, xi = held[t][r]
                z_two[r], bias_own = ordered(r_call, [me, n_own * (me ^ r) + t, far.index((t, r))], zt, x_near, x_far, xi,
                                             norms, w_sq, w_bias8)
                mine[r] = (bias_own, bias_far)
            both = jnp.stack([*mine[3], *mine[2]])
            par = exchange(both, 1)
            for r in (2, 3):
                bias = jnp.stack([mine[r][0], par[2 * r - 4], mine[r][1], par[2 * r - 3]])
                out = ordered(a_call, [n_own * (me ^ r) + t, me], z_two[r], pair_mask, bias, att_norms, w_all, w_out, out)
        return jnp.transpose(out, (0, 1, 3, 2))

    pair_spec = P('data', 'dap')
    return jax.shard_map(local_block, mesh=mesh, in_specs=(pair_spec, pair_spec) + (P(),) * 28,
                         out_specs=pair_spec, check_vma=False)
```

```python
import functools

import jax
import jax.numpy as jnp
from jax import lax
from jax.experimental import pallas as pl
from jax.experimental.pallas import tpu as pltpu
from jax.sharding import PartitionSpec as P


LN_EPS = 1e-5
F32, BF16 = jnp.float32, jnp.bfloat16
ROWS, CH, COLS = 64, 64, 256
TILE = 16


def channel_stats(vals, axis_id):
    ch_mean = jnp.mean(vals, axis=axis_id, keepdims=True)
    ch_var = jnp.mean(jnp.square(vals - ch_mean), axis=axis_id, keepdims=True)
    return ch_mean, lax.rsqrt(ch_var + LN_EPS)


def channel_norm(vals, norm, stats=None):
    ch_mean, scale = channel_stats(vals, 0) if stats is None else stats
    return (vals - ch_mean) * scale * norm[0] + norm[1]


def sigmoid(vals):
    return 0.5 * jnp.tanh(0.5 * vals) + 0.5


def mm(lhs, rhs):
    return jnp.dot(lhs, rhs, preferred_element_type=F32)


def ab_row(proj, tile_a, tile_b, slot):
    tile_a[slot] = ((jnp.tanh(proj[CH:2 * CH]) + 1.0) * proj[:CH]).astype(BF16)
    tile_b[slot] = ((jnp.tanh(proj[3 * CH:]) + 1.0) * proj[2 * CH:3 * CH]).astype(BF16)


def x_norm_tile(x_s, tile_x, base, xg, xb):
    parts = [(sub, half) for sub in range(2) for half in range(2)]

    def load(c, part):
        return x_s[c, pl.ds(pl.multiple_of(base + 8 * part[0], 8), 8), 128 * part[1]:128 * part[1] + 128]

    means = [sum(load(c, p) for c in range(CH)) * (1.0 / CH) for p in parts]
    scales = [lax.rsqrt(sum(jnp.square(load(c, p) - means[n]) for c in range(CH)) * (1.0 / CH) + LN_EPS)
              for n, p in enumerate(parts)]
    for c in range(CH):
        rows = []
        for sub in range(2):
            rows.append(jnp.concatenate(
                [(load(c, (sub, half)) - means[2 * sub + half]) * scales[2 * sub + half] * xg[c] + xb[c]
                 for half in range(2)], axis=1))
        tile_x[c] = jnp.concatenate(rows, axis=0).astype(BF16)


LAG = 3


def staggered(count, *stages):
    held = [{} for _ in stages]
    for tick in range(count + LAG * (len(stages) - 1)):
        for k, stage in enumerate(stages):
            i = tick - LAG * k
            if 0 <= i < count:
                held[k][i] = stage(i, held[k - 1].pop(i) if k else None)


def u_kernel(sc, zt, zr1, zr2, zr3, mask0, mask1, mask2, mask3, norms, xgs, w_ab, w_sq, w_bias,
             z2_own, z2_par, bias_out, far2, far3,
             z_s, a_s, b_s, x_s, mask, stats, tile_a, tile_b, tile_x, tile_c, tile_d, tile_z, in_sem, z_sem, x_sem):
    me, sample = sc[0], sc[1]
    srcs = (zt.at[sample], zr1, zr2, zr3)
    lanes = pl.ds(pl.multiple_of(LANES * (me // 2), LANES), LANES)
    out_norm = (norms[0], norms[1])
    in_norm = (norms[2], norms[3])
    att_norm = (norms[4], norms[5])
    n_tiles = COLS // TILE

    def z_copy(r):
        start = pl.multiple_of(ROWS * (me ^ r), ROWS)
        return pltpu.make_async_copy(srcs[r], z_s.at[pl.ds(start, ROWS)], in_sem.at[r])

    for r in range(4):
        z_copy(r).start()
    for r, part in enumerate((mask0, mask1, mask2, mask3)):
        mask[pl.ds(pl.multiple_of(ROWS * (me ^ r), ROWS), ROWS), :] = part[...].astype(F32)

    def mask_row(base, i):
        return mask[pl.ds(base + i, 1), :]

    def measure(base, i, vals=None):
        found = channel_stats(z_s[base + i] if vals is None else vals, 0)
        for n in range(2):
            stats[n if vals is None else n + 2, pl.ds(base + i, 1), :] = found[n]
        return found

    def recall(base, i, first):
        return [stats[first + n, pl.ds(base + i, 1), :] for n in range(2)]

    def flush(base):
        a_s[:, pl.ds(base, TILE), :] = jnp.swapaxes(tile_a[...], 0, 1)
        b_s[:, pl.ds(base, TILE), :] = jnp.swapaxes(tile_b[...], 0, 1)

    def export(t, start, outgoing, sem):
        r = (t * TILE // ROWS) ^ me
        q = t % (ROWS // TILE)
        rows = pl.ds(pl.multiple_of(TILE * q, TILE), TILE)
        half = pl.ds(pl.multiple_of(ROWS + TILE * (q % 2), TILE), TILE)
        side = pl.ds(pl.multiple_of(LANES * (q // 2), LANES), LANES)
        act = (lambda cp: cp.start()) if start else (lambda cp: cp.wait())
        for k, dst in ((0, z2_own), (1, z2_par), (2, far2), (3, far3)):
            if k > 1 or not outgoing:
                @pl.when(r == k)
                def _():
                    if k < 2:
                        src, to = tile_z.at[t % 2], dst.at[rows]
                    elif outgoing:
                        src, to = tile_c.at[t % 2, :, :, lanes], dst.at[half, :, side]
                    else:
                        src, to = tile_c.at[t % 2], dst.at[rows]
                    act(pltpu.make_async_copy(src, to, sem.at[t % 2]))

    @pl.loop(0, n_tiles)
    def _(v):
        r = v * TILE // ROWS

        @pl.when(v * TILE % ROWS == 0)
        def _():
            pltpu.make_async_copy(zr1, z_s.at[pl.ds(0, ROWS)], in_sem.at[r]).wait()

        base = pl.multiple_of(ROWS * (me ^ r) + v * TILE % ROWS, TILE)
        staggered(
            TILE,
            lambda i, _: mm(w_ab[0], (mask_row(base, i) * channel_norm(z_s[base + i], out_norm, measure(base, i))).astype(BF16)),
            lambda i, proj: ab_row(proj, tile_a, tile_b, i))
        flush(base)

    @pl.loop(0, CH, unroll=4)
    def _(c):
        x_s[c] = lax.dot_general(a_s[c], b_s[c], (((1,), (1,)), ((), ())), preferred_element_type=F32)

    @pl.loop(0, n_tiles)
    def _(t):
        base = pl.multiple_of(TILE * t, TILE)

        @pl.when(t >= 2)
        def _():
            export(t - 2, False, True, x_sem)

        x_norm_tile(x_s, tile_x, base, xgs.at[0], xgs.at[1])
        tile_c[t % 2] = jnp.swapaxes(tile_x[...], 0, 1)

        def gate_and_update(i, _):
            normed = channel_norm(z_s[base + i], out_norm, recall(base, i, 0)).astype(BF16)
            return mm(w_sq[0], normed), mm(w_sq[1], tile_c[t % 2, i])

        def next_norm(i, parts):
            z_one = z_s[base + i] + (jnp.tanh(parts[0]) + 1.0) * parts[1]
            tile_z[0, i] = z_one
            return (mask_row(base, i) * channel_norm(z_one, in_norm, measure(base, i, z_one))).astype(BF16)

        staggered(TILE, gate_and_update, next_norm, lambda i, normed: mm(w_ab[1], normed),
                  lambda i, proj: ab_row(proj, tile_a, tile_b, i))
        flush(base)
        z_s[pl.ds(base, TILE)] = tile_z[0]
        export(t, True, True, x_sem)

    for t in (n_tiles - 2, n_tiles - 1):
        export(t, False, True, x_sem)

    @pl.loop(0, CH, unroll=4)
    def _(c):
        x_s[c] = lax.dot_general(a_s[c], b_s[c], (((0,), (0,)), ((), ())), preferred_element_type=F32)

    @pl.loop(0, n_tiles)
    def _(t):
        base = pl.multiple_of(TILE * t, TILE)

        @pl.when(t >= 2)
        def _():
            export(t - 2, False, False, z_sem)

        x_norm_tile(x_s, tile_x, base, xgs.at[2], xgs.at[3])
        tile_c[t % 2] = jnp.swapaxes(tile_x[...], 0, 1)

        def gate_and_update(i, _):
            normed = channel_norm(z_s[base + i], in_norm, recall(base, i, 2)).astype(BF16)
            return mm(w_sq[2], normed), mm(w_sq[3], tile_c[t % 2, i])

        def next_norm(i, parts):
            z_two = z_s[base + i] + (jnp.tanh(parts[0]) + 1.0) * parts[1]
            tile_z[t % 2, i] = z_two
            return channel_norm(z_two, att_norm).astype(BF16)

        def bias_row(i, normed):
            tile_d[i] = mm(w_bias[...], normed)

        staggered(TILE, gate_and_update, next_norm, bias_row)
        rows = pl.ds(pl.multiple_of(t * TILE % ROWS, TILE), TILE)
        bias_out[t * TILE // ROWS, :, rows, :] = jnp.swapaxes(tile_d[...], 0, 1)[:4].astype(BF16)
        export(t, True, False, z_sem)

    def bias_copy(n):
        return pltpu.make_async_copy(bias_out.at[me ^ n], (far2, far3)[n].at[pl.ds(FAR_BIAS, 4)], x_sem.at[n])

    for n in range(2):
        bias_copy(n).start()
    for t in (n_tiles - 2, n_tiles - 1):
        export(t, False, False, z_sem)
    for n in range(2):
        bias_copy(n).wait()


LANES = 128
VM = pl.BlockSpec(memory_space=pltpu.VMEM)
HB = pl.BlockSpec(memory_space=pl.ANY)
SM = pl.BlockSpec(memory_space=pltpu.SMEM)
PARAMS = pltpu.CompilerParams(vmem_limit_bytes=40 << 20, dimension_semantics=("arbitrary",))
AB_TILE = pltpu.VMEM((TILE, CH, COLS), BF16)
DMA2 = pltpu.SemaphoreType.DMA((2,))
FAR_BIAS = ROWS + ROWS // 2
FAR = jax.ShapeDtypeStruct((FAR_BIAS + 4, CH, COLS), BF16)
ROW_WIDE = jax.ShapeDtypeStruct((ROWS, CH, COLS), F32)
SAMPLE_BF = pltpu.VMEM((CH, COLS, COLS), BF16)


def u_call(sc, zt, zr, masks, norms, xgs, w_ab, w_sq, w_bias):
    return pl.pallas_call(
        u_kernel,
        out_shape=(ROW_WIDE, ROW_WIDE, jax.ShapeDtypeStruct((4, 4, ROWS, COLS), BF16), FAR, FAR),
        in_specs=[SM] + [HB] * 4 + [VM] * 9,
        out_specs=(HB, HB, VM, HB, HB),
        scratch_shapes=[
            pltpu.VMEM((COLS, CH, COLS), F32), SAMPLE_BF, SAMPLE_BF,
            pltpu.VMEM((CH, COLS, COLS), F32), pltpu.VMEM((COLS, COLS), F32), pltpu.VMEM((4, COLS, COLS), F32), AB_TILE, AB_TILE, pltpu.VMEM((CH, TILE, COLS), BF16), pltpu.VMEM((2, TILE, CH, COLS), BF16),
            pltpu.VMEM((TILE, 8, COLS), F32), pltpu.VMEM((2, TILE, CH, COLS), F32),
            pltpu.SemaphoreType.DMA((4,)), DMA2, DMA2,
        ],
        compiler_params=pltpu.CompilerParams(vmem_limit_bytes=62 << 20),
        name="pair_updates",
    )(sc, zt, *zr, *masks, norms, xgs, w_ab, w_sq, w_bias)


def l1_kernel(ids, z_in, mask_in, norms, w_ab, a_out, b_out, mask, tile_a, tile_b):
    out_norm = (norms[0], norms[1])
    mask[...] = mask_in[0].astype(F32)

    @pl.loop(0, ROWS // TILE)
    def _(t):
        base = pl.multiple_of(TILE * t, TILE)
        staggered(
            TILE,
            lambda i, _: mm(w_ab[0], (mask[pl.ds(base + i, 1), :] * channel_norm(z_in[0, base + i], out_norm)).astype(BF16)),
            lambda i, proj: ab_row(proj, tile_a, tile_b, i))
        a_out[0, :, pl.ds(base, TILE), :] = jnp.swapaxes(tile_a[...], 0, 1)
        b_out[0, :, pl.ds(base, TILE), :] = jnp.swapaxes(tile_b[...], 0, 1)


def l1_call(ids, zt, mask, norms, w_ab):
    n = ids.shape[0]
    ab = jax.ShapeDtypeStruct((n, CH, ROWS, COLS), BF16)
    ab_spec = pl.BlockSpec((1, CH, ROWS, COLS), lambda i, ids: (i, 0, 0, 0))
    return pl.pallas_call(
        l1_kernel,
        out_shape=(ab, ab),
        grid_spec=pltpu.PrefetchScalarGridSpec(
            num_scalar_prefetch=1, grid=(n,),
            in_specs=[pl.BlockSpec((1, ROWS, CH, COLS), lambda i, ids: (ids[i], 0, 0, 0)),
                      pl.BlockSpec((1, ROWS, COLS), lambda i, ids: (ids[i], 0, 0)), VM, VM],
            out_specs=(ab_spec, ab_spec),
            scratch_shapes=[pltpu.VMEM((ROWS, COLS), F32), AB_TILE, AB_TILE]),
        compiler_params=PARAMS,
        name="near_projections",
    )(ids, zt, mask, norms, w_ab)


def l2_kernel(sc, a_in, b_own, b_par, xgs, x_out, x_s, tile_x):
    odd = sc[0] % 2 == 1

    @pl.loop(0, CH, unroll=2)
    def _(c):
        for n in range(2):
            own, par = b_own[n, c].astype(F32), b_par[1 - n, c].astype(F32)
            pair = jnp.concatenate([jnp.where(odd, par, own), jnp.where(odd, own, par)], axis=0).astype(BF16)
            x_s[c, :, LANES * n:LANES * n + LANES] = lax.dot_general(
                a_in[n, c], pair, (((1,), (1,)), ((), ())), preferred_element_type=F32)

    @pl.loop(0, ROWS // TILE)
    def _(t):
        base = pl.multiple_of(TILE * t, TILE)
        x_norm_tile(x_s, tile_x, base, xgs.at[0], xgs.at[1])
        both = jnp.swapaxes(tile_x[...], 0, 1)
        for n in range(2):
            x_out[n, pl.ds(base, TILE)] = both[:, :, LANES * n:LANES * n + LANES]


def l2_call(sc, a_all, b_own, b_par, xgs):
    n = a_all.shape[0]
    ab_spec = pl.BlockSpec((2, CH, ROWS, COLS), lambda i: (i, 0, 0, 0))
    return pl.pallas_call(
        l2_kernel,
        grid=(n // 2,),
        out_shape=jax.ShapeDtypeStruct((n, ROWS, CH, LANES), BF16),
        in_specs=[SM, ab_spec, ab_spec, ab_spec, VM],
        out_specs=pl.BlockSpec((2, ROWS, CH, LANES), lambda i: (i, 0, 0, 0)),
        scratch_shapes=[pltpu.VMEM((CH, ROWS, COLS), F32), pltpu.VMEM((CH, TILE, COLS), BF16)],
        compiler_params=PARAMS,
        name="near_product",
    )(sc, a_all, b_own, b_par, xgs)


def r_kernel(sc, z_in, x_near, x_far, xi, norms, w_sq, w_bias, z_out, bias_out, tile_d):
    first = sc[0] < 2
    out_norm = (norms[0], norms[1])
    in_norm = (norms[2], norms[3])
    att_norm = (norms[4], norms[5])

    def outgoing(i, _):
        near, far = x_near[0, i].astype(F32), x_far[i].astype(F32)
        xn = jnp.concatenate([jnp.where(first, near, far), jnp.where(first, far, near)], axis=1).astype(BF16)
        normed = channel_norm(z_in[0, i], out_norm).astype(BF16)
        return mm(w_sq[0], normed), mm(w_sq[1], xn)

    def norm_one(i, parts):
        z_one = z_in[0, i] + (jnp.tanh(parts[0]) + 1.0) * parts[1]
        z_out[i] = z_one
        return channel_norm(z_one, in_norm).astype(BF16)

    def incoming(i, normed):
        return mm(w_sq[2], normed), mm(w_sq[3], xi[i])

    def norm_two(i, parts):
        z_two = z_out[i] + (jnp.tanh(parts[0]) + 1.0) * parts[1]
        z_out[i] = z_two
        return channel_norm(z_two, att_norm).astype(BF16)

    def bias_row(i, normed):
        tile_d[i] = mm(w_bias[...], normed)

    staggered(TILE, outgoing, norm_one, incoming, norm_two, bias_row)
    bias_out[...] = jnp.swapaxes(tile_d[...], 0, 1)[:4].astype(BF16)


def r_call(sc, zt, x_near, far, norms, w_sq, w_bias):
    return pl.pallas_call(
        r_kernel,
        out_shape=(ROW_WIDE, jax.ShapeDtypeStruct((4, ROWS, COLS), BF16)),
        grid_spec=pltpu.PrefetchScalarGridSpec(
            num_scalar_prefetch=1, grid=(ROWS // TILE,),
            in_specs=[pl.BlockSpec((1, TILE, CH, COLS), lambda i, sc: (sc[1], i, 0, 0)),
                      pl.BlockSpec((1, TILE, CH, LANES), lambda i, sc: (sc[2], i, 0, 0)),
                      pl.BlockSpec((TILE, CH, LANES), lambda i, sc: (ROWS // TILE + i % 2, 0, i // 2)),
                      pl.BlockSpec((TILE, CH, COLS), lambda i, sc: (i, 0, 0)), VM, VM, VM],
            out_specs=(pl.BlockSpec((TILE, CH, COLS), lambda i, sc: (i, 0, 0)),
                       pl.BlockSpec((4, TILE, COLS), lambda i, sc: (0, i, 0))),
            scratch_shapes=[pltpu.VMEM((TILE, 8, COLS), F32)]),
        compiler_params=PARAMS,
        name="row_updates",
    )(sc, zt, x_near, far, far, norms, w_sq, w_bias)


HEADS, HEAD = 4, 16
MASK_FILL = -1e9
CHUNK = 32
SLOTS = 2
STEPS = 6


def attention_kernel(n, fresh, sc, *refs):
    z_refs, bias_refs = refs[:n], refs[n:2 * n]
    mask_in, norms, w_all, w_proj = refs[2 * n:2 * n + 4]
    rest = refs[2 * n + (4 if fresh else 5):]
    (out, z_in, z_out, mask_i, mask, bias_rows, bias_t, q_s, k_s, v_s, g_s, vn_s, gn_s, keep_s, s_buf, e_buf, p_s,
     top_s, inv_s, o_s, m_sem, z_sem, o_sem) = rest
    n_rows = n * ROWS

    def z_copy(j):
        return pltpu.make_async_copy(z_refs[j], z_in.at[pl.ds(ROWS * j, ROWS)], z_sem.at[j])

    def m_copy(j):
        return pltpu.make_async_copy(mask_in.at[sc[j]], mask_i.at[pl.ds(ROWS * j, ROWS)], m_sem.at[j])

    def o_copy(j):
        return pltpu.make_async_copy(z_out.at[pl.ds(ROWS * j, ROWS)], out.at[sc[j]], o_sem.at[j])

    for j in range(n):
        m_copy(j).start()
        z_copy(j).start()
    for j in range(n):
        for r in range(4):
            bias_rows[j, :, pl.ds(pl.multiple_of(ROWS * (sc[n + j] ^ r), ROWS), ROWS), :] = bias_refs[j][r].astype(F32)
    for j in range(n):
        m_copy(j).wait()
    z_copy(0).wait()
    mask[...] = mask_i[...].astype(F32)
    q_s[...] = jnp.zeros_like(q_s)

    @pl.loop(0, n * HEADS)
    def _(h):
        bias_t[h // HEADS, h % HEADS] = bias_rows[h // HEADS, h % HEADS].T

    def project(row, slot):
        row = jnp.minimum(row, n_rows - 1)
        normed = channel_norm(z_in[row], (norms[0], norms[1])).astype(BF16)
        proj = mm(w_all[...], normed)
        k_s[slot] = proj[CH:2 * CH].T.astype(BF16)
        q = proj[:CH].astype(BF16)
        for h in range(HEADS):
            q_s[slot, h, HEAD * h:HEAD * h + HEAD] = q[HEAD * h:HEAD * h + HEAD]
        vn_s[slot] = proj[2 * CH:3 * CH].astype(BF16)
        gn_s[slot] = sigmoid(proj[3 * CH:])

    def keep_mask(row, slot):
        row = jnp.minimum(row, n_rows - 1)
        keep_s[slot] = jnp.broadcast_to(mask[pl.ds(row, 1), :], (LANES, COLS)).T

    def fold(part, op):
        out = part[:8]
        for n in range(1, part.shape[0] // 8):
            out = op(out, part[8 * n:8 * n + 8])
        return out

    def scores(slot, h):
        return mm(k_s[slot], q_s[slot, h])

    def weigh(slot, h, probs):
        heads = slice(HEAD * h, HEAD * h + HEAD)
        o_s[slot, heads] = mm(v_s[slot, heads], probs)

    def step(row, slot, h, logits, defer):
        buf, prev = h % 2, (h + 1) % 2
        sample = jnp.clip(row, 0, n_rows - 1) // ROWS
        top, total, probs = None, None, []
        for c in range(COLS // CHUNK):
            rows = slice(CHUNK * c, CHUNK * c + CHUNK)
            probs.append((e_buf[buf, rows] * jnp.concatenate([inv_s[buf]] * (CHUNK // 8), axis=0)).astype(BF16))
            exps = jnp.exp(s_buf[prev, rows] - jnp.concatenate([top_s[prev]] * (CHUNK // 8), axis=0))
            e_buf[prev, rows] = exps
            part = fold(exps, jnp.add)
            total = part if total is None else total + part
            keep = keep_s[slot, rows]
            keep = jnp.concatenate([keep, keep], axis=1) > 0
            vals = jnp.where(keep, logits[rows] + bias_t[sample, h, rows], MASK_FILL)
            s_buf[buf, rows] = vals
            part = fold(vals, jnp.maximum)
            top = part if top is None else jnp.maximum(top, part)
        top_s[buf] = jnp.broadcast_to(jnp.max(top, axis=0, keepdims=True), (8, COLS))
        inv_s[prev] = jnp.broadcast_to(1.0 / jnp.sum(total, axis=0, keepdims=True), (8, COLS))
        if defer:
            p_s[...] = jnp.concatenate(probs, axis=0)
        else:
            weigh(1 - slot if h < 2 else slot, (h - 2) % HEADS, jnp.concatenate(probs, axis=0))

    def finish(row, slot):
        gated = (g_s[slot] * o_s[slot]).astype(BF16)
        z_out[jnp.maximum(row, 0)] = z_in[jnp.clip(row, 0, n_rows - 1)] + mm(w_proj[...], gated)

    project(0, 0)
    keep_mask(0, 0)
    n_steps = (n_rows + 2 + STEPS - 1) // STEPS

    @pl.loop(0, n_steps)
    def _(it):
        first = STEPS * it - 1
        lg = scores(1, 0)
        weigh(0, 1, p_s[...])
        for k in range(STEPS):
            row, slot, last = first + k, 1 - k % 2, k == STEPS - 1
            for h in range(HEADS):
                nxt = scores(slot, h + 1) if h < HEADS - 1 else (None if last else scores(1 - slot, 0))
                if h == 2:
                    project(row + 2, slot)
                step(row, slot, h, lg, last and h == HEADS - 1)
                lg = nxt
                if h == 3:
                    finish(row - 1, 1 - slot)
                    v_s[1 - slot] = vn_s[1 - slot]
                    g_s[1 - slot] = gn_s[1 - slot]
            keep_mask(row + 2, slot)
        for j in range(1, n):
            @pl.when(it == (ROWS * j - 1) // STEPS - 1)
            def _():
                z_copy(j).wait()

            @pl.when(it == (ROWS * j + 1) // STEPS)
            def _():
                o_copy(j - 1).start()

    o_copy(n - 1).start()
    for j in range(n):
        o_copy(j).wait()


def attend(sc, z_parts, biases, mask, norms, w_all, w_proj, out):
    n, fresh = len(z_parts), out is None
    args = (sc, *z_parts, *biases, mask, norms, w_all, w_proj) + (() if fresh else (out,))
    rows = n * ROWS
    pair = pltpu.VMEM((SLOTS, CH, COLS), BF16)
    wide = pltpu.VMEM((SLOTS, CH, COLS), F32)
    square = pltpu.VMEM((SLOTS, COLS, COLS), F32)
    each = pltpu.VMEM((n, HEADS, COLS, COLS), F32)
    line = pltpu.VMEM((SLOTS, 8, COLS), F32)
    sems = pltpu.SemaphoreType.DMA((n,))
    return pl.pallas_call(
        functools.partial(attention_kernel, n, fresh),
        out_shape=jax.ShapeDtypeStruct((mask.shape[0], ROWS, CH, COLS), F32),
        in_specs=[SM] + [HB] * n + [VM] * n + [HB] + [VM] * 3 + ([] if fresh else [HB]),
        out_specs=HB,
        scratch_shapes=[
            pltpu.VMEM((rows, CH, COLS), F32), pltpu.VMEM((rows + STEPS, CH, COLS), F32), pltpu.VMEM((rows, COLS), jnp.int32),
            pltpu.VMEM((rows, COLS), F32), each, each, pltpu.VMEM((SLOTS, HEADS, CH, COLS), BF16),
            pltpu.VMEM((SLOTS, COLS, CH), BF16), pair, wide, pair, wide, pltpu.VMEM((SLOTS, COLS, LANES), F32),
            square, square, pltpu.VMEM((COLS, COLS), BF16), line, line, wide, sems, sems, sems,
        ],
        compiler_params=pltpu.CompilerParams(vmem_limit_bytes=48 << 20),
        input_output_aliases={} if fresh else {len(args) - 1: 0},
        name="triangle_attention",
    )(*args)


def exchange(values, r):
    return lax.ppermute(values, 'dap', [(i, i ^ r) for i in range(4)])


def update_weights(params):
    norm_gain, norm_bias, w_a, w_agate, w_b, w_bgate, w_gate, x_gain, x_bias, w_proj = params
    half = jnp.bfloat16(0.5)
    wide = lambda v: jnp.broadcast_to(v[:, None], (CH, COLS))
    deep = lambda v: jnp.broadcast_to(v[:, None, None], (CH, 8, 128))
    return ([wide(norm_gain), wide(norm_bias)], [deep(x_gain), deep(x_bias)],
            half * jnp.concatenate([w_a.T, w_agate.T, w_b.T, w_bgate.T], axis=0), [half * w_gate.T, half * w_proj.T])


def solution(mesh):
    def local_block(pair_z, pair_mask, *weights):
        me = lax.axis_index('dap')
        zt = jnp.transpose(pair_z, (0, 1, 3, 2))
        n_own = zt.shape[0] // 4
        mask_bf = pair_mask.astype(BF16)
        masks = [lax.dynamic_slice_in_dim(mask_bf, n_own * (me ^ r), n_own, axis=0) for r in range(4)]
        arrived, zt_t = [], zt
        for t in range(n_own):
            sends = [lax.dynamic_index_in_dim(zt_t, n_own * (me ^ r) + t, 0, keepdims=False) for r in (2, 3, 1)]
            *sends, zt_t = lax.optimization_barrier((*sends, zt))
            if t == 0:
                weights, masks = lax.optimization_barrier((weights, masks, sends[0]))[:2]
            got = [exchange(v, r) for v, r in zip(sends, (2, 3, 1))]
            arrived.append((got[2], got[0], got[1]))
        masks = [exchange(m, r) if r else m for r, m in enumerate(masks)]

        out_n, out_x, out_ab, out_sq = update_weights(weights[:10])
        in_n, in_x, in_ab, in_sq = update_weights(weights[10:20])
        att_gain, att_shift, w_q, w_k, w_v, w_bias, w_gate, w_proj = weights[20:]
        att_n = [jnp.broadcast_to(v[:, None], (CH, COLS)) for v in (att_gain, att_shift)]
        norms = jnp.stack(out_n + in_n + att_n)
        xgs = jnp.stack(out_x + in_x)
        w_ab = jnp.stack([out_ab, in_ab])
        w_sq = jnp.stack(out_sq + in_sq)
        w_bias8 = jnp.concatenate([w_bias.T, jnp.zeros((4, CH), BF16)], axis=0)
        w_all = jnp.concatenate([w_q.T * jnp.bfloat16(HEAD ** -0.5), w_k.T, w_v.T, w_gate.T], axis=0)
        w_out = w_proj.T
        att_norms = norms[4:]

        token = [None]

        def ordered(call, sc, *args):
            sc = jnp.stack([jnp.asarray(v, jnp.int32) for v in sc])
            if token[0] is not None:
                sc = lax.optimization_barrier((sc, token[0]))[0]
            res = call(sc, *args)
            token[0] = jax.tree.leaves(res)[-1]
            return res

        def attention(jobs, out):
            samples, orders, z_parts, biases = zip(*jobs)
            return ordered(attend, samples + orders, z_parts, biases, pair_mask, att_norms, w_all, w_out, out)

        far = [(t, r) for t in range(n_own) for r in (2, 3)]
        a_far, b_far = ordered(l1_call, [n_own * (me ^ r) + t for t, r in far], zt, pair_mask, norms, w_ab)
        b_par = exchange(b_far, 1)
        x_near = ordered(l2_call, [me], a_far, b_far, b_par, xgs)

        out = None
        held, waiting = [], []
        for t in range(n_own):
            z_own, z_par, bias, far2, far3 = ordered(u_call, [me, n_own * me + t], zt, arrived[t],
                                                     [m[t] for m in masks], norms, xgs, w_ab, w_sq, w_bias8)
            held.append({2: exchange(far2, 2), 3: exchange(far3, 3)})
            near = (n_own * (me ^ 1) + t, 0, exchange(z_par, 1), exchange(bias, 1))
            out = attention(waiting + [(n_own * me + t, 0, z_own, bias)], out)
            waiting = [near]
        for t in range(n_own):
            mine, z_two = {}, {}
            for r in (2, 3):
                z_two[r], bias_own = ordered(r_call, [me, n_own * (me ^ r) + t, far.index((t, r))], zt, x_near,
                                             held[t][r], norms, w_sq, w_bias8)
                mine[r] = (bias_own, held[t][r][FAR_BIAS:])
            par = exchange(jnp.stack([*mine[3], *mine[2]]), 1)
            out = attention(waiting + [
                (n_own * (me ^ r) + t, me, z_two[r], jnp.stack([mine[r][0], par[2 * r - 4], mine[r][1], par[2 * r - 3]]))
                for r in (2, 3)], out)
            waiting = []
        return jnp.transpose(out, (0, 1, 3, 2))

    pair_spec = P('data', 'dap')
    return jax.shard_map(local_block, mesh=mesh, in_specs=(pair_spec, pair_spec) + (P(),) * 28,
                         out_specs=pair_spec, check_vma=False)
```

```python
import functools

import jax
import jax.numpy as jnp
from jax import lax
from jax.experimental import pallas as pl
from jax.experimental.pallas import tpu as pltpu
from jax.sharding import PartitionSpec as P


LN_EPS = 1e-5
F32, BF16 = jnp.float32, jnp.bfloat16
ROWS, CH, COLS = 64, 64, 256
TILE = 16


def channel_stats(vals, axis_id):
    ch_mean = jnp.mean(vals, axis=axis_id, keepdims=True)
    ch_var = jnp.mean(jnp.square(vals - ch_mean), axis=axis_id, keepdims=True)
    return ch_mean, lax.rsqrt(ch_var + LN_EPS)


def channel_norm(vals, norm, stats=None):
    ch_mean, scale = channel_stats(vals, 0) if stats is None else stats
    return (vals - ch_mean) * scale * norm[0] + norm[1]


def sigmoid(vals):
    return 0.5 * jnp.tanh(0.5 * vals) + 0.5


def mm(lhs, rhs):
    return jnp.dot(lhs, rhs, preferred_element_type=F32)


def ab_row(proj, tile_a, tile_b, slot):
    tile_a[slot] = ((jnp.tanh(proj[CH:2 * CH]) + 1.0) * proj[:CH]).astype(BF16)
    tile_b[slot] = ((jnp.tanh(proj[3 * CH:]) + 1.0) * proj[2 * CH:3 * CH]).astype(BF16)


def x_norm_tile(x_s, tile_x, base, xg, xb):
    parts = [(sub, half) for sub in range(2) for half in range(2)]

    def load(c, part):
        return x_s[c, pl.ds(pl.multiple_of(base + 8 * part[0], 8), 8), 128 * part[1]:128 * part[1] + 128]

    means = [sum(load(c, p) for c in range(CH)) * (1.0 / CH) for p in parts]
    scales = [lax.rsqrt(sum(jnp.square(load(c, p) - means[n]) for c in range(CH)) * (1.0 / CH) + LN_EPS)
              for n, p in enumerate(parts)]
    for c in range(CH):
        rows = []
        for sub in range(2):
            rows.append(jnp.concatenate(
                [(load(c, (sub, half)) - means[2 * sub + half]) * scales[2 * sub + half] * xg[c] + xb[c]
                 for half in range(2)], axis=1))
        tile_x[c] = jnp.concatenate(rows, axis=0).astype(BF16)


LAG = 3


def staggered(count, *stages):
    held = [{} for _ in stages]
    for tick in range(count + LAG * (len(stages) - 1)):
        for k, stage in enumerate(stages):
            i = tick - LAG * k
            if 0 <= i < count:
                held[k][i] = stage(i, held[k - 1].pop(i) if k else None)


def u_kernel(last, sc, zt, zr1, zr2, zr3, mask0, mask1, mask2, mask3, norms, xgs, w_ab, w_sq, w_bias,
             z2_own, z2_par, bias_out, far2, far3,
             z_s, a_s, b_s, x_s, mask, stats, tile_a, tile_b, tile_x, tile_c, tile_d, tile_z, in_sem, z_sem, x_sem):
    me, sample = sc[0], sc[1]
    srcs = (zt.at[sample], zr1, zr2, zr3)
    lanes = pl.ds(pl.multiple_of(LANES * (me // 2), LANES), LANES)
    out_norm = (norms[0], norms[1])
    in_norm = (norms[2], norms[3])
    att_norm = (norms[4], norms[5])
    n_tiles = COLS // TILE

    def z_copy(r):
        start = pl.multiple_of(ROWS * (me ^ r), ROWS)
        return pltpu.make_async_copy(srcs[r], z_s.at[pl.ds(start, ROWS)], in_sem.at[r])

    for r in range(4):
        z_copy(r).start()
    for r, part in enumerate((mask0, mask1, mask2, mask3)):
        mask[pl.ds(pl.multiple_of(ROWS * (me ^ r), ROWS), ROWS), :] = part[...].astype(F32)

    def mask_row(base, i):
        return mask[pl.ds(base + i, 1), :]

    def measure(base, i, vals=None):
        found = channel_stats(z_s[base + i] if vals is None else vals, 0)
        for n in range(2):
            stats[n if vals is None else n + 2, pl.ds(base + i, 1), :] = found[n]
        return found

    def recall(base, i, first):
        return [stats[first + n, pl.ds(base + i, 1), :] for n in range(2)]

    def flush(base):
        a_s[:, pl.ds(base, TILE), :] = jnp.swapaxes(tile_a[...], 0, 1)
        b_s[:, pl.ds(base, TILE), :] = jnp.swapaxes(tile_b[...], 0, 1)

    def export(t, start, outgoing, sem):
        r = (t * TILE // ROWS) ^ me
        q = t % (ROWS // TILE)
        rows = pl.ds(pl.multiple_of(TILE * q, TILE), TILE)
        half = pl.ds(pl.multiple_of(ROWS + TILE * (q % 2), TILE), TILE)
        side = pl.ds(pl.multiple_of(LANES * (q // 2), LANES), LANES)
        act = (lambda cp: cp.start()) if start else (lambda cp: cp.wait())
        for k, dst in ((0, z2_own), (1, z2_par), (2, far2), (3, far3)):
            plain = k < 2 or (last and k == 3)
            if not (outgoing and plain):
                @pl.when(r == k)
                def _():
                    if plain:
                        src, to = tile_z.at[t % 2], dst.at[rows]
                    elif outgoing:
                        src, to = tile_c.at[t % 2, :, :, lanes], dst.at[half, :, side]
                    else:
                        src, to = tile_c.at[t % 2], dst.at[rows]
                    act(pltpu.make_async_copy(src, to, sem.at[t % 2]))

    @pl.loop(0, n_tiles)
    def _(v):
        r = v * TILE // ROWS

        @pl.when(v * TILE % ROWS == 0)
        def _():
            pltpu.make_async_copy(zr1, z_s.at[pl.ds(0, ROWS)], in_sem.at[r]).wait()

        base = pl.multiple_of(ROWS * (me ^ r) + v * TILE % ROWS, TILE)
        staggered(
            TILE,
            lambda i, _: mm(w_ab[0], (mask_row(base, i) * channel_norm(z_s[base + i], out_norm, measure(base, i))).astype(BF16)),
            lambda i, proj: ab_row(proj, tile_a, tile_b, i))
        flush(base)

    @pl.loop(0, CH, unroll=4)
    def _(c):
        x_s[c] = lax.dot_general(a_s[c], b_s[c], (((1,), (1,)), ((), ())), preferred_element_type=F32)

    @pl.loop(0, n_tiles)
    def _(t):
        base = pl.multiple_of(TILE * t, TILE)

        @pl.when(t >= 2)
        def _():
            export(t - 2, False, True, x_sem)

        x_norm_tile(x_s, tile_x, base, xgs.at[0], xgs.at[1])
        tile_c[t % 2] = jnp.swapaxes(tile_x[...], 0, 1)

        def gate_and_update(i, _):
            normed = channel_norm(z_s[base + i], out_norm, recall(base, i, 0)).astype(BF16)
            return mm(w_sq[0], normed), mm(w_sq[1], tile_c[t % 2, i])

        def next_norm(i, parts):
            z_one = z_s[base + i] + (jnp.tanh(parts[0]) + 1.0) * parts[1]
            tile_z[0, i] = z_one
            return (mask_row(base, i) * channel_norm(z_one, in_norm, measure(base, i, z_one))).astype(BF16)

        staggered(TILE, gate_and_update, next_norm, lambda i, normed: mm(w_ab[1], normed),
                  lambda i, proj: ab_row(proj, tile_a, tile_b, i))
        flush(base)
        z_s[pl.ds(base, TILE)] = tile_z[0]
        export(t, True, True, x_sem)

    for t in (n_tiles - 2, n_tiles - 1):
        export(t, False, True, x_sem)

    @pl.loop(0, CH, unroll=4)
    def _(c):
        x_s[c] = lax.dot_general(a_s[c], b_s[c], (((0,), (0,)), ((), ())), preferred_element_type=F32)

    @pl.loop(0, n_tiles)
    def _(t):
        base = pl.multiple_of(TILE * t, TILE)

        @pl.when(t >= 2)
        def _():
            export(t - 2, False, False, z_sem)

        x_norm_tile(x_s, tile_x, base, xgs.at[2], xgs.at[3])
        tile_c[t % 2] = jnp.swapaxes(tile_x[...], 0, 1)

        def gate_and_update(i, _):
            normed = channel_norm(z_s[base + i], in_norm, recall(base, i, 2)).astype(BF16)
            return mm(w_sq[2], normed), mm(w_sq[3], tile_c[t % 2, i])

        def next_norm(i, parts):
            z_two = z_s[base + i] + (jnp.tanh(parts[0]) + 1.0) * parts[1]
            tile_z[t % 2, i] = z_two
            return channel_norm(z_two, att_norm).astype(BF16)

        def bias_row(i, normed):
            tile_d[i] = mm(w_bias[...], normed)

        staggered(TILE, gate_and_update, next_norm, bias_row)
        rows = pl.ds(pl.multiple_of(t * TILE % ROWS, TILE), TILE)
        bias_out[t * TILE // ROWS, :, rows, :] = jnp.swapaxes(tile_d[...], 0, 1)[:4].astype(BF16)
        export(t, True, False, z_sem)

    bias_to = ((far2, 0, 0), (far2, 1, 1), (far2, 3, 2)) if last else ((far2, 0, 0), (far3, 1, 0))

    def bias_copy(n):
        dst, block, place = bias_to[n]
        return pltpu.make_async_copy(bias_out.at[me ^ block], dst.at[pl.ds(FAR_BIAS + 4 * place, 4)], in_sem.at[n])

    for n in range(len(bias_to)):
        bias_copy(n).start()
    for t in (n_tiles - 2, n_tiles - 1):
        export(t, False, False, z_sem)
    for n in range(len(bias_to)):
        bias_copy(n).wait()


LANES = 128
VM = pl.BlockSpec(memory_space=pltpu.VMEM)
HB = pl.BlockSpec(memory_space=pl.ANY)
SM = pl.BlockSpec(memory_space=pltpu.SMEM)
PARAMS = pltpu.CompilerParams(vmem_limit_bytes=40 << 20, dimension_semantics=("arbitrary",))
AB_TILE = pltpu.VMEM((TILE, CH, COLS), BF16)
DMA2 = pltpu.SemaphoreType.DMA((2,))
FAR_BIAS = ROWS + ROWS // 2
FAR = jax.ShapeDtypeStruct((FAR_BIAS + 4, CH, COLS), BF16)
FAR_LAST = jax.ShapeDtypeStruct((FAR_BIAS + 12, CH, COLS), BF16)
ROW_WIDE = jax.ShapeDtypeStruct((ROWS, CH, COLS), F32)
SAMPLE_BF = pltpu.VMEM((CH, COLS, COLS), BF16)


def u_call(last, sc, zt, zr, masks, norms, xgs, w_ab, w_sq, w_bias):
    return pl.pallas_call(
        functools.partial(u_kernel, last),
        out_shape=(ROW_WIDE, ROW_WIDE, jax.ShapeDtypeStruct((4, 4, ROWS, COLS), BF16), *((FAR_LAST, ROW_WIDE) if last else (FAR, FAR))),
        in_specs=[SM] + [HB] * 4 + [VM] * 9,
        out_specs=(HB, HB, VM, HB, HB),
        scratch_shapes=[
            pltpu.VMEM((COLS, CH, COLS), F32), SAMPLE_BF, SAMPLE_BF,
            pltpu.VMEM((CH, COLS, COLS), F32), pltpu.VMEM((COLS, COLS), F32), pltpu.VMEM((4, COLS, COLS), F32), AB_TILE, AB_TILE, pltpu.VMEM((CH, TILE, COLS), BF16), pltpu.VMEM((2, TILE, CH, COLS), BF16),
            pltpu.VMEM((TILE, 8, COLS), F32), pltpu.VMEM((2, TILE, CH, COLS), F32),
            pltpu.SemaphoreType.DMA((4,)), DMA2, DMA2,
        ],
        compiler_params=pltpu.CompilerParams(vmem_limit_bytes=62 << 20),
        name="pair_updates",
    )(sc, zt, *zr, *masks, norms, xgs, w_ab, w_sq, w_bias)


def l1_kernel(ids, z_in, mask_in, norms, w_ab, a_out, b_out, mask, tile_a, tile_b):
    out_norm = (norms[0], norms[1])
    mask[...] = mask_in[0].astype(F32)

    @pl.loop(0, ROWS // TILE)
    def _(t):
        base = pl.multiple_of(TILE * t, TILE)
        staggered(
            TILE,
            lambda i, _: mm(w_ab[0], (mask[pl.ds(base + i, 1), :] * channel_norm(z_in[0, base + i], out_norm)).astype(BF16)),
            lambda i, proj: ab_row(proj, tile_a, tile_b, i))
        a_out[0, :, pl.ds(base, TILE), :] = jnp.swapaxes(tile_a[...], 0, 1)
        b_out[0, :, pl.ds(base, TILE), :] = jnp.swapaxes(tile_b[...], 0, 1)


def l1_call(ids, zt, mask, norms, w_ab):
    n = ids.shape[0]
    ab = jax.ShapeDtypeStruct((n, CH, ROWS, COLS), BF16)
    ab_spec = pl.BlockSpec((1, CH, ROWS, COLS), lambda i, ids: (i, 0, 0, 0))
    return pl.pallas_call(
        l1_kernel,
        out_shape=(ab, ab),
        grid_spec=pltpu.PrefetchScalarGridSpec(
            num_scalar_prefetch=1, grid=(n,),
            in_specs=[pl.BlockSpec((1, ROWS, CH, COLS), lambda i, ids: (ids[i], 0, 0, 0)),
                      pl.BlockSpec((1, ROWS, COLS), lambda i, ids: (ids[i], 0, 0)), VM, VM],
            out_specs=(ab_spec, ab_spec),
            scratch_shapes=[pltpu.VMEM((ROWS, COLS), F32), AB_TILE, AB_TILE]),
        compiler_params=PARAMS,
        name="near_projections",
    )(ids, zt, mask, norms, w_ab)


def l2_kernel(sc, a_in, b_own, b_par, xgs, x_out, x_s, tile_x):
    odd = sc[0] % 2 == 1

    @pl.loop(0, CH, unroll=2)
    def _(c):
        for n in range(2):
            own, par = b_own[n, c].astype(F32), b_par[1 - n, c].astype(F32)
            pair = jnp.concatenate([jnp.where(odd, par, own), jnp.where(odd, own, par)], axis=0).astype(BF16)
            x_s[c, :, LANES * n:LANES * n + LANES] = lax.dot_general(
                a_in[n, c], pair, (((1,), (1,)), ((), ())), preferred_element_type=F32)

    @pl.loop(0, ROWS // TILE)
    def _(t):
        base = pl.multiple_of(TILE * t, TILE)
        x_norm_tile(x_s, tile_x, base, xgs.at[0], xgs.at[1])
        both = jnp.swapaxes(tile_x[...], 0, 1)
        for n in range(2):
            x_out[n, pl.ds(base, TILE)] = both[:, :, LANES * n:LANES * n + LANES]


def l2_call(sc, a_all, b_own, b_par, xgs):
    n = a_all.shape[0]
    ab_spec = pl.BlockSpec((2, CH, ROWS, COLS), lambda i: (i, 0, 0, 0))
    return pl.pallas_call(
        l2_kernel,
        grid=(n // 2,),
        out_shape=jax.ShapeDtypeStruct((n, ROWS, CH, LANES), BF16),
        in_specs=[SM, ab_spec, ab_spec, ab_spec, VM],
        out_specs=pl.BlockSpec((2, ROWS, CH, LANES), lambda i: (i, 0, 0, 0)),
        scratch_shapes=[pltpu.VMEM((CH, ROWS, COLS), F32), pltpu.VMEM((CH, TILE, COLS), BF16)],
        compiler_params=PARAMS,
        name="near_product",
    )(sc, a_all, b_own, b_par, xgs)


def r_kernel(sc, z_in, x_near, x_far, xi, norms, w_sq, w_bias, z_out, bias_out, tile_d):
    first = sc[0] < 2
    out_norm = (norms[0], norms[1])
    in_norm = (norms[2], norms[3])
    att_norm = (norms[4], norms[5])

    def outgoing(i, _):
        near, far = x_near[0, i].astype(F32), x_far[i].astype(F32)
        xn = jnp.concatenate([jnp.where(first, near, far), jnp.where(first, far, near)], axis=1).astype(BF16)
        normed = channel_norm(z_in[0, i], out_norm).astype(BF16)
        return mm(w_sq[0], normed), mm(w_sq[1], xn)

    def norm_one(i, parts):
        z_one = z_in[0, i] + (jnp.tanh(parts[0]) + 1.0) * parts[1]
        z_out[i] = z_one
        return channel_norm(z_one, in_norm).astype(BF16)

    def incoming(i, normed):
        return mm(w_sq[2], normed), mm(w_sq[3], xi[i])

    def norm_two(i, parts):
        z_two = z_out[i] + (jnp.tanh(parts[0]) + 1.0) * parts[1]
        z_out[i] = z_two
        return channel_norm(z_two, att_norm).astype(BF16)

    def bias_row(i, normed):
        tile_d[i] = mm(w_bias[...], normed)

    staggered(TILE, outgoing, norm_one, incoming, norm_two, bias_row)
    bias_out[...] = jnp.swapaxes(tile_d[...], 0, 1)[:4].astype(BF16)


def r_call(sc, zt, x_near, far, norms, w_sq, w_bias):
    return pl.pallas_call(
        r_kernel,
        out_shape=(ROW_WIDE, jax.ShapeDtypeStruct((4, ROWS, COLS), BF16)),
        grid_spec=pltpu.PrefetchScalarGridSpec(
            num_scalar_prefetch=1, grid=(ROWS // TILE,),
            in_specs=[pl.BlockSpec((1, TILE, CH, COLS), lambda i, sc: (sc[1], i, 0, 0)),
                      pl.BlockSpec((1, TILE, CH, LANES), lambda i, sc: (sc[2], i, 0, 0)),
                      pl.BlockSpec((TILE, CH, LANES), lambda i, sc: (ROWS // TILE + i % 2, 0, i // 2)),
                      pl.BlockSpec((TILE, CH, COLS), lambda i, sc: (i, 0, 0)), VM, VM, VM],
            out_specs=(pl.BlockSpec((TILE, CH, COLS), lambda i, sc: (i, 0, 0)),
                       pl.BlockSpec((4, TILE, COLS), lambda i, sc: (0, i, 0))),
            scratch_shapes=[pltpu.VMEM((TILE, 8, COLS), F32)]),
        compiler_params=PARAMS,
        name="row_updates",
    )(sc, zt, x_near, far, far, norms, w_sq, w_bias)


HEADS, HEAD = 4, 16
MASK_FILL = -1e9
CHUNK = 32
SLOTS = 2
STEPS = 6


def attention_kernel(n, fresh, away, sc, *refs):
    z_refs, bias_refs = refs[:n], refs[n:2 * n]
    mask_in, norms, w_all, w_proj = refs[2 * n:2 * n + 4]
    rest = refs[2 * n + 4 + away + (not fresh):]
    mask_away, out_away = refs[2 * n + 4], rest[1]
    (out, z_in, z_out, mask_i, mask, bias_rows, bias_t, q_s, k_s, v_s, g_s, vn_s, gn_s, keep_s, s_buf, e_buf, p_s,
     top_s, inv_s, o_s, m_sem, z_sem, o_sem) = rest[:1] + rest[1 + away:]
    n_rows = n * ROWS

    def z_copy(j):
        return pltpu.make_async_copy(z_refs[j], z_in.at[pl.ds(ROWS * j, ROWS)], z_sem.at[j])

    def m_copy(j):
        src = mask_away.at[0] if away and j == n - 1 else mask_in.at[sc[j]]
        return pltpu.make_async_copy(src, mask_i.at[pl.ds(ROWS * j, ROWS)], m_sem.at[j])

    def o_copy(j):
        dst = out_away if away and j == n - 1 else out.at[sc[j]]
        return pltpu.make_async_copy(z_out.at[pl.ds(ROWS * j, ROWS)], dst, o_sem.at[j])

    for j in range(n):
        m_copy(j).start()
        z_copy(j).start()
    for j in range(n):
        for r in range(4):
            bias_rows[j, :, pl.ds(pl.multiple_of(ROWS * (sc[n + j] ^ r), ROWS), ROWS), :] = bias_refs[j][r].astype(F32)
    for j in range(n):
        m_copy(j).wait()
    z_copy(0).wait()
    mask[...] = mask_i[...].astype(F32)
    q_s[...] = jnp.zeros_like(q_s)

    @pl.loop(0, n * HEADS)
    def _(h):
        bias_t[h // HEADS, h % HEADS] = bias_rows[h // HEADS, h % HEADS].T

    def project(row, slot):
        row = jnp.minimum(row, n_rows - 1)
        normed = channel_norm(z_in[row], (norms[0], norms[1])).astype(BF16)
        proj = mm(w_all[...], normed)
        k_s[slot] = proj[CH:2 * CH].T.astype(BF16)
        q = proj[:CH].astype(BF16)
        for h in range(HEADS):
            q_s[slot, h, HEAD * h:HEAD * h + HEAD] = q[HEAD * h:HEAD * h + HEAD]
        vn_s[slot] = proj[2 * CH:3 * CH].astype(BF16)
        gn_s[slot] = sigmoid(proj[3 * CH:])

    def keep_mask(row, slot):
        row = jnp.minimum(row, n_rows - 1)
        keep_s[slot] = jnp.broadcast_to(mask[pl.ds(row, 1), :], (LANES, COLS)).T

    def fold(part, op):
        out = part[:8]
        for n in range(1, part.shape[0] // 8):
            out = op(out, part[8 * n:8 * n + 8])
        return out

    def scores(slot, h):
        return mm(k_s[slot], q_s[slot, h])

    def weigh(slot, h, probs):
        heads = slice(HEAD * h, HEAD * h + HEAD)
        o_s[slot, heads] = mm(v_s[slot, heads], probs)

    def step(row, slot, h, logits, defer):
        buf, prev = h % 2, (h + 1) % 2
        sample = jnp.clip(row, 0, n_rows - 1) // ROWS
        top, total, probs = None, None, []
        for c in range(COLS // CHUNK):
            rows = slice(CHUNK * c, CHUNK * c + CHUNK)
            probs.append((e_buf[buf, rows] * jnp.concatenate([inv_s[buf]] * (CHUNK // 8), axis=0)).astype(BF16))
            exps = jnp.exp(s_buf[prev, rows] - jnp.concatenate([top_s[prev]] * (CHUNK // 8), axis=0))
            e_buf[prev, rows] = exps
            part = fold(exps, jnp.add)
            total = part if total is None else total + part
            keep = keep_s[slot, rows]
            keep = jnp.concatenate([keep, keep], axis=1) > 0
            vals = jnp.where(keep, logits[rows] + bias_t[sample, h, rows], MASK_FILL)
            s_buf[buf, rows] = vals
            part = fold(vals, jnp.maximum)
            top = part if top is None else jnp.maximum(top, part)
        top_s[buf] = jnp.broadcast_to(jnp.max(top, axis=0, keepdims=True), (8, COLS))
        inv_s[prev] = jnp.broadcast_to(1.0 / jnp.sum(total, axis=0, keepdims=True), (8, COLS))
        if defer:
            p_s[...] = jnp.concatenate(probs, axis=0)
        else:
            weigh(1 - slot if h < 2 else slot, (h - 2) % HEADS, jnp.concatenate(probs, axis=0))

    def finish(row, slot):
        gated = (g_s[slot] * o_s[slot]).astype(BF16)
        z_out[jnp.maximum(row, 0)] = z_in[jnp.clip(row, 0, n_rows - 1)] + mm(w_proj[...], gated)

    project(0, 0)
    keep_mask(0, 0)
    n_steps = (n_rows + 2 + STEPS - 1) // STEPS

    @pl.loop(0, n_steps)
    def _(it):
        first = STEPS * it - 1
        lg = scores(1, 0)
        weigh(0, 1, p_s[...])
        for k in range(STEPS):
            row, slot, last = first + k, 1 - k % 2, k == STEPS - 1
            for h in range(HEADS):
                nxt = scores(slot, h + 1) if h < HEADS - 1 else (None if last else scores(1 - slot, 0))
                if h == 2:
                    project(row + 2, slot)
                step(row, slot, h, lg, last and h == HEADS - 1)
                lg = nxt
                if h == 3:
                    finish(row - 1, 1 - slot)
                    v_s[1 - slot] = vn_s[1 - slot]
                    g_s[1 - slot] = gn_s[1 - slot]
            keep_mask(row + 2, slot)
        for j in range(1, n):
            @pl.when(it == (ROWS * j - 1) // STEPS - 1)
            def _():
                z_copy(j).wait()

            @pl.when(it == (ROWS * j + 1) // STEPS)
            def _():
                o_copy(j - 1).start()

    o_copy(n - 1).start()
    for j in range(n):
        o_copy(j).wait()


def attend(sc, z_parts, biases, mask, norms, w_all, w_proj, out, mask_away=None):
    n, fresh, away = len(z_parts), out is None, mask_away is not None
    args = (sc, *z_parts, *biases, mask, norms, w_all, w_proj) + ((mask_away,) if away else ()) + (() if fresh else (out,))
    whole = jax.ShapeDtypeStruct((mask.shape[0], ROWS, CH, COLS), F32)
    rows = n * ROWS
    pair = pltpu.VMEM((SLOTS, CH, COLS), BF16)
    wide = pltpu.VMEM((SLOTS, CH, COLS), F32)
    square = pltpu.VMEM((SLOTS, COLS, COLS), F32)
    each = pltpu.VMEM((n, HEADS, COLS, COLS), F32)
    line = pltpu.VMEM((SLOTS, 8, COLS), F32)
    sems = pltpu.SemaphoreType.DMA((n,))
    return pl.pallas_call(
        functools.partial(attention_kernel, n, fresh, away),
        out_shape=(whole, ROW_WIDE) if away else whole,
        in_specs=[SM] + [HB] * n + [VM] * n + [HB] + [VM] * 3 + [HB] * (away + (not fresh)),
        out_specs=(HB, HB) if away else HB,
        scratch_shapes=[
            pltpu.VMEM((rows, CH, COLS), F32), pltpu.VMEM((rows + STEPS, CH, COLS), F32), pltpu.VMEM((rows, COLS), jnp.int32),
            pltpu.VMEM((rows, COLS), F32), each, each, pltpu.VMEM((SLOTS, HEADS, CH, COLS), BF16),
            pltpu.VMEM((SLOTS, COLS, CH), BF16), pair, wide, pair, wide, pltpu.VMEM((SLOTS, COLS, LANES), F32),
            square, square, pltpu.VMEM((COLS, COLS), BF16), line, line, wide, sems, sems, sems,
        ],
        compiler_params=pltpu.CompilerParams(vmem_limit_bytes=48 << 20),
        input_output_aliases={} if fresh else {len(args) - 1: 0},
        name="triangle_attention",
    )(*args)


def exchange(values, r):
    return lax.ppermute(values, 'dap', [(i, i ^ r) for i in range(4)])


def update_weights(params):
    norm_gain, norm_bias, w_a, w_agate, w_b, w_bgate, w_gate, x_gain, x_bias, w_proj = params
    half = jnp.bfloat16(0.5)
    wide = lambda v: jnp.broadcast_to(v[:, None], (CH, COLS))
    deep = lambda v: jnp.broadcast_to(v[:, None, None], (CH, 8, 128))
    return ([wide(norm_gain), wide(norm_bias)], [deep(x_gain), deep(x_bias)],
            half * jnp.concatenate([w_a.T, w_agate.T, w_b.T, w_bgate.T], axis=0), [half * w_gate.T, half * w_proj.T])


def solution(mesh):
    def local_block(pair_z, pair_mask, *weights):
        me = lax.axis_index('dap')
        zt = jnp.transpose(pair_z, (0, 1, 3, 2))
        n_own = zt.shape[0] // 4
        mask_bf = pair_mask.astype(BF16)
        arrived, before = [], ()
        for t in range(n_own):
            got = {}
            for r in (2, 3, 1):
                send = lax.dynamic_index_in_dim(lax.optimization_barrier((zt, *before))[0], n_own * (me ^ r) + t, 0, keepdims=False)
                if t == 0 or r == 1:
                    before = (send,)
                got[r] = exchange(send, r)
                if t == 0 and r == 2:
                    mask_bf, weights = lax.optimization_barrier((mask_bf, weights, send))[:2]
                    masks = [lax.dynamic_slice_in_dim(mask_bf, n_own * (me ^ k), n_own, axis=0) for k in range(4)]
                    before = (*before, *masks)
                    masks = [exchange(m, k) if k else m for k, m in enumerate(masks)]
            arrived.append((got[1], got[2], got[3]))

        out_n, out_x, out_ab, out_sq = update_weights(weights[:10])
        in_n, in_x, in_ab, in_sq = update_weights(weights[10:20])
        att_gain, att_shift, w_q, w_k, w_v, w_bias, w_gate, w_proj = weights[20:]
        att_n = [jnp.broadcast_to(v[:, None], (CH, COLS)) for v in (att_gain, att_shift)]
        norms = jnp.stack(out_n + in_n + att_n)
        xgs = jnp.stack(out_x + in_x)
        w_ab = jnp.stack([out_ab, in_ab])
        w_sq = jnp.stack(out_sq + in_sq)
        w_bias8 = jnp.concatenate([w_bias.T, jnp.zeros((4, CH), BF16)], axis=0)
        w_all = jnp.concatenate([w_q.T * jnp.bfloat16(HEAD ** -0.5), w_k.T, w_v.T, w_gate.T], axis=0)
        w_out = w_proj.T
        att_norms = norms[4:]

        token = [None]

        def ordered(call, sc, *args):
            sc = jnp.stack([jnp.asarray(v, jnp.int32) for v in sc])
            if token[0] is not None:
                sc = lax.optimization_barrier((sc, token[0]))[0]
            res = call(sc, *args)
            token[0] = jax.tree.leaves(res)[-1]
            return res

        def attention(jobs, out, mask_away=None):
            samples, orders, z_parts, biases = zip(*jobs)
            return ordered(attend, samples + orders, z_parts, biases, pair_mask, att_norms, w_all, w_out, out, mask_away)

        far = [(t, r) for t in range(n_own) for r in (2, 3)]
        a_far, b_far = ordered(l1_call, [n_own * (me ^ r) + t for t, r in far], zt, pair_mask, norms, w_ab)
        b_par = exchange(b_far, 1)
        x_near = ordered(l2_call, [me], a_far, b_far, b_par, xgs)

        out = None
        held = []
        for t in range(n_own):
            last = t == n_own - 1
            z_own, z_par, bias, far2, far3 = ordered(functools.partial(u_call, last), [me, n_own * me + t], zt,
                                                     arrived[t], [m[t] for m in masks], norms, xgs, w_ab, w_sq, w_bias8)
            near = (n_own * (me ^ 1) + t, 0, exchange(z_par, 1), exchange(bias, 1))
            held.append({2: exchange(far2, 2)})
            own = (n_own * me + t, 0, z_own, bias)
            if last:
                out, away = attention([own, (0, 0, far3, bias)], out, masks[3][t][None].astype(jnp.int32))
                away = exchange(away, 3)
            else:
                held[t][3] = exchange(far3, 3)
                out = attention([own, near], out)
        for t in range(n_own):
            last = t == n_own - 1
            mine, z_two, biases = {}, {}, {}
            for r in held[t]:
                z_two[r], bias_own = ordered(r_call, [me, n_own * (me ^ r) + t, far.index((t, r))], zt, x_near,
                                             held[t][r], norms, w_sq, w_bias8)
                mine[r] = [bias_own, *jnp.split(held[t][r][FAR_BIAS:], 3 if last else 1)]
            if last:
                biases[2] = jnp.stack([mine[2][k] for k in (0, 3, 1, 2)])
            else:
                par = exchange(jnp.stack(mine[3] + mine[2]), 1)
                biases = {r: jnp.stack([mine[r][0], par[2 * r - 4], mine[r][1], par[2 * r - 3]]) for r in (2, 3)}
            out = attention(([] if t else [near]) + [
                (n_own * (me ^ r) + t, me, z_two[r], biases[r]) for r in biases], out)
        out = lax.dynamic_update_index_in_dim(out, away, n_own * (me ^ 3) + n_own - 1, 0)
        return jnp.transpose(out, (0, 1, 3, 2))

    pair_spec = P('data', 'dap')
    return jax.shard_map(local_block, mesh=mesh, in_specs=(pair_spec, pair_spec) + (P(),) * 28,
                         out_specs=pair_spec, check_vma=False)
```

```python
import functools

import jax
import jax.numpy as jnp
from jax import lax
from jax.experimental import pallas as pl
from jax.experimental.pallas import tpu as pltpu
from jax.sharding import PartitionSpec as P


LN_EPS = 1e-5
F32, BF16 = jnp.float32, jnp.bfloat16
ROWS, CH, COLS = 64, 64, 256
TILE = 16


def channel_stats(vals, axis_id):
    ch_mean = jnp.mean(vals, axis=axis_id, keepdims=True)
    ch_var = jnp.mean(jnp.square(vals - ch_mean), axis=axis_id, keepdims=True)
    return ch_mean, lax.rsqrt(ch_var + LN_EPS)


def channel_norm(vals, norm, stats=None):
    ch_mean, scale = channel_stats(vals, 0) if stats is None else stats
    return (vals - ch_mean) * scale * norm[0] + norm[1]


def sigmoid(vals):
    return 0.5 * jnp.tanh(0.5 * vals) + 0.5


def mm(lhs, rhs):
    return jnp.dot(lhs, rhs, preferred_element_type=F32)


def ab_row(proj, tile_a, tile_b, slot):
    for n, tile in enumerate((tile_a, tile_b)):
        linear, gate = jnp.split(proj[2 * CH * n:2 * CH * n + 2 * CH], 2, axis=0)
        tile[slot] = ((jnp.tanh(gate) + 1.0) * linear).astype(BF16)


def x_norm_tile(x_s, tile_x, base, xg, xb):
    parts = [(sub, half) for sub in range(2) for half in range(2)]

    def load(c, part):
        return x_s[c, pl.ds(pl.multiple_of(base + 8 * part[0], 8), 8), 128 * part[1]:128 * part[1] + 128]

    means = [sum(load(c, p) for c in range(CH)) * (1.0 / CH) for p in parts]
    scales = [lax.rsqrt(sum(jnp.square(load(c, p) - means[n]) for c in range(CH)) * (1.0 / CH) + LN_EPS)
              for n, p in enumerate(parts)]
    for c in range(CH):
        rows = []
        for sub in range(2):
            rows.append(jnp.concatenate(
                [(load(c, (sub, half)) - means[2 * sub + half]) * scales[2 * sub + half] * xg[c] + xb[c]
                 for half in range(2)], axis=1))
        tile_x[c] = jnp.concatenate(rows, axis=0).astype(BF16)


LAG = 3


def staggered(count, *stages):
    held = [{} for _ in stages]
    for tick in range(count + LAG * (len(stages) - 1)):
        for k, stage in enumerate(stages):
            i = tick - LAG * k
            if 0 <= i < count:
                held[k][i] = stage(i, held[k - 1].pop(i) if k else None)


def u_kernel(last, layout, sc, *refs):
    z_refs = refs[:len(layout)]
    (mask0, mask1, mask2, mask3, norms, xgs, w_ab, w_sq, w_bias, z2_own, z2_par, bias_out, far2, far3,
     z_s, a_s, b_s, x_s, mask, stats, tile_a, tile_b, tile_x, tile_c, tile_d, tile_z, in_sem, z_sem, x_sem) = refs[len(layout):]
    me, sample = sc[0], sc[1]
    lanes = pl.ds(pl.multiple_of(LANES * (me // 2), LANES), LANES)
    out_norm = (norms[0], norms[1])
    in_norm = (norms[2], norms[3])
    att_norm = (norms[4], norms[5])
    n_tiles = COLS // TILE

    for ref, (r, start) in zip(z_refs, layout):
        src = ref if r else ref.at[sample]
        rows = pl.ds(pl.multiple_of(ROWS * (me ^ r) + start, 8), src.shape[0])
        pltpu.make_async_copy(src, z_s.at[rows], in_sem.at[r]).start()
    for r, part in enumerate((mask0, mask1, mask2, mask3)):
        mask[pl.ds(pl.multiple_of(ROWS * (me ^ r), ROWS), ROWS), :] = part[:].astype(F32)

    def mask_row(base, i):
        return mask[pl.ds(base + i, 1), :]

    def measure(base, i, vals=None):
        found = channel_stats(z_s[base + i] if vals is None else vals, 0)
        for n in range(2):
            stats[n if vals is None else n + 2, pl.ds(base + i, 1), :] = found[n]
        return found

    def recall(base, i, first):
        return [stats[first + n, pl.ds(base + i, 1), :] for n in range(2)]

    def flush(base):
        a_s[:, pl.ds(base, TILE), :] = jnp.swapaxes(tile_a[:], 0, 1)
        b_s[:, pl.ds(base, TILE), :] = jnp.swapaxes(tile_b[:], 0, 1)

    def export(t, start, outgoing, sem):
        r = (t * TILE // ROWS) ^ me
        q = t % (ROWS // TILE)
        rows = pl.ds(pl.multiple_of(TILE * q, TILE), TILE)
        half = pl.ds(pl.multiple_of(ROWS + TILE * (q % 2), TILE), TILE)
        side = pl.ds(pl.multiple_of(LANES * (q // 2), LANES), LANES)
        act = (lambda cp: cp.start()) if start else (lambda cp: cp.wait())
        for k, dst in ((0, z2_own), (1, z2_par), (2, far2), (3, far3)):
            plain = k < 2 or (last and k == 3)
            if not (outgoing and plain):
                @pl.when(r == k)
                def _():
                    if plain:
                        src, to = tile_z.at[t % 2], dst.at[rows]
                    elif outgoing:
                        src, to = tile_c.at[t % 2, :, :, lanes], dst.at[half, :, side]
                    else:
                        src, to = tile_c.at[t % 2], dst.at[rows]
                    act(pltpu.make_async_copy(src, to, sem.at[t % 2]))

    @pl.loop(0, n_tiles)
    def _(v):
        r = v * TILE // ROWS

        @pl.when(v * TILE % ROWS == 0)
        def _():
            pltpu.make_async_copy(z_refs[0].at[sample], z_s.at[pl.ds(0, ROWS)], in_sem.at[r]).wait()

        base = pl.multiple_of(ROWS * (me ^ r) + v * TILE % ROWS, TILE)
        staggered(
            TILE,
            lambda i, _: mm(w_ab[0], (mask_row(base, i) * channel_norm(z_s[base + i], out_norm, measure(base, i))).astype(BF16)),
            lambda i, proj: ab_row(proj, tile_a, tile_b, i))
        flush(base)

    @pl.loop(0, CH, unroll=4)
    def _(c):
        x_s[c] = lax.dot_general(a_s[c], b_s[c], (((1,), (1,)), ((), ())), preferred_element_type=F32)

    @pl.loop(0, n_tiles)
    def _(t):
        base = pl.multiple_of(TILE * t, TILE)

        @pl.when(t >= 2)
        def _():
            export(t - 2, False, True, x_sem)

        x_norm_tile(x_s, tile_x, base, xgs.at[0], xgs.at[1])
        tile_c[t % 2] = jnp.swapaxes(tile_x[:], 0, 1)

        def gate_and_update(i, _):
            normed = channel_norm(z_s[base + i], out_norm, recall(base, i, 0)).astype(BF16)
            return mm(w_sq[0], normed), mm(w_sq[1], tile_c[t % 2, i])

        def next_norm(i, parts):
            z_one = z_s[base + i] + (jnp.tanh(parts[0]) + 1.0) * parts[1]
            tile_z[0, i] = z_one
            return (mask_row(base, i) * channel_norm(z_one, in_norm, measure(base, i, z_one))).astype(BF16)

        staggered(TILE, gate_and_update, next_norm, lambda i, normed: mm(w_ab[1], normed),
                  lambda i, proj: ab_row(proj, tile_a, tile_b, i))
        flush(base)
        z_s[pl.ds(base, TILE)] = tile_z[0]
        export(t, True, True, x_sem)

    for t in (n_tiles - 2, n_tiles - 1):
        export(t, False, True, x_sem)

    @pl.loop(0, CH, unroll=4)
    def _(c):
        x_s[c] = lax.dot_general(a_s[c], b_s[c], (((0,), (0,)), ((), ())), preferred_element_type=F32)

    @pl.loop(0, n_tiles)
    def _(t):
        base = pl.multiple_of(TILE * t, TILE)

        @pl.when(t >= 2)
        def _():
            export(t - 2, False, False, z_sem)

        x_norm_tile(x_s, tile_x, base, xgs.at[2], xgs.at[3])
        tile_c[t % 2] = jnp.swapaxes(tile_x[:], 0, 1)

        def gate_and_update(i, _):
            normed = channel_norm(z_s[base + i], in_norm, recall(base, i, 2)).astype(BF16)
            return mm(w_sq[2], normed), mm(w_sq[3], tile_c[t % 2, i])

        def next_norm(i, parts):
            z_two = z_s[base + i] + (jnp.tanh(parts[0]) + 1.0) * parts[1]
            tile_z[t % 2, i] = z_two
            return channel_norm(z_two, att_norm).astype(BF16)

        def bias_row(i, normed):
            tile_d[i] = mm(w_bias[:], normed)

        staggered(TILE, gate_and_update, next_norm, bias_row)
        rows = pl.ds(pl.multiple_of(t * TILE % ROWS, TILE), TILE)
        bias_out[t * TILE // ROWS, :, rows, :] = jnp.swapaxes(tile_d[:], 0, 1)[:4].astype(BF16)
        export(t, True, False, z_sem)

    bias_to = ((far2, 0, 0), (far2, 1, 1), (far2, 3, 2)) if last else ((far2, 0, 0), (far3, 1, 0))

    def bias_copy(n):
        dst, block, place = bias_to[n]
        return pltpu.make_async_copy(bias_out.at[me ^ block], dst.at[pl.ds(FAR_BIAS + 4 * place, 4)], in_sem.at[n])

    for n in range(len(bias_to)):
        bias_copy(n).start()
    for t in (n_tiles - 2, n_tiles - 1):
        export(t, False, False, z_sem)
    for n in range(len(bias_to)):
        bias_copy(n).wait()


LANES = 128
VM = pl.BlockSpec(memory_space=pltpu.VMEM)
HB = pl.BlockSpec(memory_space=pl.ANY)
SM = pl.BlockSpec(memory_space=pltpu.SMEM)
PARAMS = pltpu.CompilerParams(vmem_limit_bytes=40 << 20, dimension_semantics=("arbitrary",))
AB_TILE = pltpu.VMEM((TILE, CH, COLS), BF16)
DMA2 = pltpu.SemaphoreType.DMA((2,))
FAR_BIAS = ROWS + ROWS // 2
FAR = jax.ShapeDtypeStruct((FAR_BIAS + 4, CH, COLS), BF16)
FAR_LAST = jax.ShapeDtypeStruct((FAR_BIAS + 12, CH, COLS), BF16)
ROW_WIDE = jax.ShapeDtypeStruct((ROWS, CH, COLS), F32)
SAMPLE_BF = pltpu.VMEM((CH, COLS, COLS), BF16)


def u_call(last, layout, sc, z_parts, masks, norms, xgs, w_ab, w_sq, w_bias):
    return pl.pallas_call(
        functools.partial(u_kernel, last, layout),
        out_shape=(ROW_WIDE, ROW_WIDE, jax.ShapeDtypeStruct((4, 4, ROWS, COLS), BF16), *((FAR_LAST, ROW_WIDE) if last else (FAR, FAR))),
        in_specs=[SM] + [HB] * len(layout) + [VM] * 9,
        out_specs=(HB, HB, VM, HB, HB),
        scratch_shapes=[
            pltpu.VMEM((COLS, CH, COLS), F32), SAMPLE_BF, SAMPLE_BF,
            pltpu.VMEM((CH, COLS, COLS), F32), pltpu.VMEM((COLS, COLS), F32), pltpu.VMEM((4, COLS, COLS), F32), AB_TILE, AB_TILE, pltpu.VMEM((CH, TILE, COLS), BF16), pltpu.VMEM((2, TILE, CH, COLS), BF16),
            pltpu.VMEM((TILE, 8, COLS), F32), pltpu.VMEM((2, TILE, CH, COLS), F32),
            pltpu.SemaphoreType.DMA((4,)), DMA2, DMA2,
        ],
        compiler_params=pltpu.CompilerParams(vmem_limit_bytes=62 << 20),
        name="pair_updates",
    )(sc, *z_parts, *masks, norms, xgs, w_ab, w_sq, w_bias)


def l1_kernel(ids, z_in, mask_in, norms, w_ab, a_out, b_out, mask, tile_a, tile_b):
    out_norm = (norms[0], norms[1])
    mask[:] = mask_in[0].astype(F32)

    @pl.loop(0, ROWS // TILE)
    def _(t):
        base = pl.multiple_of(TILE * t, TILE)
        staggered(
            TILE,
            lambda i, _: mm(w_ab[0], (mask[pl.ds(base + i, 1), :] * channel_norm(z_in[0, base + i], out_norm)).astype(BF16)),
            lambda i, proj: ab_row(proj, tile_a, tile_b, i))
        a_out[0, :, pl.ds(base, TILE), :] = jnp.swapaxes(tile_a[:], 0, 1)
        b_out[0, :, pl.ds(base, TILE), :] = jnp.swapaxes(tile_b[:], 0, 1)


def l1_call(ids, zt, mask, norms, w_ab):
    n = ids.shape[0]
    ab = jax.ShapeDtypeStruct((n, CH, ROWS, COLS), BF16)
    ab_spec = pl.BlockSpec((1, CH, ROWS, COLS), lambda i, ids: (i, 0, 0, 0))
    return pl.pallas_call(
        l1_kernel,
        out_shape=(ab, ab),
        grid_spec=pltpu.PrefetchScalarGridSpec(
            num_scalar_prefetch=1, grid=(n,),
            in_specs=[pl.BlockSpec((1, ROWS, CH, COLS), lambda i, ids: (ids[i], 0, 0, 0)),
                      pl.BlockSpec((1, ROWS, COLS), lambda i, ids: (ids[i], 0, 0)), VM, VM],
            out_specs=(ab_spec, ab_spec),
            scratch_shapes=[pltpu.VMEM((ROWS, COLS), F32), AB_TILE, AB_TILE]),
        compiler_params=PARAMS,
        name="near_projections",
    )(ids, zt, mask, norms, w_ab)


def l2_kernel(sc, a_in, b_own, b_par, xgs, x_out, x_s, tile_x):
    odd = sc[0] % 2 == 1

    @pl.loop(0, CH, unroll=2)
    def _(c):
        for n in range(2):
            own, par = b_own[n, c].astype(F32), b_par[1 - n, c].astype(F32)
            pair = jnp.concatenate([jnp.where(odd, par, own), jnp.where(odd, own, par)], axis=0).astype(BF16)
            x_s[c, :, LANES * n:LANES * n + LANES] = lax.dot_general(
                a_in[n, c], pair, (((1,), (1,)), ((), ())), preferred_element_type=F32)

    @pl.loop(0, ROWS // TILE)
    def _(t):
        base = pl.multiple_of(TILE * t, TILE)
        x_norm_tile(x_s, tile_x, base, xgs.at[0], xgs.at[1])
        both = jnp.swapaxes(tile_x[:], 0, 1)
        for n in range(2):
            x_out[n, pl.ds(base, TILE)] = both[:, :, LANES * n:LANES * n + LANES]


def l2_call(sc, a_all, b_own, b_par, xgs):
    n = a_all.shape[0]
    ab_spec = pl.BlockSpec((2, CH, ROWS, COLS), lambda i: (i, 0, 0, 0))
    return pl.pallas_call(
        l2_kernel,
        grid=(n // 2,),
        out_shape=jax.ShapeDtypeStruct((n, ROWS, CH, LANES), BF16),
        in_specs=[SM, ab_spec, ab_spec, ab_spec, VM],
        out_specs=pl.BlockSpec((2, ROWS, CH, LANES), lambda i: (i, 0, 0, 0)),
        scratch_shapes=[pltpu.VMEM((CH, ROWS, COLS), F32), pltpu.VMEM((CH, TILE, COLS), BF16)],
        compiler_params=PARAMS,
        name="near_product",
    )(sc, a_all, b_own, b_par, xgs)


def r_kernel(sc, z_in, x_near, x_far, xi, norms, w_sq, w_bias, z_out, bias_out, tile_d):
    first = sc[0] < 2
    out_norm = (norms[0], norms[1])
    in_norm = (norms[2], norms[3])
    att_norm = (norms[4], norms[5])

    def outgoing(i, _):
        near, far = x_near[0, i].astype(F32), x_far[i].astype(F32)
        xn = jnp.concatenate([jnp.where(first, near, far), jnp.where(first, far, near)], axis=1).astype(BF16)
        normed = channel_norm(z_in[0, i], out_norm).astype(BF16)
        return mm(w_sq[0], normed), mm(w_sq[1], xn)

    def norm_one(i, parts):
        z_one = z_in[0, i] + (jnp.tanh(parts[0]) + 1.0) * parts[1]
        z_out[i] = z_one
        return channel_norm(z_one, in_norm).astype(BF16)

    def incoming(i, normed):
        return mm(w_sq[2], normed), mm(w_sq[3], xi[i])

    def norm_two(i, parts):
        z_two = z_out[i] + (jnp.tanh(parts[0]) + 1.0) * parts[1]
        z_out[i] = z_two
        return channel_norm(z_two, att_norm).astype(BF16)

    def bias_row(i, normed):
        tile_d[i] = mm(w_bias[:], normed)

    staggered(TILE, outgoing, norm_one, incoming, norm_two, bias_row)
    bias_out[:] = jnp.swapaxes(tile_d[:], 0, 1)[:4].astype(BF16)


def r_call(sc, zt, x_near, far, norms, w_sq, w_bias):
    return pl.pallas_call(
        r_kernel,
        out_shape=(ROW_WIDE, jax.ShapeDtypeStruct((4, ROWS, COLS), BF16)),
        grid_spec=pltpu.PrefetchScalarGridSpec(
            num_scalar_prefetch=1, grid=(ROWS // TILE,),
            in_specs=[pl.BlockSpec((1, TILE, CH, COLS), lambda i, sc: (sc[1], i, 0, 0)),
                      pl.BlockSpec((1, TILE, CH, LANES), lambda i, sc: (sc[2], i, 0, 0)),
                      pl.BlockSpec((TILE, CH, LANES), lambda i, sc: (ROWS // TILE + i % 2, 0, i // 2)),
                      pl.BlockSpec((TILE, CH, COLS), lambda i, sc: (i, 0, 0)), VM, VM, VM],
            out_specs=(pl.BlockSpec((TILE, CH, COLS), lambda i, sc: (i, 0, 0)),
                       pl.BlockSpec((4, TILE, COLS), lambda i, sc: (0, i, 0))),
            scratch_shapes=[pltpu.VMEM((TILE, 8, COLS), F32)]),
        compiler_params=PARAMS,
        name="row_updates",
    )(sc, zt, x_near, far, far, norms, w_sq, w_bias)


HEADS, HEAD = 4, 16
MASK_FILL = -1e9
CHUNK = 32
SLOTS = 2
STEPS = 6
AWAY_FIRST = 48


def attention_kernel(n, fresh, away, sc, *refs):
    z_refs, bias_refs = refs[:n], refs[n:2 * n]
    mask_in, norms, w_all, w_proj = refs[2 * n:2 * n + 4]
    rest = refs[2 * n + 4 + away + (not fresh):]
    mask_away, out_away = refs[2 * n + 4], rest[1:1 + 2 * away]
    (out, z_in, z_out, mask_i, mask, bias_rows, bias_t, q_s, k_s, v_s, g_s, vn_s, gn_s, keep_s, s_buf, e_buf, p_s,
     top_s, inv_s, o_s, m_sem, z_sem, o_sem) = rest[:1] + rest[1 + 2 * away:]
    n_rows = n * ROWS

    def z_copy(j):
        return pltpu.make_async_copy(z_refs[j], z_in.at[pl.ds(ROWS * j, ROWS)], z_sem.at[j])

    def m_copy(j):
        src = mask_away.at[0] if away and j == n - 1 else mask_in.at[sc[j]]
        return pltpu.make_async_copy(src, mask_i.at[pl.ds(ROWS * j, ROWS)], m_sem.at[j])

    def o_copy(j):
        return pltpu.make_async_copy(z_out.at[pl.ds(ROWS * j, ROWS)], out.at[sc[j]], o_sem.at[j])

    def o_copies(j):
        if not (away and j == n - 1):
            return [o_copy(j)]
        return [pltpu.make_async_copy(z_out.at[pl.ds(ROWS * j + start, ref.shape[0])], ref, o_sem.at[j])
                for ref, start in zip(out_away, (0, AWAY_FIRST))]

    for j in range(n):
        m_copy(j).start()
        z_copy(j).start()
    for j in range(n):
        for r in range(4):
            bias_rows[j, :, pl.ds(pl.multiple_of(ROWS * (sc[n + j] ^ r), ROWS), ROWS), :] = bias_refs[j][r].astype(F32)
    for j in range(n):
        m_copy(j).wait()
    z_copy(0).wait()
    mask[:] = mask_i[:].astype(F32)
    q_s[:] = jnp.zeros_like(q_s)

    @pl.loop(0, n * HEADS)
    def _(h):
        bias_t[h // HEADS, h % HEADS] = bias_rows[h // HEADS, h % HEADS].T

    def project(row, slot):
        row = jnp.minimum(row, n_rows - 1)
        normed = channel_norm(z_in[row], (norms[0], norms[1])).astype(BF16)
        proj = mm(w_all[:], normed)
        k_s[slot] = proj[CH:2 * CH].T.astype(BF16)
        q = proj[:CH].astype(BF16)
        for h in range(HEADS):
            q_s[slot, h, HEAD * h:HEAD * h + HEAD] = q[HEAD * h:HEAD * h + HEAD]
        vn_s[slot] = proj[2 * CH:3 * CH].astype(BF16)
        gn_s[slot] = sigmoid(proj[3 * CH:])

    def keep_mask(row, slot):
        row = jnp.minimum(row, n_rows - 1)
        keep_s[slot] = jnp.broadcast_to(mask[pl.ds(row, 1), :], (LANES, COLS)).T

    def fold(part, op):
        out = part[:8]
        for n in range(1, part.shape[0] // 8):
            out = op(out, part[8 * n:8 * n + 8])
        return out

    def scores(slot, h):
        return mm(k_s[slot], q_s[slot, h])

    def weigh(slot, h, probs):
        heads = slice(HEAD * h, HEAD * h + HEAD)
        o_s[slot, heads] = mm(v_s[slot, heads], probs)

    def step(row, slot, h, logits, defer):
        buf, prev = h % 2, (h + 1) % 2
        sample = jnp.clip(row, 0, n_rows - 1) // ROWS
        top, total, probs = None, None, []
        for c in range(COLS // CHUNK):
            rows = slice(CHUNK * c, CHUNK * c + CHUNK)
            probs.append((e_buf[buf, rows] * jnp.concatenate([inv_s[buf]] * (CHUNK // 8), axis=0)).astype(BF16))
            exps = jnp.exp(s_buf[prev, rows] - jnp.concatenate([top_s[prev]] * (CHUNK // 8), axis=0))
            e_buf[prev, rows] = exps
            part = fold(exps, jnp.add)
            total = part if total is None else total + part
            keep = keep_s[slot, rows]
            keep = jnp.concatenate([keep, keep], axis=1) > 0
            vals = jnp.where(keep, logits[rows] + bias_t[sample, h, rows], MASK_FILL)
            s_buf[buf, rows] = vals
            part = fold(vals, jnp.maximum)
            top = part if top is None else jnp.maximum(top, part)
        top_s[buf] = jnp.broadcast_to(jnp.max(top, axis=0, keepdims=True), (8, COLS))
        inv_s[prev] = jnp.broadcast_to(1.0 / jnp.sum(total, axis=0, keepdims=True), (8, COLS))
        if defer:
            p_s[:] = jnp.concatenate(probs, axis=0)
        else:
            weigh(1 - slot if h < 2 else slot, (h - 2) % HEADS, jnp.concatenate(probs, axis=0))

    def finish(row, slot):
        gated = (g_s[slot] * o_s[slot]).astype(BF16)
        z_out[jnp.maximum(row, 0)] = z_in[jnp.clip(row, 0, n_rows - 1)] + mm(w_proj[:], gated)

    project(0, 0)
    keep_mask(0, 0)
    n_steps = (n_rows + 2 + STEPS - 1) // STEPS

    @pl.loop(0, n_steps)
    def _(it):
        first = STEPS * it - 1
        lg = scores(1, 0)
        weigh(0, 1, p_s[:])
        for k in range(STEPS):
            row, slot, last = first + k, 1 - k % 2, k == STEPS - 1
            for h in range(HEADS):
                nxt = scores(slot, h + 1) if h < HEADS - 1 else (None if last else scores(1 - slot, 0))
                if h == 2:
                    project(row + 2, slot)
                step(row, slot, h, lg, last and h == HEADS - 1)
                lg = nxt
                if h == 3:
                    finish(row - 1, 1 - slot)
                    v_s[1 - slot] = vn_s[1 - slot]
                    g_s[1 - slot] = gn_s[1 - slot]
            keep_mask(row + 2, slot)
        for j in range(1, n):
            @pl.when(it == (ROWS * j - 1) // STEPS - 1)
            def _():
                z_copy(j).wait()

            @pl.when(it == (ROWS * j + 1) // STEPS)
            def _():
                o_copy(j - 1).start()

    for copy in o_copies(n - 1):
        copy.start()
    for j in range(n):
        for copy in o_copies(j):
            copy.wait()


def attend(sc, z_parts, biases, mask, norms, w_all, w_proj, out, mask_away=None):
    n, fresh, away = len(z_parts), out is None, mask_away is not None
    args = (sc, *z_parts, *biases, mask, norms, w_all, w_proj) + ((mask_away,) if away else ()) + (() if fresh else (out,))
    whole = jax.ShapeDtypeStruct((mask.shape[0], ROWS, CH, COLS), F32)
    aways = [jax.ShapeDtypeStruct((k, CH, COLS), F32) for k in (AWAY_FIRST, ROWS - AWAY_FIRST)]
    rows = n * ROWS
    pair = pltpu.VMEM((SLOTS, CH, COLS), BF16)
    wide = pltpu.VMEM((SLOTS, CH, COLS), F32)
    square = pltpu.VMEM((SLOTS, COLS, COLS), F32)
    each = pltpu.VMEM((n, HEADS, COLS, COLS), F32)
    line = pltpu.VMEM((SLOTS, 8, COLS), F32)
    sems = pltpu.SemaphoreType.DMA((n,))
    return pl.pallas_call(
        functools.partial(attention_kernel, n, fresh, away),
        out_shape=(whole, *aways) if away else whole,
        in_specs=[SM] + [HB] * n + [VM] * n + [HB] + [VM] * 3 + [HB] * (away + (not fresh)),
        out_specs=(HB, HB, HB) if away else HB,
        scratch_shapes=[
            pltpu.VMEM((rows, CH, COLS), F32), pltpu.VMEM((rows + STEPS, CH, COLS), F32), pltpu.VMEM((rows, COLS), jnp.int32),
            pltpu.VMEM((rows, COLS), F32), each, each, pltpu.VMEM((SLOTS, HEADS, CH, COLS), BF16),
            pltpu.VMEM((SLOTS, COLS, CH), BF16), pair, wide, pair, wide, pltpu.VMEM((SLOTS, COLS, LANES), F32),
            square, square, pltpu.VMEM((COLS, COLS), BF16), line, line, wide, sems, sems, sems,
        ],
        compiler_params=pltpu.CompilerParams(vmem_limit_bytes=48 << 20),
        input_output_aliases={} if fresh else {len(args) - 1: 0},
        name="triangle_attention",
    )(*args)


FIRST = 8


def exchange(values, r):
    return lax.ppermute(values, 'dap', [(i, i ^ r) for i in range(4)])


def update_weights(params):
    norm_gain, norm_bias, w_a, w_agate, w_b, w_bgate, w_gate, x_gain, x_bias, w_proj = params
    half = jnp.bfloat16(0.5)
    wide = lambda v: jnp.broadcast_to(v[:, None], (CH, COLS))
    deep = lambda v: jnp.broadcast_to(v[:, None, None], (CH, 8, 128))
    return ([wide(norm_gain), wide(norm_bias)], [deep(x_gain), deep(x_bias)],
            half * jnp.concatenate([w_a.T, w_agate.T, w_b.T, w_bgate.T], axis=0), [half * w_gate.T, half * w_proj.T])


def solution(mesh):
    def local_block(pair_z, pair_mask, *weights):
        me = lax.axis_index('dap')
        zt = jnp.transpose(pair_z, (0, 1, 3, 2))
        n_own = zt.shape[0] // 4
        mask_bf = pair_mask.astype(BF16)
        arrived, layouts, before = [], [], ()
        for t in range(n_own):
            pieces = [(2, 0, FIRST), (2, FIRST, ROWS)] if t == 0 else [(2, 0, ROWS)]
            pieces += [(3, 0, ROWS), (1, 0, ROWS)]
            got = []
            for r, start, stop in pieces:
                where = (n_own * (me ^ r) + t, start, 0, 0)
                send = lax.dynamic_slice(lax.optimization_barrier((zt, *before))[0], where, (1, stop - start, CH, COLS))[0]
                if t == 0 or r == 1:
                    before = (send,)
                got.append(exchange(send, r))
                if t == 0 and stop == ROWS and r == 2:
                    mask_bf, weights = lax.optimization_barrier((mask_bf, weights, send))[:2]
                    masks = [lax.dynamic_slice_in_dim(mask_bf, n_own * (me ^ k), n_own, axis=0) for k in range(4)]
                    before = (*before, *masks)
                    masks = [exchange(m, k) if k else m for k, m in enumerate(masks)]
            arrived.append([zt, *got])
            layouts.append(((0, 0), *((r, start) for r, start, _ in pieces)))

        out_n, out_x, out_ab, out_sq = update_weights(weights[:10])
        in_n, in_x, in_ab, in_sq = update_weights(weights[10:20])
        att_gain, att_shift, w_q, w_k, w_v, w_bias, w_gate, w_proj = weights[20:]
        att_n = [jnp.broadcast_to(v[:, None], (CH, COLS)) for v in (att_gain, att_shift)]
        norms = jnp.stack(out_n + in_n + att_n)
        xgs = jnp.stack(out_x + in_x)
        w_ab = jnp.stack([out_ab, in_ab])
        w_sq = jnp.stack(out_sq + in_sq)
        w_bias8 = jnp.concatenate([w_bias.T, jnp.zeros((4, CH), BF16)], axis=0)
        w_all = jnp.concatenate([w_q.T * jnp.bfloat16(HEAD ** -0.5), w_k.T, w_v.T, w_gate.T], axis=0)
        w_out = w_proj.T
        att_norms = norms[4:]

        token = [None]

        def ordered(call, sc, *args):
            sc = jnp.stack([jnp.asarray(v, jnp.int32) for v in sc])
            if token[0] is not None:
                sc = lax.optimization_barrier((sc, token[0]))[0]
            res = call(sc, *args)
            token[0] = jax.tree.leaves(res)[-1]
            return res

        def attention(jobs, out, mask_away=None):
            samples, orders, z_parts, biases = zip(*jobs)
            return ordered(attend, samples + orders, z_parts, biases, pair_mask, att_norms, w_all, w_out, out, mask_away)

        far = [(t, r) for t in range(n_own) for r in (2, 3)]
        a_far, b_far = ordered(l1_call, [n_own * (me ^ r) + t for t, r in far], zt, pair_mask, norms, w_ab)
        b_par = exchange(b_far, 1)
        x_near = ordered(l2_call, [me], a_far, b_far, b_par, xgs)

        out = None
        held = []
        for t in range(n_own):
            last = t == n_own - 1
            z_own, z_par, bias, far2, far3 = ordered(functools.partial(u_call, last, layouts[t]), [me, n_own * me + t],
                                                     arrived[t], [m[t] for m in masks], norms, xgs, w_ab, w_sq, w_bias8)
            near = (n_own * (me ^ 1) + t, 0, exchange(z_par, 1), exchange(bias, 1))
            held.append({2: exchange(far2, 2)})
            own = (n_own * me + t, 0, z_own, bias)
            if last:
                out, *away = attention([own, (0, 0, far3, bias)], out, masks[3][t][None].astype(jnp.int32))
                away = [exchange(v, 3) for v in away]
            else:
                held[t][3] = exchange(far3, 3)
                out = attention([own, near], out)
        for t in range(n_own):
            last = t == n_own - 1
            mine, z_two, biases = {}, {}, {}
            for r in held[t]:
                z_two[r], bias_own = ordered(r_call, [me, n_own * (me ^ r) + t, far.index((t, r))], zt, x_near,
                                             held[t][r], norms, w_sq, w_bias8)
                mine[r] = [bias_own, *jnp.split(held[t][r][FAR_BIAS:], 3 if last else 1)]
            if last:
                biases[2] = jnp.stack([mine[2][k] for k in (0, 3, 1, 2)])
            else:
                par = exchange(jnp.stack(mine[3] + mine[2]), 1)
                biases = {r: jnp.stack([mine[r][0], par[2 * r - 4], mine[r][1], par[2 * r - 3]]) for r in (2, 3)}
            out = attention(([] if t else [near]) + [
                (n_own * (me ^ r) + t, me, z_two[r], biases[r]) for r in biases], out)
        for v, start in zip(away, (0, AWAY_FIRST)):
            out = lax.dynamic_update_slice(out, v[None], (n_own * (me ^ 3) + n_own - 1, start, 0, 0))
        return jnp.transpose(out, (0, 1, 3, 2))

    pair_spec = P('data', 'dap')
    return jax.shard_map(local_block, mesh=mesh, in_specs=(pair_spec, pair_spec) + (P(),) * 28,
                         out_specs=pair_spec, check_vma=False)
```

```python
import functools

import jax
import jax.numpy as jnp
from jax import lax
from jax.experimental import pallas as pl
from jax.experimental.pallas import tpu as pltpu
from jax.sharding import PartitionSpec as P


LN_EPS = 1e-5
F32, BF16 = jnp.float32, jnp.bfloat16
ROWS, CH, COLS = 64, 64, 256
TILE = 16


def channel_stats(vals, axis_id):
    ch_mean = jnp.mean(vals, axis=axis_id, keepdims=True)
    ch_var = jnp.mean(jnp.square(vals - ch_mean), axis=axis_id, keepdims=True)
    return ch_mean, lax.rsqrt(ch_var + LN_EPS)


def channel_norm(vals, norm, stats=None):
    ch_mean, scale = channel_stats(vals, 0) if stats is None else stats
    return (vals - ch_mean) * scale * norm[0] + norm[1]


def sigmoid(vals):
    return 0.5 * jnp.tanh(0.5 * vals) + 0.5


def swap_major(vals):
    return jnp.swapaxes(vals, 0, 1)


def norm_of(norms, place):
    return norms[2 * place], norms[2 * place + 1]


def contract(lhs, rhs, axis_id):
    return lax.dot_general(lhs, rhs, (((axis_id,), (axis_id,)), ((), ())), preferred_element_type=F32)


def mm(lhs, rhs):
    return jnp.dot(lhs, rhs, preferred_element_type=F32)


def ab_row(proj, tile_a, tile_b, slot):
    for n, tile in enumerate((tile_a, tile_b)):
        linear, gate = jnp.split(proj[2 * CH * n:2 * CH * n + 2 * CH], 2)
        tile[slot] = ((jnp.tanh(gate) + 1.0) * linear).astype(BF16)


def x_norm_tile(x_s, tile_x, base, xg, xb):
    parts = [(sub, half) for sub in range(2) for half in range(2)]

    def load(c, part):
        return x_s[c, pl.ds(pl.multiple_of(base + 8 * part[0], 8), 8), 128 * part[1]:128 * part[1] + 128]

    means = [sum(load(c, p) for c in range(CH)) * (1.0 / CH) for p in parts]
    scales = [lax.rsqrt(sum(jnp.square(load(c, p) - means[n]) for c in range(CH)) * (1.0 / CH) + LN_EPS)
              for n, p in enumerate(parts)]
    for c in range(CH):
        rows = []
        for sub in range(2):
            rows.append(jnp.concatenate(
                [(load(c, (sub, half)) - means[2 * sub + half]) * scales[2 * sub + half] * xg[c] + xb[c]
                 for half in range(2)], axis=1))
        tile_x[c] = jnp.concatenate(rows).astype(BF16)


LAG = 3


def staggered(count, *stages):
    held = [{} for _ in stages]
    for tick in range(count + LAG * (len(stages) - 1)):
        for k, stage in enumerate(stages):
            i = tick - LAG * k
            if 0 <= i < count:
                held[k][i] = stage(i, held[k - 1].pop(i) if k else None)


def u_kernel(last, layout, sc, *refs):
    z_refs = refs[:len(layout)]
    n_far = 3 if last else 1
    (mask0, mask1, mask2, mask3, norms, xgs, w_ab, w_sq, w_bias, z2_own, z2_par, bias_out, far2, *far3) = refs[len(layout):][:13 + n_far]
    (z_s, a_s, b_s, x_s, mask, stats, tile_a, tile_b, tile_x, tile_c, tile_d, tile_z, in_sem, z_sem, x_sem) = refs[len(layout) + 13 + n_far:]
    me, sample = sc[0], sc[1]
    lanes = pl.ds(pl.multiple_of(LANES * (me // 2), LANES), LANES)
    out_norm = norm_of(norms, 0)
    in_norm = norm_of(norms, 1)
    att_norm = norm_of(norms, 2)
    n_tiles = COLS // TILE

    for ref, (r, start) in zip(z_refs, layout):
        src = ref if r else ref.at[sample]
        rows = pl.ds(pl.multiple_of(ROWS * (me ^ r) + start, 8), src.shape[0])
        pltpu.make_async_copy(src, z_s.at[rows], in_sem.at[r]).start()
    for r, part in enumerate((mask0, mask1, mask2, mask3)):
        mask[pl.ds(pl.multiple_of(ROWS * (me ^ r), ROWS), ROWS), :] = part[:].astype(F32)

    def mask_row(base, i):
        return mask[pl.ds(base + i, 1), :]

    def measure(base, i, vals=None):
        found = channel_stats(z_s[base + i] if vals is None else vals, 0)
        for n in range(2):
            stats[n if vals is None else n + 2, pl.ds(base + i, 1), :] = found[n]
        return found

    def recall(base, i, first):
        return [stats[first + n, pl.ds(base + i, 1), :] for n in range(2)]

    def flush(base):
        a_s[:, pl.ds(base, TILE), :] = swap_major(tile_a[:])
        b_s[:, pl.ds(base, TILE), :] = swap_major(tile_b[:])

    def export(t, start, outgoing, sem):
        r = (t * TILE // ROWS) ^ me
        q = t % (ROWS // TILE)
        rows = pl.ds(pl.multiple_of(TILE * q, TILE), TILE)
        half = pl.ds(pl.multiple_of(ROWS + TILE * (q % 2), TILE), TILE)
        side = pl.ds(pl.multiple_of(LANES * (q // 2), LANES), LANES)
        act = (lambda cp: cp.start()) if start else (lambda cp: cp.wait())
        wide, z_tile = tile_c.at[t % 2], tile_z.at[t % 2]
        narrow = tile_c.at[t % 2, :, :, lanes]
        jobs = [(r == 2, narrow, far2.at[half, :, side])] if outgoing else [
            (r == 0, z_tile, z2_own.at[rows]), (r == 1, z_tile, z2_par.at[rows]), (r == 2, wide, far2.at[rows])]
        if last:
            jobs += [((r == 3) & (q == 0), narrow, far3[1]) if outgoing else ((r == 3) & (q == 0), wide, far3[0])]
            if not outgoing:
                rest = pl.ds(pl.multiple_of(jnp.maximum(q - 1, 0) * TILE, TILE), TILE)
                jobs += [((r == 3) & (q > 0), z_tile, far3[2].at[rest])]
        else:
            jobs += [(r == 3, narrow, far3[0].at[half, :, side]) if outgoing else (r == 3, wide, far3[0].at[rows])]
        for when, src, dst in jobs:
            @pl.when(when)
            def _():
                act(pltpu.make_async_copy(src, dst, sem.at[t % 2]))

    @pl.loop(0, n_tiles)
    def _(v):
        r = v * TILE // ROWS

        @pl.when(v * TILE % ROWS == 0)
        def _():
            pltpu.make_async_copy(z_refs[0].at[sample], z_s.at[pl.ds(0, ROWS)], in_sem.at[r]).wait()

        base = pl.multiple_of(ROWS * (me ^ r) + v * TILE % ROWS, TILE)
        staggered(
            TILE,
            lambda i, _: mm(w_ab[0], (mask_row(base, i) * channel_norm(z_s[base + i], out_norm, measure(base, i))).astype(BF16)),
            lambda i, proj: ab_row(proj, tile_a, tile_b, i))
        flush(base)

    @pl.loop(0, CH, unroll=4)
    def _(c):
        x_s[c] = contract(a_s[c], b_s[c], 1)

    @pl.loop(0, n_tiles)
    def _(t):
        base = pl.multiple_of(TILE * t, TILE)

        @pl.when(t >= 2)
        def _():
            export(t - 2, False, True, x_sem)

        x_norm_tile(x_s, tile_x, base, xgs.at[0], xgs.at[1])
        tile_c[t % 2] = swap_major(tile_x[:])

        def gate_and_update(i, _):
            normed = channel_norm(z_s[base + i], out_norm, recall(base, i, 0)).astype(BF16)
            return mm(w_sq[0], normed), mm(w_sq[1], tile_c[t % 2, i])

        def next_norm(i, parts):
            z_one = z_s[base + i] + (jnp.tanh(parts[0]) + 1.0) * parts[1]
            tile_z[0, i] = z_one
            return (mask_row(base, i) * channel_norm(z_one, in_norm, measure(base, i, z_one))).astype(BF16)

        staggered(TILE, gate_and_update, next_norm, lambda i, normed: mm(w_ab[1], normed),
                  lambda i, proj: ab_row(proj, tile_a, tile_b, i))
        flush(base)
        z_s[pl.ds(base, TILE)] = tile_z[0]
        export(t, True, True, x_sem)

    for t in (n_tiles - 2, n_tiles - 1):
        export(t, False, True, x_sem)

    @pl.loop(0, CH, unroll=4)
    def _(c):
        x_s[c] = contract(a_s[c], b_s[c], 0)

    @pl.loop(0, n_tiles)
    def _(t):
        base = pl.multiple_of(TILE * t, TILE)

        @pl.when(t >= 2)
        def _():
            export(t - 2, False, False, z_sem)

        x_norm_tile(x_s, tile_x, base, xgs.at[2], xgs.at[3])
        tile_c[t % 2] = swap_major(tile_x[:])

        def gate_and_update(i, _):
            normed = channel_norm(z_s[base + i], in_norm, recall(base, i, 2)).astype(BF16)
            return mm(w_sq[2], normed), mm(w_sq[3], tile_c[t % 2, i])

        def next_norm(i, parts):
            z_two = z_s[base + i] + (jnp.tanh(parts[0]) + 1.0) * parts[1]
            tile_z[t % 2, i] = z_two
            return channel_norm(z_two, att_norm).astype(BF16)

        def bias_row(i, normed):
            tile_d[i] = mm(w_bias[:], normed)

        staggered(TILE, gate_and_update, next_norm, bias_row)
        rows = pl.ds(pl.multiple_of(t * TILE % ROWS, TILE), TILE)
        bias_out[t * TILE // ROWS, :, rows, :] = swap_major(tile_d[:])[:4].astype(BF16)
        export(t, True, False, z_sem)

    bias_to = ((far2, 0, 0), (far2, 1, 1), (far2, 3, 2)) if last else ((far2, 0, 0), (far3[0], 1, 0))

    def bias_copy(n):
        dst, block, place = bias_to[n]
        return pltpu.make_async_copy(bias_out.at[me ^ block], dst.at[pl.ds(FAR_BIAS + 4 * place, 4)], in_sem.at[n])

    for n in range(len(bias_to)):
        bias_copy(n).start()
    for t in (n_tiles - 2, n_tiles - 1):
        export(t, False, False, z_sem)
    for n in range(len(bias_to)):
        bias_copy(n).wait()


LANES = 128
VM = pl.BlockSpec(memory_space=pltpu.VMEM)
HB = pl.BlockSpec(memory_space=pl.ANY)
SDS = jax.ShapeDtypeStruct
AT_FIRST = lambda i, *_: (i, 0, 0, 0)
SM = pl.BlockSpec(memory_space=pltpu.SMEM)
PARAMS = pltpu.CompilerParams(vmem_limit_bytes=40 << 20, dimension_semantics=("arbitrary",))
AB_TILE = pltpu.VMEM((TILE, CH, COLS), BF16)
DMA2 = pltpu.SemaphoreType.DMA((2,))
FAR_BIAS = ROWS + ROWS // 2
FAR = SDS((FAR_BIAS + 4, CH, COLS), BF16)
TILE_FULL = SDS((TILE, CH, COLS), BF16)
TILE_HALF = SDS((TILE, CH, LANES), BF16)
AWAY = SDS((ROWS - TILE, CH, COLS), F32)
FAR_LAST = SDS((FAR_BIAS + 12, CH, COLS), BF16)
ROW_WIDE = SDS((ROWS, CH, COLS), F32)
SAMPLE_BF = pltpu.VMEM((CH, COLS, COLS), BF16)


def u_call(last, layout, sc, z_parts, masks, norms, xgs, w_ab, w_sq, w_bias):
    return pl.pallas_call(
        functools.partial(u_kernel, last, layout),
        out_shape=(ROW_WIDE, ROW_WIDE, SDS((4, 4, ROWS, COLS), BF16), *((FAR_LAST, TILE_FULL, TILE_HALF, AWAY) if last else (FAR, FAR))),
        in_specs=[SM] + [HB] * len(layout) + [VM] * 9,
        out_specs=(HB, HB, VM) + (HB,) * (4 if last else 2),
        scratch_shapes=[
            pltpu.VMEM((COLS, CH, COLS), F32), SAMPLE_BF, SAMPLE_BF,
            pltpu.VMEM((CH, COLS, COLS), F32), pltpu.VMEM((COLS, COLS), F32), pltpu.VMEM((4, COLS, COLS), F32), AB_TILE, AB_TILE, pltpu.VMEM((CH, TILE, COLS), BF16), pltpu.VMEM((2, TILE, CH, COLS), BF16),
            pltpu.VMEM((TILE, 8, COLS), F32), pltpu.VMEM((2, TILE, CH, COLS), F32),
            pltpu.SemaphoreType.DMA((4,)), DMA2, DMA2,
        ],
        compiler_params=pltpu.CompilerParams(vmem_limit_bytes=62 << 20),
        name="pair_updates",
    )(sc, *z_parts, *masks, norms, xgs, w_ab, w_sq, w_bias)


def l1_kernel(ids, z_in, mask_in, norms, w_ab, a_out, b_out, mask, tile_a, tile_b):
    out_norm = norm_of(norms, 0)
    mask[:] = mask_in[0].astype(F32)

    @pl.loop(0, ROWS // TILE)
    def _(t):
        base = pl.multiple_of(TILE * t, TILE)
        staggered(
            TILE,
            lambda i, _: mm(w_ab[0], (mask[pl.ds(base + i, 1), :] * channel_norm(z_in[0, base + i], out_norm)).astype(BF16)),
            lambda i, proj: ab_row(proj, tile_a, tile_b, i))
        a_out[0, :, pl.ds(base, TILE), :] = swap_major(tile_a[:])
        b_out[0, :, pl.ds(base, TILE), :] = swap_major(tile_b[:])


def l1_call(ids, zt, mask, norms, w_ab):
    n = ids.shape[0]
    ab = SDS((n, CH, ROWS, COLS), BF16)
    ab_spec = pl.BlockSpec((1, CH, ROWS, COLS), AT_FIRST)
    return pl.pallas_call(
        l1_kernel,
        out_shape=(ab, ab),
        grid_spec=pltpu.PrefetchScalarGridSpec(
            num_scalar_prefetch=1, grid=(n,),
            in_specs=[pl.BlockSpec((1, ROWS, CH, COLS), lambda i, ids: (ids[i], 0, 0, 0)),
                      pl.BlockSpec((1, ROWS, COLS), lambda i, ids: (ids[i], 0, 0)), VM, VM],
            out_specs=(ab_spec, ab_spec),
            scratch_shapes=[pltpu.VMEM((ROWS, COLS), F32), AB_TILE, AB_TILE]),
        compiler_params=PARAMS,
        name="near_projections",
    )(ids, zt, mask, norms, w_ab)


def l2_kernel(sc, a_in, b_own, b_par, xgs, x_out, x_s, tile_x):
    odd = sc[0] % 2 == 1

    @pl.loop(0, CH, unroll=2)
    def _(c):
        for n in range(2):
            own, par = b_own[n, c].astype(F32), b_par[1 - n, c].astype(F32)
            pair = jnp.concatenate([jnp.where(odd, par, own), jnp.where(odd, own, par)]).astype(BF16)
            x_s[c, :, LANES * n:LANES * n + LANES] = contract(a_in[n, c], pair, 1)

    @pl.loop(0, ROWS // TILE)
    def _(t):
        base = pl.multiple_of(TILE * t, TILE)
        x_norm_tile(x_s, tile_x, base, xgs.at[0], xgs.at[1])
        both = swap_major(tile_x[:])
        for n in range(2):
            x_out[n, pl.ds(base, TILE)] = both[:, :, LANES * n:LANES * n + LANES]


def l2_call(sc, a_all, b_own, b_par, xgs):
    n = a_all.shape[0]
    ab_spec = pl.BlockSpec((2, CH, ROWS, COLS), AT_FIRST)
    return pl.pallas_call(
        l2_kernel,
        grid=(n // 2,),
        out_shape=SDS((n, ROWS, CH, LANES), BF16),
        in_specs=[SM, ab_spec, ab_spec, ab_spec, VM],
        out_specs=pl.BlockSpec((2, ROWS, CH, LANES), AT_FIRST),
        scratch_shapes=[pltpu.VMEM((CH, ROWS, COLS), F32), pltpu.VMEM((CH, TILE, COLS), BF16)],
        compiler_params=PARAMS,
        name="near_product",
    )(sc, a_all, b_own, b_par, xgs)


def r_kernel(sc, z_in, x_near, x_far, xi, norms, w_sq, w_bias, z_out, bias_out, tile_d):
    first = sc[0] < 2
    out_norm = norm_of(norms, 0)
    in_norm = norm_of(norms, 1)
    att_norm = norm_of(norms, 2)

    def outgoing(i, _):
        near, far = x_near[0, i].astype(F32), x_far[i].astype(F32)
        xn = jnp.concatenate([jnp.where(first, near, far), jnp.where(first, far, near)], axis=1).astype(BF16)
        normed = channel_norm(z_in[0, i], out_norm).astype(BF16)
        return mm(w_sq[0], normed), mm(w_sq[1], xn)

    def norm_one(i, parts):
        z_one = z_in[0, i] + (jnp.tanh(parts[0]) + 1.0) * parts[1]
        z_out[i] = z_one
        return channel_norm(z_one, in_norm).astype(BF16)

    def incoming(i, normed):
        return mm(w_sq[2], normed), mm(w_sq[3], xi[i])

    def norm_two(i, parts):
        z_two = z_out[i] + (jnp.tanh(parts[0]) + 1.0) * parts[1]
        z_out[i] = z_two
        return channel_norm(z_two, att_norm).astype(BF16)

    def bias_row(i, normed):
        tile_d[i] = mm(w_bias[:], normed)

    staggered(TILE, outgoing, norm_one, incoming, norm_two, bias_row)
    bias_out[:] = swap_major(tile_d[:])[:4].astype(BF16)


def r_call(sc, zt, x_near, x_far, xi, norms, w_sq, w_bias):
    steps = 1 if x_far.shape[0] == TILE else ROWS // TILE
    far_map = (lambda i, sc: (i, 0, 0)) if steps == 1 else (lambda i, sc: (ROWS // TILE + i % 2, 0, i // 2))
    row_map = lambda i, sc: (i, 0, 0)
    return pl.pallas_call(
        r_kernel,
        out_shape=(SDS((steps * TILE, CH, COLS), F32), SDS((4, steps * TILE, COLS), BF16)),
        grid_spec=pltpu.PrefetchScalarGridSpec(
            num_scalar_prefetch=1, grid=(steps,),
            in_specs=[pl.BlockSpec((1, TILE, CH, COLS), lambda i, sc: (sc[1], i, 0, 0)),
                      pl.BlockSpec((1, TILE, CH, LANES), lambda i, sc: (sc[2], i, 0, 0)),
                      pl.BlockSpec((TILE, CH, LANES), far_map), pl.BlockSpec((TILE, CH, COLS), row_map), VM, VM, VM],
            out_specs=(pl.BlockSpec((TILE, CH, COLS), row_map), pl.BlockSpec((4, TILE, COLS), lambda i, sc: (0, i, 0))),
            scratch_shapes=[pltpu.VMEM((TILE, 8, COLS), F32)]),
        compiler_params=PARAMS,
        name="row_updates",
    )(sc, zt, x_near, x_far, xi, norms, w_sq, w_bias)


HEADS, HEAD = 4, 16
MASK_FILL = -1e9
CHUNK = 32
SLOTS = 2
STEPS = 6
AWAY_FIRST = 32


def attention_kernel(sizes, fresh, away, sc, *refs):
    n = len(sizes)
    z_refs, bias_refs = refs[:n], refs[n:2 * n]
    mask_in, norms, w_all, w_proj = refs[2 * n:2 * n + 4]
    rest = refs[2 * n + 4 + away + (not fresh):]
    mask_away, out_away = refs[2 * n + 4], rest[1:1 + 2 * away]
    (out, z_in, z_out, mask_i, mask, bias_rows, bias_t, q_s, k_s, v_s, g_s, vn_s, gn_s, keep_s, s_buf, e_buf, p_s,
     top_s, inv_s, o_s, m_sem, z_sem, o_sem) = rest[:1] + rest[1 + 2 * away:]
    n_rows = sum(sizes)

    def z_copy(j):
        return pltpu.make_async_copy(z_refs[j], z_in.at[pl.ds(ROWS * j, sizes[j])], z_sem.at[j])

    def m_copy(j):
        src = mask_away.at[0] if away and j == n - 1 else mask_in.at[sc[j], pl.ds(0, sizes[j])]
        return pltpu.make_async_copy(src, mask_i.at[pl.ds(ROWS * j, sizes[j])], m_sem.at[j])

    def o_copy(j):
        return pltpu.make_async_copy(z_out.at[pl.ds(ROWS * j, sizes[j])], out.at[sc[j], pl.ds(0, sizes[j])], o_sem.at[j])

    def o_copies(j):
        if not (away and j == n - 1):
            return [o_copy(j)]
        return [pltpu.make_async_copy(z_out.at[pl.ds(ROWS * j + start, ref.shape[0])], ref, o_sem.at[j])
                for ref, start in zip(out_away, (0, AWAY_FIRST))]

    for j in range(n):
        m_copy(j).start()
        z_copy(j).start()
    for j in range(n):
        for r in range(4):
            bias_rows[j, :, pl.ds(pl.multiple_of(ROWS * (sc[n + j] ^ r), ROWS), ROWS), :] = bias_refs[j][r].astype(F32)
    for j in range(n):
        m_copy(j).wait()
    z_copy(0).wait()
    mask[:] = mask_i[:].astype(F32)
    q_s[:] = jnp.zeros_like(q_s)

    @pl.loop(0, n * HEADS)
    def _(h):
        bias_t[h // HEADS, h % HEADS] = bias_rows[h // HEADS, h % HEADS].T

    def project(row, slot):
        row = jnp.minimum(row, n_rows - 1)
        normed = channel_norm(z_in[row], norm_of(norms, 0)).astype(BF16)
        proj = mm(w_all[:], normed)
        k_s[slot] = proj[CH:2 * CH].T.astype(BF16)
        q = proj[:CH].astype(BF16)
        for h in range(HEADS):
            q_s[slot, h, HEAD * h:HEAD * h + HEAD] = q[HEAD * h:HEAD * h + HEAD]
        vn_s[slot] = proj[2 * CH:3 * CH].astype(BF16)
        gn_s[slot] = sigmoid(proj[3 * CH:])

    def keep_mask(row, slot):
        row = jnp.minimum(row, n_rows - 1)
        keep_s[slot] = jnp.broadcast_to(mask[pl.ds(row, 1), :], (LANES, COLS)).T

    def tall(line):
        return jnp.concatenate([line] * (CHUNK // 8))

    def fold(part, op):
        out = part[:8]
        for n in range(1, part.shape[0] // 8):
            out = op(out, part[8 * n:8 * n + 8])
        return out

    def scores(slot, h):
        return mm(k_s[slot], q_s[slot, h])

    def weigh(slot, h, probs):
        heads = slice(HEAD * h, HEAD * h + HEAD)
        o_s[slot, heads] = mm(v_s[slot, heads], probs)

    def step(row, slot, h, logits, defer):
        buf, prev = h % 2, (h + 1) % 2
        sample = jnp.clip(row, 0, n_rows - 1) // ROWS
        top, total, probs = None, None, []
        for c in range(COLS // CHUNK):
            rows = slice(CHUNK * c, CHUNK * c + CHUNK)
            probs.append((e_buf[buf, rows] * tall(inv_s[buf])).astype(BF16))
            exps = jnp.exp(s_buf[prev, rows] - tall(top_s[prev]))
            e_buf[prev, rows] = exps
            part = fold(exps, jnp.add)
            total = part if total is None else total + part
            keep = keep_s[slot, rows]
            keep = jnp.concatenate([keep, keep], axis=1) > 0
            vals = jnp.where(keep, logits[rows] + bias_t[sample, h, rows], MASK_FILL)
            s_buf[buf, rows] = vals
            part = fold(vals, jnp.maximum)
            top = part if top is None else jnp.maximum(top, part)
        top_s[buf] = jnp.broadcast_to(jnp.max(top, axis=0, keepdims=True), (8, COLS))
        inv_s[prev] = jnp.broadcast_to(1.0 / jnp.sum(total, axis=0, keepdims=True), (8, COLS))
        if defer:
            p_s[:] = jnp.concatenate(probs)
        else:
            weigh(1 - slot if h < 2 else slot, (h - 2) % HEADS, jnp.concatenate(probs))

    def finish(row, slot):
        gated = (g_s[slot] * o_s[slot]).astype(BF16)
        z_out[jnp.maximum(row, 0)] = z_in[jnp.clip(row, 0, n_rows - 1)] + mm(w_proj[:], gated)

    project(0, 0)
    keep_mask(0, 0)
    n_steps = (n_rows + 2 + STEPS - 1) // STEPS

    @pl.loop(0, n_steps)
    def _(it):
        first = STEPS * it - 1
        lg = scores(1, 0)
        weigh(0, 1, p_s[:])
        for k in range(STEPS):
            row, slot, last = first + k, 1 - k % 2, k == STEPS - 1
            for h in range(HEADS):
                nxt = scores(slot, h + 1) if h < HEADS - 1 else (None if last else scores(1 - slot, 0))
                if h == 2:
                    project(row + 2, slot)
                step(row, slot, h, lg, last and h == HEADS - 1)
                lg = nxt
                if h == 3:
                    finish(row - 1, 1 - slot)
                    v_s[1 - slot] = vn_s[1 - slot]
                    g_s[1 - slot] = gn_s[1 - slot]
            keep_mask(row + 2, slot)
        for j in range(1, n):
            @pl.when(it == (ROWS * j - 1) // STEPS - 1)
            def _():
                z_copy(j).wait()

            @pl.when(it == (ROWS * j + 1) // STEPS)
            def _():
                o_copy(j - 1).start()

    for copy in o_copies(n - 1):
        copy.start()
    for j in range(n):
        for copy in o_copies(j):
            copy.wait()


def attend(sc, z_parts, biases, mask, norms, w_all, w_proj, out, mask_away=None):
    n, fresh, away = len(z_parts), out is None, mask_away is not None
    sizes = tuple(z.shape[0] for z in z_parts)
    args = (sc, *z_parts, *biases, mask, norms, w_all, w_proj) + ((mask_away,) if away else ()) + (() if fresh else (out,))
    whole = SDS((mask.shape[0], ROWS, CH, COLS), F32)
    aways = [SDS((k, CH, COLS), F32) for k in (AWAY_FIRST, AWAY.shape[0] - AWAY_FIRST)]
    rows = sum(sizes)
    pair = pltpu.VMEM((SLOTS, CH, COLS), BF16)
    wide = pltpu.VMEM((SLOTS, CH, COLS), F32)
    square = pltpu.VMEM((SLOTS, COLS, COLS), F32)
    each = pltpu.VMEM((n, HEADS, COLS, COLS), F32)
    line = pltpu.VMEM((SLOTS, 8, COLS), F32)
    sems = pltpu.SemaphoreType.DMA((n,))
    return pl.pallas_call(
        functools.partial(attention_kernel, sizes, fresh, away),
        out_shape=(whole, *aways) if away else whole,
        in_specs=[SM] + [HB] * n + [VM] * n + [HB] + [VM] * 3 + [HB] * (away + (not fresh)),
        out_specs=(HB, HB, HB) if away else HB,
        scratch_shapes=[
            pltpu.VMEM((rows, CH, COLS), F32), pltpu.VMEM((rows + STEPS, CH, COLS), F32), pltpu.VMEM((rows, COLS), jnp.int32),
            pltpu.VMEM((rows, COLS), F32), each, each, pltpu.VMEM((SLOTS, HEADS, CH, COLS), BF16),
            pltpu.VMEM((SLOTS, COLS, CH), BF16), pair, wide, pair, wide, pltpu.VMEM((SLOTS, COLS, LANES), F32),
            square, square, pltpu.VMEM((COLS, COLS), BF16), line, line, wide, sems, sems, sems,
        ],
        compiler_params=pltpu.CompilerParams(vmem_limit_bytes=48 << 20),
        input_output_aliases={} if fresh else {len(args) - 1: 0},
        name="triangle_attention",
    )(*args)


FIRST = 8


def exchange(values, r):
    return lax.ppermute(values, 'dap', [(i, i ^ r) for i in range(4)])


def update_weights(params):
    norm_gain, norm_bias, w_a, w_agate, w_b, w_bgate, w_gate, x_gain, x_bias, w_proj = params
    half = jnp.bfloat16(0.5)
    wide = lambda v: jnp.broadcast_to(v[:, None], (CH, COLS))
    deep = lambda v: jnp.broadcast_to(v[:, None, None], (CH, 8, 128))
    return ([wide(norm_gain), wide(norm_bias)], [deep(x_gain), deep(x_bias)],
            half * jnp.concatenate([w_a.T, w_agate.T, w_b.T, w_bgate.T]), [half * w_gate.T, half * w_proj.T])


def solution(mesh):
    def local_block(pair_z, pair_mask, *weights):
        me = lax.axis_index('dap')
        zt = jnp.transpose(pair_z, (0, 1, 3, 2))
        n_own = zt.shape[0] // 4
        mask_bf = pair_mask.astype(BF16)
        arrived, layouts, before = [], [], ()
        for t in range(n_own):
            pieces = [(2, 0, FIRST), (2, FIRST, ROWS)] if t == 0 else [(2, 0, ROWS)]
            pieces += [(3, 0, ROWS), (1, 0, ROWS)]
            got = []
            for r, start, stop in pieces:
                where = (n_own * (me ^ r) + t, start, 0, 0)
                send = lax.dynamic_slice(lax.optimization_barrier((zt, *before))[0], where, (1, stop - start, CH, COLS))[0]
                if t == 0 or r == 1:
                    before = (send,)
                got.append(exchange(send, r))
                if t == 0 and stop == ROWS and r == 2:
                    mask_bf, weights = lax.optimization_barrier((mask_bf, weights, send))[:2]
                    masks = [lax.dynamic_slice_in_dim(mask_bf, n_own * (me ^ k), n_own) for k in range(4)]
                    before = (*before, *masks)
                    masks = [exchange(m, k) if k else m for k, m in enumerate(masks)]
            arrived.append([zt, *got])
            layouts.append(((0, 0), *((r, start) for r, start, _ in pieces)))

        out_n, out_x, out_ab, out_sq = update_weights(weights[:10])
        in_n, in_x, in_ab, in_sq = update_weights(weights[10:20])
        att_gain, att_shift, w_q, w_k, w_v, w_bias, w_gate, w_proj = weights[20:]
        att_n = [jnp.broadcast_to(v[:, None], (CH, COLS)) for v in (att_gain, att_shift)]
        norms = jnp.stack(out_n + in_n + att_n)
        xgs = jnp.stack(out_x + in_x)
        w_ab = jnp.stack([out_ab, in_ab])
        w_sq = jnp.stack(out_sq + in_sq)
        w_bias8 = jnp.concatenate([w_bias.T, jnp.zeros((4, CH), BF16)])
        w_all = jnp.concatenate([w_q.T * jnp.bfloat16(HEAD ** -0.5), w_k.T, w_v.T, w_gate.T])
        w_out = w_proj.T
        att_norms = norms[4:]

        token = [None]

        def ordered(call, sc, *args):
            sc = jnp.stack([jnp.asarray(v, jnp.int32) for v in sc])
            if token[0] is not None:
                sc = lax.optimization_barrier((sc, token[0]))[0]
            res = call(sc, *args)
            token[0] = jax.tree.leaves(res)[-1]
            return res

        def attention(jobs, out, mask_away=None):
            samples, orders, z_parts, biases = zip(*jobs)
            return ordered(attend, samples + orders, z_parts, biases, pair_mask, att_norms, w_all, w_out, out, mask_away)

        far = [(t, r) for t in range(n_own) for r in (2, 3)]
        a_far, b_far = ordered(l1_call, [n_own * (me ^ r) + t for t, r in far], zt, pair_mask, norms, w_ab)
        b_par = exchange(b_far, 1)
        x_near = ordered(l2_call, [me], a_far, b_far, b_par, xgs)

        out = None
        held = []
        for t in range(n_own):
            last = t == n_own - 1
            z_own, z_par, bias, far2, *far3 = ordered(functools.partial(u_call, last, layouts[t]), [me, n_own * me + t],
                                                      arrived[t], [m[t] for m in masks], norms, xgs, w_ab, w_sq, w_bias8)
            near = (n_own * (me ^ 1) + t, 0, exchange(z_par, 1), exchange(bias, 1))
            own = (n_own * me + t, 0, z_own, bias)
            three = [exchange(v, 3) for v in (far3[:2] if last else far3)]
            two = exchange(far2, 2)
            held.append({2: (two, two), 3: (three[-1], three[0])})
            if last:
                out, *away = attention([own, (0, 0, far3[2], bias)], out, masks[3][t][None, TILE:].astype(jnp.int32))
                away = [exchange(v, 3) for v in away]
            else:
                out = attention([own, near], out)
        for t in range(n_own):
            last = t == n_own - 1
            mine, z_two = {}, {}
            for r in (2, 3):
                z_two[r], bias_own = ordered(r_call, [me, n_own * (me ^ r) + t, far.index((t, r))], zt, x_near,
                                             *held[t][r], norms, w_sq, w_bias8)
                mine[r] = [bias_own, *jnp.split(held[t][r][0][FAR_BIAS:], 3 if last else 1)]
            par = exchange(jnp.stack(mine[2] + ([] if last else mine[3])), 1)
            if last:
                blocks = {2: [mine[2][k] for k in (0, 3, 1, 2)], 3: [par[k] for k in (3, 0, 2, 1)]}
            else:
                blocks = {2: [mine[2][0], par[2], mine[2][1], par[3]], 3: [mine[3][0], par[0], mine[3][1], par[1]]}
            out = attention(([] if t else [near]) + [
                (n_own * (me ^ r) + t, me, z_two[r], jnp.stack(blocks[r])) for r in (2, 3)], out)
        for v, start in zip(away, (TILE, TILE + AWAY_FIRST)):
            out = lax.dynamic_update_slice(out, v[None], (n_own * (me ^ 3) + n_own - 1, start, 0, 0))
        return jnp.transpose(out, (0, 1, 3, 2))

    pair_spec = P('data', 'dap')
    return jax.shard_map(local_block, mesh=mesh, in_specs=(pair_spec, pair_spec) + (P(),) * 28,
                         out_specs=pair_spec, check_vma=False)
```

```python
import functools

import jax
import jax.numpy as jnp
from jax import lax
from jax.experimental import pallas as pl
from jax.experimental.pallas import tpu as pltpu
from jax.sharding import PartitionSpec as P


LN_EPS = 1e-5
F32, BF16 = jnp.float32, jnp.bfloat16
ROWS, CH, COLS = 64, 64, 256
TILE = 16
MIB = 1 << 20
OUT, IN, ATT = range(3)


def channel_stats(vals):
    ch_mean = jnp.mean(vals, axis=0, keepdims=True)
    ch_var = jnp.mean(jnp.square(vals - ch_mean), axis=0, keepdims=True)
    return ch_mean, lax.rsqrt(ch_var + LN_EPS)


def channel_norm(vals, norm, stats=None):
    gain, shift = norm
    ch_mean, scale = channel_stats(vals) if stats is None else stats
    return (vals - ch_mean) * scale * gain + shift


def sigmoid(vals):
    return 0.5 * jnp.tanh(0.5 * vals) + 0.5


def swap_major(vals):
    return jnp.swapaxes(vals, 0, 1)


def pair_of(ref, place):
    return ref.at[2 * place], ref.at[2 * place + 1]


def norm_of(ref, place):
    return [part[:] for part in pair_of(ref, place)]


def contract(lhs, rhs, axis_id):
    return lax.dot_general(lhs, rhs, (((axis_id,), (axis_id,)), ((), ())), preferred_element_type=F32)


def mm(lhs, rhs):
    return jnp.dot(lhs, rhs, preferred_element_type=F32)


def opened(gate, product):
    return (jnp.tanh(gate) + 1.0) * product


def row_at(base, i):
    return pl.ds(base + i, 1)


def ab_row(proj, tile_a, tile_b, slot):
    for n, tile in enumerate((tile_a, tile_b)):
        linear, gate = jnp.split(proj[2 * CH * n:2 * CH * n + 2 * CH], 2)
        tile[slot] = opened(gate, linear).astype(BF16)


def x_norm_tile(x_s, tile_x, base, xg, xb):
    parts = [(sub, half) for sub in range(2) for half in range(2)]

    def load(c, part):
        return x_s[c, pl.ds(pl.multiple_of(base + 8 * part[0], 8), 8), 128 * part[1]:128 * part[1] + 128]

    means = [sum(load(c, p) for c in range(CH)) * (1.0 / CH) for p in parts]
    scales = [lax.rsqrt(sum(jnp.square(load(c, p) - means[n]) for c in range(CH)) * (1.0 / CH) + LN_EPS)
              for n, p in enumerate(parts)]
    for c in range(CH):
        rows = []
        for sub in range(2):
            rows.append(jnp.concatenate(
                [(load(c, (sub, half)) - means[2 * sub + half]) * scales[2 * sub + half] * xg[c] + xb[c]
                 for half in range(2)], axis=1))
        tile_x[c] = jnp.concatenate(rows).astype(BF16)


LAG = 3


def staggered(count, *stages):
    held = [{} for _ in stages]
    for tick in range(count + LAG * (len(stages) - 1)):
        for k, stage in enumerate(stages):
            i = tick - LAG * k
            if 0 <= i < count:
                held[k][i] = stage(i, held[k - 1].pop(i) if k else None)


def u_kernel(last, layout, sc, *refs):
    z_refs = refs[:len(layout)]
    n_far = 2 * CHUNKS + 1 if last else 1
    (mask0, mask1, mask2, mask3, norms, xgs, w_ab, w_sq, w_bias, z2_own, z2_par, bias_out, far2, *far3) = refs[len(layout):][:13 + n_far]
    (z_s, a_s, b_s, x_s, mask, stats, tile_a, tile_b, tile_x, tile_c, tile_d, tile_z, in_sem, z_sem, x_sem) = refs[len(layout) + 13 + n_far:]
    me, sample = sc[0], sc[1]
    lanes = pl.ds(pl.multiple_of(LANES * (me // 2), LANES), LANES)
    out_norm = norm_of(norms, OUT)
    in_norm = norm_of(norms, IN)
    att_norm = norm_of(norms, ATT)
    n_tiles = COLS // TILE

    for ref, (r, start) in zip(z_refs, layout):
        src = ref if r else ref.at[sample]
        rows = pl.ds(pl.multiple_of(ROWS * (me ^ r) + start, 8), src.shape[0])
        pltpu.make_async_copy(src, z_s.at[rows], in_sem.at[r]).start()
    for r, part in enumerate((mask0, mask1, mask2, mask3)):
        mask[pl.ds(pl.multiple_of(ROWS * (me ^ r), ROWS), ROWS), :] = part[:].astype(F32)

    def gate_and_product(place, normed, product):
        gate, proj = pair_of(w_sq, place)
        return mm(gate[:], normed), mm(proj[:], product)

    def mask_row(base, i):
        return mask[row_at(base, i), :]

    def measure(base, i, vals=None):
        found = channel_stats(z_s[base + i] if vals is None else vals)
        for n in range(2):
            stats[n if vals is None else n + 2, row_at(base, i), :] = found[n]
        return found

    def recall(base, i, first):
        return [stats[first + n, row_at(base, i), :] for n in range(2)]

    def flush(base):
        a_s[:, pl.ds(base, TILE), :] = swap_major(tile_a[:])
        b_s[:, pl.ds(base, TILE), :] = swap_major(tile_b[:])

    def export(t, start, outgoing, sem):
        r = (t * TILE // ROWS) ^ me
        q = t % (ROWS // TILE)
        rows = pl.ds(pl.multiple_of(TILE * q, TILE), TILE)
        half = pl.ds(pl.multiple_of(ROWS + TILE * (q % 2), TILE), TILE)
        side = pl.ds(pl.multiple_of(LANES * (q // 2), LANES), LANES)
        act = (lambda cp: cp.start()) if start else (lambda cp: cp.wait())
        wide, z_tile = tile_c.at[t % 2], tile_z.at[t % 2]
        narrow = tile_c.at[t % 2, :, :, lanes]
        jobs = [(r == 2, narrow, far2.at[half, :, side])] if outgoing else [
            (r == 0, z_tile, z2_own.at[rows]), (r == 1, z_tile, z2_par.at[rows]), (r == 2, wide, far2.at[rows])]
        if last:
            for n in range(CHUNKS):
                jobs += [((r == 3) & (q == n), narrow, far3[2 * n + 1]) if outgoing else ((r == 3) & (q == n), wide, far3[2 * n])]
            if not outgoing:
                rest = pl.ds(pl.multiple_of(jnp.maximum(q - CHUNKS, 0) * TILE, TILE), TILE)
                jobs += [((r == 3) & (q >= CHUNKS), z_tile, far3[-1].at[rest])]
        else:
            jobs += [(r == 3, narrow, far3[0].at[half, :, side]) if outgoing else (r == 3, wide, far3[0].at[rows])]
        for when, src, dst in jobs:
            @pl.when(when)
            def _():
                act(pltpu.make_async_copy(src, dst, sem.at[t % 2]))

    @pl.loop(0, n_tiles)
    def _(v):
        r = v * TILE // ROWS

        @pl.when(v * TILE % ROWS == 0)
        def _():
            pltpu.make_async_copy(z_refs[0].at[sample], z_s.at[pl.ds(0, ROWS)], in_sem.at[r]).wait()

        base = pl.multiple_of(ROWS * (me ^ r) + v * TILE % ROWS, TILE)
        staggered(
            TILE,
            lambda i, _: mm(w_ab[OUT], (mask_row(base, i) * channel_norm(z_s[base + i], out_norm, measure(base, i))).astype(BF16)),
            lambda i, proj: ab_row(proj, tile_a, tile_b, i))
        flush(base)

    @pl.loop(0, CH, unroll=16)
    def _(c):
        x_s[c] = contract(a_s[c], b_s[c], 1)

    @pl.loop(0, n_tiles)
    def _(t):
        base = pl.multiple_of(TILE * t, TILE)

        @pl.when(t >= 2)
        def _():
            export(t - 2, False, True, x_sem)

        x_norm_tile(x_s, tile_x, base, *pair_of(xgs, OUT))
        tile_c[t % 2] = swap_major(tile_x[:])

        def gate_and_update(i, _):
            normed = channel_norm(z_s[base + i], out_norm, recall(base, i, 0)).astype(BF16)
            return gate_and_product(OUT, normed, tile_c[t % 2, i])

        def next_norm(i, parts):
            z_one = z_s[base + i] + opened(*parts)
            tile_z[0, i] = z_one
            return (mask_row(base, i) * channel_norm(z_one, in_norm, measure(base, i, z_one))).astype(BF16)

        staggered(TILE, gate_and_update, next_norm, lambda i, normed: mm(w_ab[IN], normed),
                  lambda i, proj: ab_row(proj, tile_a, tile_b, i))
        flush(base)
        z_s[pl.ds(base, TILE)] = tile_z[0]
        export(t, True, True, x_sem)

    for t in (n_tiles - 2, n_tiles - 1):
        export(t, False, True, x_sem)

    @pl.loop(0, CH, unroll=16)
    def _(c):
        x_s[c] = contract(a_s[c], b_s[c], 0)

    @pl.loop(0, n_tiles)
    def _(t):
        base = pl.multiple_of(TILE * t, TILE)

        @pl.when(t >= 2)
        def _():
            export(t - 2, False, False, z_sem)

        x_norm_tile(x_s, tile_x, base, *pair_of(xgs, IN))
        tile_c[t % 2] = swap_major(tile_x[:])

        def gate_and_update(i, _):
            normed = channel_norm(z_s[base + i], in_norm, recall(base, i, 2)).astype(BF16)
            return gate_and_product(IN, normed, tile_c[t % 2, i])

        def next_norm(i, parts):
            z_two = z_s[base + i] + opened(*parts)
            tile_z[t % 2, i] = z_two
            return channel_norm(z_two, att_norm).astype(BF16)

        def bias_row(i, normed):
            tile_d[i] = mm(w_bias[:], normed)

        staggered(TILE, gate_and_update, next_norm, bias_row)
        rows = pl.ds(pl.multiple_of(t * TILE % ROWS, TILE), TILE)
        bias_out[t * TILE // ROWS, :, rows, :] = swap_major(tile_d[:])[:4].astype(BF16)
        export(t, True, False, z_sem)

    bias_to = ((far2, 0, 0), (far2, 1, 1), (far2, 3, 2)) if last else ((far2, 0, 0), (far3[0], 1, 0))

    def bias_copy(n):
        dst, block, place = bias_to[n]
        return pltpu.make_async_copy(bias_out.at[me ^ block], dst.at[pl.ds(FAR_BIAS + 4 * place, 4)], in_sem.at[n])

    for n in range(len(bias_to)):
        bias_copy(n).start()
    for t in (n_tiles - 2, n_tiles - 1):
        export(t, False, False, z_sem)
    for n in range(len(bias_to)):
        bias_copy(n).wait()


LANES = 128
VM = pl.BlockSpec(memory_space=pltpu.VMEM)
HB = pl.BlockSpec(memory_space=pltpu.HBM)
SDS = jax.ShapeDtypeStruct
AT_FIRST = lambda i, *_: (i, 0, 0, 0)
SM = pl.BlockSpec(memory_space=pltpu.SMEM)
PARAMS = pltpu.CompilerParams(vmem_limit_bytes=40 * MIB, dimension_semantics=("arbitrary",))
AB_TILE = pltpu.VMEM((TILE, CH, COLS), BF16)
DMA2 = pltpu.SemaphoreType.DMA((2,))
FAR_BIAS = ROWS + ROWS // 2
FAR = SDS((FAR_BIAS + 4, CH, COLS), BF16)
TILE_FULL = SDS((TILE, CH, COLS), BF16)
TILE_HALF = SDS((TILE, CH, LANES), BF16)
CHUNKS = 2
AWAY = SDS((ROWS - CHUNKS * TILE, CH, COLS), F32)
FAR_LAST = SDS((FAR_BIAS + 12, CH, COLS), BF16)
ROW_WIDE = SDS((ROWS, CH, COLS), F32)
SAMPLE_BF = pltpu.VMEM((CH, COLS, COLS), BF16)


def u_call(last, layout, sc, z_parts, masks, norms, xgs, w_ab, w_sq, w_bias):
    return pl.pallas_call(
        functools.partial(u_kernel, last, layout),
        out_shape=(ROW_WIDE, ROW_WIDE, SDS((4, 4, ROWS, COLS), BF16), *((FAR_LAST, *(TILE_FULL, TILE_HALF) * CHUNKS, AWAY) if last else (FAR, FAR))),
        in_specs=[SM] + [HB] * len(layout) + [VM] * 9,
        out_specs=(HB, HB, VM) + (HB,) * (2 * CHUNKS + 2 if last else 2),
        scratch_shapes=[
            pltpu.VMEM((COLS, CH, COLS), F32), SAMPLE_BF, SAMPLE_BF,
            pltpu.VMEM((CH, COLS, COLS), F32), pltpu.VMEM((COLS, COLS), F32), pltpu.VMEM((4, COLS, COLS), F32), AB_TILE, AB_TILE, pltpu.VMEM((CH, TILE, COLS), BF16), pltpu.VMEM((2, TILE, CH, COLS), BF16),
            pltpu.VMEM((TILE, 8, COLS), F32), pltpu.VMEM((2, TILE, CH, COLS), F32),
            pltpu.SemaphoreType.DMA((4,)), DMA2, DMA2,
        ],
        compiler_params=pltpu.CompilerParams(vmem_limit_bytes=62 * MIB),
        name="pair_updates",
    )(sc, *z_parts, *masks, norms, xgs, w_ab, w_sq, w_bias)


def l1_kernel(ids, z_in, mask_in, norms, w_ab, a_out, b_out, mask, tile_a, tile_b):
    out_norm = norm_of(norms, OUT)
    mask[:] = mask_in[0].astype(F32)

    @pl.loop(0, ROWS // TILE)
    def _(t):
        base = pl.multiple_of(TILE * t, TILE)
        staggered(
            TILE,
            lambda i, _: mm(w_ab[OUT], (mask[row_at(base, i), :] * channel_norm(z_in[0, base + i], out_norm)).astype(BF16)),
            lambda i, proj: ab_row(proj, tile_a, tile_b, i))
        a_out[0, :, pl.ds(base, TILE), :] = swap_major(tile_a[:])
        b_out[0, :, pl.ds(base, TILE), :] = swap_major(tile_b[:])


def l1_call(ids, zt, mask, norms, w_ab):
    n = ids.shape[0]
    ab = SDS((n, CH, ROWS, COLS), BF16)
    ab_spec = pl.BlockSpec((1, CH, ROWS, COLS), AT_FIRST)
    return pl.pallas_call(
        l1_kernel,
        out_shape=(ab, ab),
        grid_spec=pltpu.PrefetchScalarGridSpec(
            num_scalar_prefetch=1, grid=(n,),
            in_specs=[pl.BlockSpec((1, ROWS, CH, COLS), lambda i, ids: (ids[i], 0, 0, 0)),
                      pl.BlockSpec((1, ROWS, COLS), lambda i, ids: (ids[i], 0, 0)), VM, VM],
            out_specs=(ab_spec, ab_spec),
            scratch_shapes=[pltpu.VMEM((ROWS, COLS), F32), AB_TILE, AB_TILE]),
        compiler_params=PARAMS,
        name="near_projections",
    )(ids, zt, mask, norms, w_ab)


def l2_kernel(sc, a_in, b_own, b_par, xgs, x_out, x_s, tile_x):
    odd = sc[0] % 2 == 1

    @pl.loop(0, CH, unroll=2)
    def _(c):
        for n in range(2):
            own, par = b_own[n, c].astype(F32), b_par[1 - n, c].astype(F32)
            pair = jnp.concatenate([jnp.where(odd, par, own), jnp.where(odd, own, par)]).astype(BF16)
            x_s[c, :, LANES * n:LANES * n + LANES] = contract(a_in[n, c], pair, 1)

    @pl.loop(0, ROWS // TILE)
    def _(t):
        base = pl.multiple_of(TILE * t, TILE)
        x_norm_tile(x_s, tile_x, base, *pair_of(xgs, OUT))
        both = swap_major(tile_x[:])
        for n in range(2):
            x_out[n, pl.ds(base, TILE)] = both[:, :, LANES * n:LANES * n + LANES]


def l2_call(sc, a_all, b_own, b_par, xgs):
    n = a_all.shape[0]
    ab_spec = pl.BlockSpec((2, CH, ROWS, COLS), AT_FIRST)
    return pl.pallas_call(
        l2_kernel,
        grid=(n // 2,),
        out_shape=SDS((n, ROWS, CH, LANES), BF16),
        in_specs=[SM, ab_spec, ab_spec, ab_spec, VM],
        out_specs=pl.BlockSpec((2, ROWS, CH, LANES), AT_FIRST),
        scratch_shapes=[pltpu.VMEM((CH, ROWS, COLS), F32), pltpu.VMEM((CH, TILE, COLS), BF16)],
        compiler_params=PARAMS,
        name="near_product",
    )(sc, a_all, b_own, b_par, xgs)


def r_kernel(blocks, sc, z_in, x_near, x_far, xi, *refs):
    bias_far, refs = (refs[0], refs[1:]) if blocks else (None, refs)
    norms, w_sq, w_bias, z_out, *refs = refs
    swap, refs = (refs[0], refs[1:]) if blocks else (None, refs)
    tile_d, tile_z, z_buf, sem = refs
    step, steps = pl.program_id(0), pl.num_programs(0)
    first = sc[0] < 2
    out_norm, in_norm, att_norm = [norm_of(norms, place) for place in (OUT, IN, ATT)]

    def z_copy(n):
        return pltpu.make_async_copy(z_buf.at[n % 2], z_out.at[pl.ds(pl.multiple_of(n * TILE, TILE), TILE)], sem.at[n % 2])

    @pl.when(step >= 2)
    def _():
        z_copy(step - 2).wait()

    def gate_and_product(place, normed, product):
        gate, proj = pair_of(w_sq, place)
        return mm(gate[:], normed), mm(proj[:], product)

    def outgoing(i, _):
        near, far = x_near[0, i].astype(F32), x_far[i].astype(F32)
        xn = jnp.concatenate([jnp.where(first, near, far), jnp.where(first, far, near)], axis=1).astype(BF16)
        return gate_and_product(OUT, channel_norm(z_in[0, i], out_norm).astype(BF16), xn)

    def norm_one(i, parts):
        z_one = z_in[0, i] + opened(*parts)
        tile_z[i] = z_one
        return channel_norm(z_one, in_norm).astype(BF16)

    def incoming(i, normed):
        return gate_and_product(IN, normed, xi[i])

    def norm_two(i, parts):
        z_two = tile_z[i] + opened(*parts)
        z_buf[step % 2, i] = z_two
        return channel_norm(z_two, att_norm).astype(BF16) if blocks else None

    def bias_row(i, normed):
        tile_d[i] = mm(w_bias[:], normed)

    staggered(TILE, outgoing, norm_one, incoming, norm_two, *([bias_row] if blocks else []))
    z_copy(step).start()
    if blocks:
        swap[0, :, pl.ds(pl.multiple_of(step * TILE, TILE), TILE), :] = swap_major(tile_d[:])[:4].astype(BF16)

        @pl.when(step == 0)
        def _():
            for n in range(blocks):
                swap[n + 1] = bias_far[4 * n:4 * n + 4]

    @pl.when(step == steps - 1)
    def _():
        @pl.when(steps > 1)
        def _():
            z_copy(step - 1).wait()

        z_copy(step).wait()


def r_call(blocks, start, sc, zt, x_near, x_far, xi, norms, w_sq, w_bias):
    steps = ROWS // TILE if blocks else 1
    far_map = (lambda i, sc: (ROWS // TILE + i % 2, 0, i // 2)) if blocks else (lambda i, sc: (i, 0, 0))
    return pl.pallas_call(
        functools.partial(r_kernel, blocks),
        out_shape=[pltpu.HBM((steps * TILE, CH, COLS), F32)] + [pltpu.HBM((blocks + 1, 4, ROWS, COLS), BF16)] * (blocks > 0),
        grid_spec=pltpu.PrefetchScalarGridSpec(
            num_scalar_prefetch=1, grid=(steps,),
            in_specs=[pl.BlockSpec((1, TILE, CH, COLS), lambda i, sc: (sc[1], start + i, 0, 0)),
                      pl.BlockSpec((1, TILE, CH, LANES), lambda i, sc: (sc[2], start + i, 0, 0)),
                      pl.BlockSpec((TILE, CH, LANES), far_map), pl.BlockSpec((TILE, CH, COLS), lambda i, sc: (i, 0, 0)),
                      *[pl.BlockSpec((4 * blocks, CH, COLS), lambda i, sc: (FAR_BIAS // (4 * blocks), 0, 0))] * (blocks > 0),
                      VM, VM, VM],
            out_specs=[HB] + [pl.BlockSpec((blocks + 1, 4, ROWS, COLS), lambda i, sc: (0, 0, 0, 0))] * (blocks > 0),
            scratch_shapes=[pltpu.VMEM((TILE, 8, COLS), F32), pltpu.VMEM((TILE, CH, COLS), F32),
                            pltpu.VMEM((2, TILE, CH, COLS), F32), DMA2]),
        compiler_params=PARAMS,
        name="row_updates",
    )(sc, zt, x_near, x_far, xi, *[xi] * (blocks > 0), norms, w_sq, w_bias)


HEADS, HEAD = 4, 16
MASK_FILL = -1e9
CHUNK = 32
SLOTS = 2
STEPS = 6
AWAY_FIRST = 24


def attention_kernel(parts, fresh, away, sc, *refs):
    n = len(parts)
    z_refs, bias_refs, (mask_in, norms, w_all, w_proj, *rest) = refs[:n], refs[n:5 * n], refs[5 * n:]
    mask_away, rest = (rest[0], rest[1:]) if away else (None, rest)
    out, *rest = rest if fresh else rest[1:]
    out_away, rest = (rest[:2], rest[2:]) if away else ((), rest)
    (z_in, z_out, mask_i, mask, bias_in, bias_t, q_s, k_s, v_s, g_s, vn_s, gn_s, keep_s, s_buf, e_buf, p_s,
     top_s, inv_s, o_s, m_sem, z_sem, o_sem, b_sem) = rest
    n_rows = sum(size for _, size, _ in parts)
    att_norm = norm_of(norms, 0)

    def rows_of(j):
        return pl.ds(ROWS * j, parts[j][1])

    def own(ref, j):
        return ref.at[sc[j], pl.ds(*parts[j][:2])]

    def z_copy(j):
        return pltpu.make_async_copy(z_refs[j], z_in.at[rows_of(j)], z_sem.at[j])

    def m_copy(j):
        src = mask_away.at[0] if away and j == n - 1 else own(mask_in, j)
        return pltpu.make_async_copy(src, mask_i.at[rows_of(j)], m_sem.at[j])

    def b_copy(j, r):
        rows = pl.ds(pl.multiple_of(ROWS * (sc[n + j] ^ r), ROWS), ROWS)
        return pltpu.make_async_copy(bias_refs[4 * j + r].at[parts[j][2][r]], bias_in.at[j, :, rows], b_sem.at[j])

    def o_copies(j):
        if away and j == n - 1:
            return [pltpu.make_async_copy(z_out.at[pl.ds(ROWS * j + start, ref.shape[0])], ref, o_sem.at[j])
                    for ref, start in zip(out_away, (0, AWAY_FIRST))]
        return [pltpu.make_async_copy(z_out.at[rows_of(j)], own(out, j), o_sem.at[j])]

    starts = [f(j) for j in range(n) for f in (m_copy, *(functools.partial(b_copy, r=r) for r in range(4)))]
    for copy in starts + [z_copy(j) for j in range(n)]:
        copy.start()
    for copy in starts:
        copy.wait()
    mask[:] = mask_i[:].astype(F32)
    q_s[:] = jnp.zeros_like(q_s)

    @pl.loop(0, n * HEADS, unroll=4)
    def _(h):
        bias_t[h // HEADS, h % HEADS] = bias_in[h // HEADS, h % HEADS].astype(F32).T

    z_copy(0).wait()

    def project(row, slot):
        row = jnp.minimum(row, n_rows - 1)
        normed = channel_norm(z_in[row], att_norm).astype(BF16)
        proj = mm(w_all[:], normed)
        k_s[slot] = proj[CH:2 * CH].T.astype(BF16)
        q = proj[:CH].astype(BF16)
        for h in range(HEADS):
            q_s[slot, h, HEAD * h:HEAD * h + HEAD] = q[HEAD * h:HEAD * h + HEAD]
        vn_s[slot] = proj[2 * CH:3 * CH].astype(BF16)
        gn_s[slot] = sigmoid(proj[3 * CH:])

    def keep_mask(row, slot):
        row = jnp.minimum(row, n_rows - 1)
        keep_s[slot] = jnp.broadcast_to(mask[pl.ds(row, 1), :], (LANES, COLS)).T

    def tall(line):
        return jnp.concatenate([line] * (CHUNK // 8))

    def fold(part, op):
        out = part[:8]
        for n in range(1, part.shape[0] // 8):
            out = op(out, part[8 * n:8 * n + 8])
        return out

    def scores(slot, h):
        return mm(k_s[slot], q_s[slot, h])

    def weigh(slot, h, probs):
        heads = slice(HEAD * h, HEAD * h + HEAD)
        o_s[slot, heads] = mm(v_s[slot, heads], probs)

    def step(row, slot, h, logits, defer):
        buf, prev = h % 2, (h + 1) % 2
        sample = jnp.clip(row, 0, n_rows - 1) // ROWS
        top, total, probs = None, None, []
        for c in range(COLS // CHUNK):
            rows = slice(CHUNK * c, CHUNK * c + CHUNK)
            probs.append((e_buf[buf, rows] * tall(inv_s[buf])).astype(BF16))
            exps = jnp.exp(s_buf[prev, rows] - tall(top_s[prev]))
            e_buf[prev, rows] = exps
            part = fold(exps, jnp.add)
            total = part if total is None else total + part
            keep = keep_s[slot, rows]
            keep = jnp.concatenate([keep, keep], axis=1) > 0
            vals = jnp.where(keep, logits[rows] + bias_t[sample, h, rows], MASK_FILL)
            s_buf[buf, rows] = vals
            part = fold(vals, jnp.maximum)
            top = part if top is None else jnp.maximum(top, part)
        top_s[buf] = jnp.broadcast_to(jnp.max(top, axis=0, keepdims=True), (8, COLS))
        inv_s[prev] = jnp.broadcast_to(1.0 / jnp.sum(total, axis=0, keepdims=True), (8, COLS))
        if defer:
            p_s[:] = jnp.concatenate(probs)
        else:
            weigh(1 - slot if h < 2 else slot, (h - 2) % HEADS, jnp.concatenate(probs))

    def finish(row, slot):
        gated = (g_s[slot] * o_s[slot]).astype(BF16)
        z_out[jnp.maximum(row, 0)] = z_in[jnp.clip(row, 0, n_rows - 1)] + mm(w_proj[:], gated)

    project(0, 0)
    keep_mask(0, 0)
    n_steps = (n_rows + 2 + STEPS - 1) // STEPS

    @pl.loop(0, n_steps)
    def _(it):
        first = STEPS * it - 1
        lg = scores(1, 0)
        weigh(0, 1, p_s[:])
        for k in range(STEPS):
            row, slot, last = first + k, 1 - k % 2, k == STEPS - 1
            for h in range(HEADS):
                nxt = scores(slot, h + 1) if h < HEADS - 1 else (None if last else scores(1 - slot, 0))
                if h == 2:
                    project(row + 2, slot)
                step(row, slot, h, lg, last and h == HEADS - 1)
                lg = nxt
                if h == 3:
                    finish(row - 1, 1 - slot)
                    v_s[1 - slot] = vn_s[1 - slot]
                    g_s[1 - slot] = gn_s[1 - slot]
            keep_mask(row + 2, slot)
        for j in range(1, n):
            @pl.when(it == (ROWS * j - 1) // STEPS - 1)
            def _():
                z_copy(j).wait()

            @pl.when(it == (ROWS * j + 1) // STEPS)
            def _():
                for copy in o_copies(j - 1):
                    copy.start()

    for copy in o_copies(n - 1):
        copy.start()
    for j in range(n):
        for copy in o_copies(j):
            copy.wait()


def attend(static, sc, z_parts, biases, mask, norms, w_all, w_proj, out, mask_away=None):
    n, fresh, away = len(z_parts), out is None, mask_away is not None
    z_parts, biases = jax.tree.map(lambda v: pltpu.with_memory_space_constraint(v, pltpu.HBM), (list(z_parts), list(biases)))
    args = (sc, *z_parts, *biases, mask, norms, w_all, w_proj, *[mask_away] * away, *[out] * (not fresh))
    whole = SDS((mask.shape[0], ROWS, CH, COLS), F32)
    aways = [SDS((k, CH, COLS), F32) for k in (AWAY_FIRST, AWAY.shape[0] - AWAY_FIRST)] * away
    rows = sum(z.shape[0] for z in z_parts)
    pair, wide, square, line = [pltpu.VMEM((SLOTS, *shape), dtype) for shape, dtype in (
        ((CH, COLS), BF16), ((CH, COLS), F32), ((COLS, COLS), F32), ((8, COLS), F32))]
    each = [pltpu.VMEM((n, HEADS, COLS, COLS), dtype) for dtype in (BF16, F32)]
    sems = pltpu.SemaphoreType.DMA((n,))
    return pl.pallas_call(
        functools.partial(attention_kernel, static, fresh, away),
        out_shape=(whole, *aways),
        in_specs=[SM] + [HB] * (5 * n + 1) + [VM] * 3 + [HB] * (away + (not fresh)),
        out_specs=(HB,) * (1 + len(aways)),
        scratch_shapes=[
            pltpu.VMEM((rows, CH, COLS), F32), pltpu.VMEM((rows + STEPS, CH, COLS), F32), pltpu.VMEM((rows, COLS), jnp.int32),
            pltpu.VMEM((rows, COLS), F32), *each, pltpu.VMEM((SLOTS, HEADS, CH, COLS), BF16),
            pltpu.VMEM((SLOTS, COLS, CH), BF16), pair, wide, pair, wide, pltpu.VMEM((SLOTS, COLS, LANES), F32),
            square, square, pltpu.VMEM((COLS, COLS), BF16), line, line, wide, sems, sems, sems, sems,
        ],
        compiler_params=pltpu.CompilerParams(vmem_limit_bytes=48 * MIB),
        input_output_aliases={} if fresh else {len(args) - 1: 0},
        name="triangle_attention",
    )(*args)


FIRST = 8


def exchange(values, r):
    return lax.ppermute(values, 'dap', [(i, i ^ r) for i in range(4)])


def update_weights(params):
    norm_gain, norm_bias, w_a, w_agate, w_b, w_bgate, w_gate, x_gain, x_bias, w_proj = params
    half = jnp.bfloat16(0.5)
    wide = lambda v: jnp.broadcast_to(v[:, None], (CH, COLS))
    deep = lambda v: jnp.broadcast_to(v[:, None, None], (CH, 8, 128))
    return ([wide(norm_gain), wide(norm_bias)], [deep(x_gain), deep(x_bias)],
            half * jnp.concatenate([w_a.T, w_agate.T, w_b.T, w_bgate.T]), [half * w_gate.T, half * w_proj.T])


def solution(mesh):
    def local_block(pair_z, pair_mask, *weights):
        me = lax.axis_index('dap')
        zt = jnp.transpose(pair_z, (0, 1, 3, 2))
        n_own = zt.shape[0] // 4
        mask_bf = pair_mask.astype(BF16)
        arrived, layouts, before = [], [], ()
        for t in range(n_own):
            pieces = [(2, 0, FIRST), (2, FIRST, ROWS)] if t == 0 else [(2, 0, ROWS)]
            pieces += [(3, 0, ROWS), (1, 0, ROWS)]
            got = []
            for r, start, stop in pieces:
                where = (n_own * (me ^ r) + t, start, 0, 0)
                send = lax.dynamic_slice(lax.optimization_barrier((zt, *before))[0], where, (1, stop - start, CH, COLS))[0]
                if t == 0 or r == 1:
                    before = (send,)
                got.append(exchange(send, r))
                if t == 0 and stop == ROWS and r == 2:
                    mask_bf, weights = lax.optimization_barrier((mask_bf, weights, send))[:2]
                    masks = [lax.dynamic_slice_in_dim(mask_bf, n_own * (me ^ k), n_own) for k in range(4)]
                    before = (*before, *masks)
                    masks = [exchange(m, k) if k else m for k, m in enumerate(masks)]
            arrived.append([zt, *got])
            layouts.append(((0, 0), *((r, start) for r, start, _ in pieces)))

        out_n, out_x, out_ab, out_sq = update_weights(weights[:10])
        in_n, in_x, in_ab, in_sq = update_weights(weights[10:20])
        att_gain, att_shift, w_q, w_k, w_v, w_bias, w_gate, w_proj = weights[20:]
        att_n = [jnp.broadcast_to(v[:, None], (CH, COLS)) for v in (att_gain, att_shift)]
        norms = jnp.stack(out_n + in_n + att_n)
        xgs = jnp.stack(out_x + in_x)
        w_ab = jnp.stack([out_ab, in_ab])
        w_sq = jnp.stack(out_sq + in_sq)
        w_bias8 = jnp.concatenate([w_bias.T, jnp.zeros((4, CH), BF16)])
        w_all = jnp.concatenate([w_q.T * jnp.bfloat16(HEAD ** -0.5), w_k.T, w_v.T, w_gate.T])
        w_out = w_proj.T
        att_norms = norms[4:]

        token = [None]

        def ordered(call, sc, *args):
            sc = jnp.stack([jnp.asarray(v, jnp.int32) for v in sc])
            if token[0] is not None:
                sc = lax.optimization_barrier((sc, token[0]))[0]
            res = call(sc, *args)
            token[0] = jax.tree.leaves(res)[-1]
            return res

        def attention(jobs, out, mask_away=None):
            samples, orders, z_parts, biases, starts = zip(*jobs)
            static = tuple((start, z.shape[0], tuple(place for _, place in blocks))
                           for start, z, blocks in zip(starts, z_parts, biases))
            arrays = [array for blocks in biases for array, _ in blocks]
            return ordered(functools.partial(attend, static), samples + orders, z_parts, arrays, pair_mask, att_norms,
                           w_all, w_out, out, mask_away)

        far = [(t, r) for t in range(n_own) for r in (2, 3)]
        a_far, b_far = ordered(l1_call, [n_own * (me ^ r) + t for t, r in far], zt, pair_mask, norms, w_ab)
        b_par = exchange(b_far, 1)
        x_near = ordered(l2_call, [me], a_far, b_far, b_par, xgs)

        out = None
        held = []
        for t in range(n_own):
            last = t == n_own - 1
            z_own, z_par, bias, far2, *far3 = ordered(functools.partial(u_call, last, layouts[t]), [me, n_own * me + t],
                                                      arrived[t], [m[t] for m in masks], norms, xgs, w_ab, w_sq, w_bias8)
            here = lambda array: [(array, r) for r in range(4)]
            near = (n_own * (me ^ 1) + t, 0, exchange(z_par, 1), here(exchange(bias, 1)), 0)
            own = (n_own * me + t, 0, z_own, here(bias), 0)
            two = exchange(far2, 2)
            three = [exchange(v, 3) for v in far3[:2 * CHUNKS]]
            held.append((two, three))
            if last:
                out, *away = attention([own, (0, 0, far3[-1], here(bias), 0)], out,
                                       masks[3][t][None, CHUNKS * TILE:].astype(jnp.int32))
                away = [exchange(v, 3) for v in away]
            else:
                out, = attention([own, near], out)

        def rows_of(t, r, blocks, x_far, xi, start=0):
            return ordered(functools.partial(r_call, blocks, start), [me, n_own * (me ^ r) + t, far.index((t, r))],
                           zt, x_near, x_far, xi, norms, w_sq, w_bias8)

        for t in range(n_own - 1):
            two, (three,) = held[t]
            z_two, mine_two = rows_of(t, 2, 1, two, two)
            z_three, mine_three = rows_of(t, 3, 1, three, three)
            par_two, par_three = exchange(mine_two, 1), exchange(mine_three, 1)
            jobs = [(n_own * (me ^ r) + t, me, z, [(mine, 0), (par, 0), (mine, 1), (par, 1)], 0)
                    for r, z, mine, par in ((2, z_two, mine_two, par_three), (3, z_three, mine_three, par_two))]
            out, = attention(([] if t else [near]) + jobs, out)
        two, three = held[t + 1]
        z_two, mine = rows_of(t + 1, 2, 3, two, two)
        par = exchange(mine, 1)
        jobs = [(n_own * (me ^ 2) + t + 1, me, z_two, [(mine, k) for k in (0, 3, 1, 2)], 0)]
        for n in range(CHUNKS):
            z_three, = rows_of(t + 1, 3, 0, three[2 * n + 1], three[2 * n], n)
            jobs += [(n_own * (me ^ 3) + t + 1, me, z_three, [(par, k) for k in (3, 0, 2, 1)], n * TILE)]
            out, = attention(jobs, out)
            jobs = []
        for v, start in zip(away, (CHUNKS * TILE, CHUNKS * TILE + AWAY_FIRST)):
            out = lax.dynamic_update_slice(out, v[None], (n_own * (me ^ 3) + n_own - 1, start, 0, 0))
        return jnp.transpose(out, (0, 1, 3, 2))

    pair_spec = P('data', 'dap')
    return jax.shard_map(local_block, mesh=mesh, in_specs=(pair_spec, pair_spec) + (P(),) * 28,
                         out_specs=pair_spec, check_vma=False)
```

```python
import functools

import jax
import jax.numpy as jnp
from jax import lax
from jax.experimental import pallas as pl
from jax.experimental.pallas import tpu as pltpu
from jax.sharding import PartitionSpec as P


LN_EPS = 1e-5
F32, BF16 = jnp.float32, jnp.bfloat16
ROWS, CH, COLS = 64, 64, 256
TILE = 16
MIB = 1 << 20
OUT, IN, ATT = range(3)


def channel_stats(vals):
    ch_mean = jnp.mean(vals, axis=0, keepdims=True)
    ch_var = jnp.mean(jnp.square(vals - ch_mean), axis=0, keepdims=True)
    return ch_mean, lax.rsqrt(ch_var + LN_EPS)


def channel_norm(vals, norm, stats=None):
    gain, shift = norm
    ch_mean, scale = channel_stats(vals) if stats is None else stats
    return (vals - ch_mean) * scale * gain + shift


def sigmoid(vals):
    return 0.5 * jnp.tanh(0.5 * vals) + 0.5


def swap_major(vals):
    return jnp.swapaxes(vals, 0, 1)


def pair_of(ref, place):
    return ref.at[2 * place], ref.at[2 * place + 1]


def norm_of(ref, place):
    return [part[:] for part in pair_of(ref, place)]


def contract(lhs, rhs, axis_id):
    return lax.dot_general(lhs, rhs, (((axis_id,), (axis_id,)), ((), ())), preferred_element_type=F32)


def mm(lhs, rhs):
    return jnp.dot(lhs, rhs, preferred_element_type=F32)


def opened(gate, product):
    return (jnp.tanh(gate) + 1.0) * product


def row_at(base, i):
    return pl.ds(base + i, 1)


def ab_row(proj, tile_a, tile_b, slot):
    for n, tile in enumerate((tile_a, tile_b)):
        linear, gate = jnp.split(proj[2 * CH * n:2 * CH * n + 2 * CH], 2)
        tile[slot] = opened(gate, linear).astype(BF16)


def x_norm_tile(x_s, tile_x, base, xg, xb):
    parts = [(sub, half) for sub in range(2) for half in range(2)]

    def load(c, part):
        return x_s[c, pl.ds(pl.multiple_of(base + 8 * part[0], 8), 8), 128 * part[1]:128 * part[1] + 128]

    means = [sum(load(c, p) for c in range(CH)) * (1.0 / CH) for p in parts]
    scales = [lax.rsqrt(sum(jnp.square(load(c, p) - means[n]) for c in range(CH)) * (1.0 / CH) + LN_EPS)
              for n, p in enumerate(parts)]
    for c in range(CH):
        rows = []
        for sub in range(2):
            rows.append(jnp.concatenate(
                [(load(c, (sub, half)) - means[2 * sub + half]) * scales[2 * sub + half] * xg[c] + xb[c]
                 for half in range(2)], axis=1))
        tile_x[c] = jnp.concatenate(rows).astype(BF16)


LAG = 3


def staggered(count, *stages):
    held = [{} for _ in stages]
    for tick in range(count + LAG * (len(stages) - 1)):
        for k, stage in enumerate(stages):
            i = tick - LAG * k
            if 0 <= i < count:
                held[k][i] = stage(i, held[k - 1].pop(i) if k else None)


def u_kernel(last, layout, sc, *refs):
    z_refs = refs[:len(layout)]
    n_far = 3 if last else 1
    (mask0, mask1, mask2, mask3, norms, xgs, w_ab, w_sq, w_bias, z2_own, z2_par, bias_out, far2, *far3) = refs[len(layout):][:13 + n_far]
    (z_s, a_s, b_s, x_s, mask, stats, tile_a, tile_b, tile_x, tile_c, tile_d, tile_z, in_sem, z_sem, x_sem) = refs[len(layout) + 13 + n_far:]
    me, sample = sc[0], sc[1]
    lanes = pl.ds(pl.multiple_of(LANES * (me // 2), LANES), LANES)
    out_norm = norm_of(norms, OUT)
    in_norm = norm_of(norms, IN)
    att_norm = norm_of(norms, ATT)
    n_tiles = COLS // TILE

    for ref, (r, start) in zip(z_refs, layout):
        src = ref if r else ref.at[sample]
        rows = pl.ds(pl.multiple_of(ROWS * (me ^ r) + start, 8), src.shape[0])
        pltpu.make_async_copy(src, z_s.at[rows], in_sem.at[r]).start()
    for r, part in enumerate((mask0, mask1, mask2, mask3)):
        mask[pl.ds(pl.multiple_of(ROWS * (me ^ r), ROWS), ROWS), :] = part[:].astype(F32)

    def gate_and_product(place, normed, product):
        gate, proj = pair_of(w_sq, place)
        return mm(gate[:], normed), mm(proj[:], product)

    def mask_row(base, i):
        return mask[row_at(base, i), :]

    def measure(base, i, vals=None):
        found = channel_stats(z_s[base + i] if vals is None else vals)
        for n in range(2):
            stats[n if vals is None else n + 2, row_at(base, i), :] = found[n]
        return found

    def recall(base, i, first):
        return [stats[first + n, row_at(base, i), :] for n in range(2)]

    def flush(base):
        a_s[:, pl.ds(base, TILE), :] = swap_major(tile_a[:])
        b_s[:, pl.ds(base, TILE), :] = swap_major(tile_b[:])

    def export(t, start, outgoing, sem):
        r = (t * TILE // ROWS) ^ me
        q = t % (ROWS // TILE)
        rows = pl.ds(pl.multiple_of(TILE * q, TILE), TILE)
        half = pl.ds(pl.multiple_of(ROWS + TILE * (q % 2), TILE), TILE)
        side = pl.ds(pl.multiple_of(LANES * (q // 2), LANES), LANES)
        act = (lambda cp: cp.start()) if start else (lambda cp: cp.wait())
        wide, z_tile = tile_c.at[t % 2], tile_z.at[t % 2]
        narrow = tile_c.at[t % 2, :, :, lanes]
        jobs = [(r == 2, narrow, far2.at[half, :, side])] if outgoing else [
            (r == 0, z_tile, z2_own.at[rows]), (r == 1, z_tile, z2_par.at[rows]), (r == 2, wide, far2.at[rows])]
        if last:
            near_rows, away_rows = (pl.ds(pl.multiple_of(TILE * row, TILE), TILE)
                                    for row in (jnp.minimum(q, CHUNKS - 1), jnp.maximum(q - CHUNKS, 0)))
            jobs += [((r == 3) & (q < CHUNKS), *((narrow, far3[1].at[near_rows]) if outgoing else (wide, far3[0].at[near_rows])))]
            if not outgoing:
                jobs += [((r == 3) & (q >= CHUNKS), z_tile, far3[-1].at[away_rows])]
        else:
            jobs += [(r == 3, narrow, far3[0].at[half, :, side]) if outgoing else (r == 3, wide, far3[0].at[rows])]
        for when, src, dst in jobs:
            @pl.when(when)
            def _():
                act(pltpu.make_async_copy(src, dst, sem.at[t % 2]))

    @pl.loop(0, n_tiles)
    def _(v):
        r = v * TILE // ROWS

        @pl.when(v * TILE % ROWS == 0)
        def _():
            pltpu.make_async_copy(z_refs[0].at[sample], z_s.at[pl.ds(0, ROWS)], in_sem.at[r]).wait()

        base = pl.multiple_of(ROWS * (me ^ r) + v * TILE % ROWS, TILE)
        staggered(
            TILE,
            lambda i, _: mm(w_ab[OUT], (mask_row(base, i) * channel_norm(z_s[base + i], out_norm, measure(base, i))).astype(BF16)),
            lambda i, proj: ab_row(proj, tile_a, tile_b, i))
        flush(base)

    @pl.loop(0, CH, unroll=16)
    def _(c):
        x_s[c] = contract(a_s[c], b_s[c], 1)

    @pl.loop(0, n_tiles)
    def _(t):
        base = pl.multiple_of(TILE * t, TILE)

        @pl.when(t >= 2)
        def _():
            export(t - 2, False, True, x_sem)

        x_norm_tile(x_s, tile_x, base, *pair_of(xgs, OUT))
        tile_c[t % 2] = swap_major(tile_x[:])

        def gate_and_update(i, _):
            normed = channel_norm(z_s[base + i], out_norm, recall(base, i, 0)).astype(BF16)
            return gate_and_product(OUT, normed, tile_c[t % 2, i])

        def next_norm(i, parts):
            z_one = z_s[base + i] + opened(*parts)
            tile_z[0, i] = z_one
            return (mask_row(base, i) * channel_norm(z_one, in_norm, measure(base, i, z_one))).astype(BF16)

        staggered(TILE, gate_and_update, next_norm, lambda i, normed: mm(w_ab[IN], normed),
                  lambda i, proj: ab_row(proj, tile_a, tile_b, i))
        flush(base)
        z_s[pl.ds(base, TILE)] = tile_z[0]
        export(t, True, True, x_sem)

    for t in (n_tiles - 2, n_tiles - 1):
        export(t, False, True, x_sem)

    @pl.loop(0, CH, unroll=16)
    def _(c):
        x_s[c] = contract(a_s[c], b_s[c], 0)

    @pl.loop(0, n_tiles)
    def _(t):
        base = pl.multiple_of(TILE * t, TILE)

        @pl.when(t >= 2)
        def _():
            export(t - 2, False, False, z_sem)

        x_norm_tile(x_s, tile_x, base, *pair_of(xgs, IN))
        tile_c[t % 2] = swap_major(tile_x[:])

        def gate_and_update(i, _):
            normed = channel_norm(z_s[base + i], in_norm, recall(base, i, 2)).astype(BF16)
            return gate_and_product(IN, normed, tile_c[t % 2, i])

        def next_norm(i, parts):
            z_two = z_s[base + i] + opened(*parts)
            tile_z[t % 2, i] = z_two
            return channel_norm(z_two, att_norm).astype(BF16)

        def bias_row(i, normed):
            tile_d[i] = mm(w_bias[:], normed)

        staggered(TILE, gate_and_update, next_norm, bias_row)
        rows = pl.ds(pl.multiple_of(t * TILE % ROWS, TILE), TILE)
        bias_out[t * TILE // ROWS, :, rows, :] = swap_major(tile_d[:])[:4].astype(BF16)
        export(t, True, False, z_sem)

    bias_to = ((far2, 0, 0), (far2, 1, 1), (far2, 3, 2)) if last else ((far2, 0, 0), (far3[0], 1, 0))

    def bias_copy(n):
        dst, block, place = bias_to[n]
        return pltpu.make_async_copy(bias_out.at[me ^ block], dst.at[pl.ds(FAR_BIAS + 4 * place, 4)], in_sem.at[n])

    for n in range(len(bias_to)):
        bias_copy(n).start()
    for t in (n_tiles - 2, n_tiles - 1):
        export(t, False, False, z_sem)
    for n in range(len(bias_to)):
        bias_copy(n).wait()


LANES = 128
VM = pl.BlockSpec(memory_space=pltpu.VMEM)
HB = pl.BlockSpec(memory_space=pltpu.HBM)
SDS = jax.ShapeDtypeStruct
AT_FIRST = lambda i, *_: (i, 0, 0, 0)
SM = pl.BlockSpec(memory_space=pltpu.SMEM)
PARAMS = pltpu.CompilerParams(vmem_limit_bytes=40 * MIB, dimension_semantics=("arbitrary",))
AB_TILE = pltpu.VMEM((TILE, CH, COLS), BF16)
DMA2 = pltpu.SemaphoreType.DMA((2,))
FAR_BIAS = ROWS + ROWS // 2
FAR = SDS((FAR_BIAS + 4, CH, COLS), BF16)
CHUNKS = 2
SOME = CHUNKS * TILE
AWAY = SDS((ROWS - SOME, CH, COLS), F32)
SOME_FULL = SDS((SOME, CH, COLS), BF16)
SOME_HALF = SDS((SOME, CH, LANES), BF16)
FAR_LAST = SDS((FAR_BIAS + 12, CH, COLS), BF16)
ROW_WIDE = SDS((ROWS, CH, COLS), F32)
SAMPLE_BF = pltpu.VMEM((CH, COLS, COLS), BF16)


def u_call(last, layout, sc, z_parts, masks, norms, xgs, w_ab, w_sq, w_bias):
    return pl.pallas_call(
        functools.partial(u_kernel, last, layout),
        out_shape=(ROW_WIDE, ROW_WIDE, SDS((4, 4, ROWS, COLS), BF16), *((FAR_LAST, SOME_FULL, SOME_HALF, AWAY) if last else (FAR, FAR))),
        in_specs=[SM] + [HB] * len(layout) + [VM] * 9,
        out_specs=(HB, HB, VM) + (HB,) * (4 if last else 2),
        scratch_shapes=[
            pltpu.VMEM((COLS, CH, COLS), F32), SAMPLE_BF, SAMPLE_BF,
            pltpu.VMEM((CH, COLS, COLS), F32), pltpu.VMEM((COLS, COLS), F32), pltpu.VMEM((4, COLS, COLS), F32), AB_TILE, AB_TILE, pltpu.VMEM((CH, TILE, COLS), BF16), pltpu.VMEM((2, TILE, CH, COLS), BF16),
            pltpu.VMEM((TILE, 8, COLS), F32), pltpu.VMEM((2, TILE, CH, COLS), F32),
            pltpu.SemaphoreType.DMA((4,)), DMA2, DMA2,
        ],
        compiler_params=pltpu.CompilerParams(vmem_limit_bytes=62 * MIB),
        name="pair_updates",
    )(sc, *z_parts, *masks, norms, xgs, w_ab, w_sq, w_bias)


def l1_kernel(ids, z_in, mask_in, norms, w_ab, a_out, b_out, mask, tile_a, tile_b):
    out_norm = norm_of(norms, OUT)
    mask[:] = mask_in[0].astype(F32)

    @pl.loop(0, ROWS // TILE)
    def _(t):
        base = pl.multiple_of(TILE * t, TILE)
        staggered(
            TILE,
            lambda i, _: mm(w_ab[OUT], (mask[row_at(base, i), :] * channel_norm(z_in[0, base + i], out_norm)).astype(BF16)),
            lambda i, proj: ab_row(proj, tile_a, tile_b, i))
        a_out[0, :, pl.ds(base, TILE), :] = swap_major(tile_a[:])
        b_out[0, :, pl.ds(base, TILE), :] = swap_major(tile_b[:])


def l1_call(ids, zt, mask, norms, w_ab):
    n = ids.shape[0]
    ab = SDS((n, CH, ROWS, COLS), BF16)
    ab_spec = pl.BlockSpec((1, CH, ROWS, COLS), AT_FIRST)
    return pl.pallas_call(
        l1_kernel,
        out_shape=(ab, ab),
        grid_spec=pltpu.PrefetchScalarGridSpec(
            num_scalar_prefetch=1, grid=(n,),
            in_specs=[pl.BlockSpec((1, ROWS, CH, COLS), lambda i, ids: (ids[i], 0, 0, 0)),
                      pl.BlockSpec((1, ROWS, COLS), lambda i, ids: (ids[i], 0, 0)), VM, VM],
            out_specs=(ab_spec, ab_spec),
            scratch_shapes=[pltpu.VMEM((ROWS, COLS), F32), AB_TILE, AB_TILE]),
        compiler_params=PARAMS,
        name="near_projections",
    )(ids, zt, mask, norms, w_ab)


def l2_kernel(sc, a_in, b_own, b_par, xgs, x_out, x_s, tile_x):
    odd = sc[0] % 2 == 1

    @pl.loop(0, CH, unroll=2)
    def _(c):
        for n in range(2):
            own, par = b_own[n, c].astype(F32), b_par[1 - n, c].astype(F32)
            pair = jnp.concatenate([jnp.where(odd, par, own), jnp.where(odd, own, par)]).astype(BF16)
            x_s[c, :, LANES * n:LANES * n + LANES] = contract(a_in[n, c], pair, 1)

    @pl.loop(0, ROWS // TILE)
    def _(t):
        base = pl.multiple_of(TILE * t, TILE)
        x_norm_tile(x_s, tile_x, base, *pair_of(xgs, OUT))
        both = swap_major(tile_x[:])
        for n in range(2):
            x_out[n, pl.ds(base, TILE)] = both[:, :, LANES * n:LANES * n + LANES]


def l2_call(sc, a_all, b_own, b_par, xgs):
    n = a_all.shape[0]
    ab_spec = pl.BlockSpec((2, CH, ROWS, COLS), AT_FIRST)
    return pl.pallas_call(
        l2_kernel,
        grid=(n // 2,),
        out_shape=SDS((n, ROWS, CH, LANES), BF16),
        in_specs=[SM, ab_spec, ab_spec, ab_spec, VM],
        out_specs=pl.BlockSpec((2, ROWS, CH, LANES), AT_FIRST),
        scratch_shapes=[pltpu.VMEM((CH, ROWS, COLS), F32), pltpu.VMEM((CH, TILE, COLS), BF16)],
        compiler_params=PARAMS,
        name="near_product",
    )(sc, a_all, b_own, b_par, xgs)


def r_kernel(blocks, sc, z_in, x_near, x_far, xi, *refs):
    bias_far, refs = (refs[0], refs[1:]) if blocks else (None, refs)
    norms, w_sq, w_bias, z_out, *refs = refs
    swap, refs = (refs[0], refs[1:]) if blocks else (None, refs)
    tile_d, tile_z, z_buf, sem = refs
    step, steps = pl.program_id(0), pl.num_programs(0)
    first = sc[0] < 2
    out_norm, in_norm, att_norm = [norm_of(norms, place) for place in (OUT, IN, ATT)]

    def z_copy(n):
        return pltpu.make_async_copy(z_buf.at[n % 2], z_out.at[pl.ds(pl.multiple_of(n * TILE, TILE), TILE)], sem.at[n % 2])

    @pl.when(step >= 2)
    def _():
        z_copy(step - 2).wait()

    def gate_and_product(place, normed, product):
        gate, proj = pair_of(w_sq, place)
        return mm(gate[:], normed), mm(proj[:], product)

    def outgoing(i, _):
        near, far = x_near[0, i].astype(F32), x_far[i].astype(F32)
        xn = jnp.concatenate([jnp.where(first, near, far), jnp.where(first, far, near)], axis=1).astype(BF16)
        return gate_and_product(OUT, channel_norm(z_in[0, i], out_norm).astype(BF16), xn)

    def norm_one(i, parts):
        z_one = z_in[0, i] + opened(*parts)
        tile_z[i] = z_one
        return channel_norm(z_one, in_norm).astype(BF16)

    def incoming(i, normed):
        return gate_and_product(IN, normed, xi[i])

    def norm_two(i, parts):
        z_two = tile_z[i] + opened(*parts)
        z_buf[step % 2, i] = z_two
        return channel_norm(z_two, att_norm).astype(BF16) if blocks else None

    def bias_row(i, normed):
        tile_d[i] = mm(w_bias[:], normed)

    staggered(TILE, outgoing, norm_one, incoming, norm_two, *([bias_row] if blocks else []))
    z_copy(step).start()
    if blocks:
        swap[0, :, pl.ds(pl.multiple_of(step * TILE, TILE), TILE), :] = swap_major(tile_d[:])[:4].astype(BF16)

        @pl.when(step == 0)
        def _():
            for n in range(blocks):
                swap[n + 1] = bias_far[4 * n:4 * n + 4]

    @pl.when(step == steps - 1)
    def _():
        z_copy(step - 1).wait()
        z_copy(step).wait()


def r_call(blocks, sc, zt, x_near, x_far, xi, norms, w_sq, w_bias):
    steps = ROWS // TILE if blocks else CHUNKS
    far_map = (lambda i, sc: (ROWS // TILE + i % 2, 0, i // 2)) if blocks else (lambda i, sc: (i, 0, 0))
    return pl.pallas_call(
        functools.partial(r_kernel, blocks),
        out_shape=[pltpu.HBM((steps * TILE, CH, COLS), F32)] + [pltpu.HBM((blocks + 1, 4, ROWS, COLS), BF16)] * (blocks > 0),
        grid_spec=pltpu.PrefetchScalarGridSpec(
            num_scalar_prefetch=1, grid=(steps,),
            in_specs=[pl.BlockSpec((1, TILE, CH, COLS), lambda i, sc: (sc[1], i, 0, 0)),
                      pl.BlockSpec((1, TILE, CH, LANES), lambda i, sc: (sc[2], i, 0, 0)),
                      pl.BlockSpec((TILE, CH, LANES), far_map), pl.BlockSpec((TILE, CH, COLS), lambda i, sc: (i, 0, 0)),
                      *[pl.BlockSpec((4 * blocks, CH, COLS), lambda i, sc: (FAR_BIAS // (4 * blocks), 0, 0))] * (blocks > 0),
                      VM, VM, VM],
            out_specs=[HB] + [pl.BlockSpec((blocks + 1, 4, ROWS, COLS), lambda i, sc: (0, 0, 0, 0))] * (blocks > 0),
            scratch_shapes=[pltpu.VMEM((TILE, 8, COLS), F32), pltpu.VMEM((TILE, CH, COLS), F32),
                            pltpu.VMEM((2, TILE, CH, COLS), F32), DMA2]),
        compiler_params=PARAMS,
        name="row_updates",
    )(sc, zt, x_near, x_far, xi, *[xi] * (blocks > 0), norms, w_sq, w_bias)


HEADS, HEAD = 4, 16
MASK_FILL = -1e9
CHUNK = 32
SLOTS = 2
STEPS = 6
AWAY_FIRST = 24


def attention_kernel(parts, fresh, away, sc, *refs):
    n = len(parts)
    z_refs, bias_refs, (mask_in, norms, w_all, w_proj, *rest) = refs[:n], refs[n:5 * n], refs[5 * n:]
    mask_away, rest = (rest[0], rest[1:]) if away else (None, rest)
    out, *rest = rest if fresh else rest[1:]
    out_away, rest = (rest[:2], rest[2:]) if away else ((), rest)
    (z_in, z_out, mask_i, mask, bias_in, bias_t, q_s, k_s, v_s, g_s, vn_s, gn_s, keep_s, s_buf, e_buf, p_s,
     top_s, inv_s, o_s, m_sem, z_sem, o_sem, b_sem) = rest
    n_rows = sum(size for _, size, _ in parts)
    att_norm = norm_of(norms, 0)

    def rows_of(j):
        return pl.ds(ROWS * j, parts[j][1])

    def own(ref, j):
        return ref.at[sc[j], pl.ds(*parts[j][:2])]

    def z_copy(j):
        return pltpu.make_async_copy(z_refs[j], z_in.at[rows_of(j)], z_sem.at[j])

    def m_copy(j):
        src = mask_away.at[0] if away and j == n - 1 else own(mask_in, j)
        return pltpu.make_async_copy(src, mask_i.at[rows_of(j)], m_sem.at[j])

    def b_copy(j, r):
        rows = pl.ds(pl.multiple_of(ROWS * (sc[n + j] ^ r), ROWS), ROWS)
        return pltpu.make_async_copy(bias_refs[4 * j + r].at[parts[j][2][r]], bias_in.at[j, :, rows], b_sem.at[j])

    def o_copies(j):
        if away and j == n - 1:
            return [pltpu.make_async_copy(z_out.at[pl.ds(ROWS * j + start, ref.shape[0])], ref, o_sem.at[j])
                    for ref, start in zip(out_away, (0, AWAY_FIRST))]
        return [pltpu.make_async_copy(z_out.at[rows_of(j)], own(out, j), o_sem.at[j])]

    starts = [f(j) for j in range(n) for f in (m_copy, *(functools.partial(b_copy, r=r) for r in range(4)))]
    for copy in starts + [z_copy(j) for j in range(n)]:
        copy.start()
    for copy in starts:
        copy.wait()
    mask[:] = mask_i[:].astype(F32)
    q_s[:] = jnp.zeros_like(q_s)

    @pl.loop(0, n * HEADS, unroll=4)
    def _(h):
        bias_t[h // HEADS, h % HEADS] = bias_in[h // HEADS, h % HEADS].astype(F32).T

    z_copy(0).wait()

    def project(row, slot):
        row = jnp.minimum(row, n_rows - 1)
        normed = channel_norm(z_in[row], att_norm).astype(BF16)
        proj = mm(w_all[:], normed)
        k_s[slot] = proj[CH:2 * CH].T.astype(BF16)
        q = proj[:CH].astype(BF16)
        for h in range(HEADS):
            q_s[slot, h, HEAD * h:HEAD * h + HEAD] = q[HEAD * h:HEAD * h + HEAD]
        vn_s[slot] = proj[2 * CH:3 * CH].astype(BF16)
        gn_s[slot] = sigmoid(proj[3 * CH:])

    def keep_mask(row, slot):
        row = jnp.minimum(row, n_rows - 1)
        keep_s[slot] = jnp.broadcast_to(mask[pl.ds(row, 1), :], (LANES, COLS)).T

    def tall(line):
        return jnp.concatenate([line] * (CHUNK // 8))

    def fold(part, op):
        out = part[:8]
        for n in range(1, part.shape[0] // 8):
            out = op(out, part[8 * n:8 * n + 8])
        return out

    def scores(slot, h):
        return mm(k_s[slot], q_s[slot, h])

    def weigh(slot, h, probs):
        heads = slice(HEAD * h, HEAD * h + HEAD)
        o_s[slot, heads] = mm(v_s[slot, heads], probs)

    def step(row, slot, h, logits, defer):
        buf, prev = h % 2, (h + 1) % 2
        sample = jnp.clip(row, 0, n_rows - 1) // ROWS
        top, total, probs = None, None, []
        for c in range(COLS // CHUNK):
            rows = slice(CHUNK * c, CHUNK * c + CHUNK)
            probs.append((e_buf[buf, rows] * tall(inv_s[buf])).astype(BF16))
            exps = jnp.exp(s_buf[prev, rows] - tall(top_s[prev]))
            e_buf[prev, rows] = exps
            part = fold(exps, jnp.add)
            total = part if total is None else total + part
            keep = keep_s[slot, rows]
            keep = jnp.concatenate([keep, keep], axis=1) > 0
            vals = jnp.where(keep, logits[rows] + bias_t[sample, h, rows], MASK_FILL)
            s_buf[buf, rows] = vals
            part = fold(vals, jnp.maximum)
            top = part if top is None else jnp.maximum(top, part)
        top_s[buf] = jnp.broadcast_to(jnp.max(top, axis=0, keepdims=True), (8, COLS))
        inv_s[prev] = jnp.broadcast_to(1.0 / jnp.sum(total, axis=0, keepdims=True), (8, COLS))
        if defer:
            p_s[:] = jnp.concatenate(probs)
        else:
            weigh(1 - slot if h < 2 else slot, (h - 2) % HEADS, jnp.concatenate(probs))

    def finish(row, slot):
        gated = (g_s[slot] * o_s[slot]).astype(BF16)
        z_out[jnp.maximum(row, 0)] = z_in[jnp.clip(row, 0, n_rows - 1)] + mm(w_proj[:], gated)

    project(0, 0)
    keep_mask(0, 0)
    n_steps = (n_rows + 2 + STEPS - 1) // STEPS

    @pl.loop(0, n_steps)
    def _(it):
        first = STEPS * it - 1
        lg = scores(1, 0)
        weigh(0, 1, p_s[:])
        for k in range(STEPS):
            row, slot, last = first + k, 1 - k % 2, k == STEPS - 1
            for h in range(HEADS):
                nxt = scores(slot, h + 1) if h < HEADS - 1 else (None if last else scores(1 - slot, 0))
                if h == 2:
                    project(row + 2, slot)
                step(row, slot, h, lg, last and h == HEADS - 1)
                lg = nxt
                if h == 3:
                    finish(row - 1, 1 - slot)
                    v_s[1 - slot] = vn_s[1 - slot]
                    g_s[1 - slot] = gn_s[1 - slot]
            keep_mask(row + 2, slot)
        for j in range(1, n):
            @pl.when(it == (ROWS * j - 1) // STEPS - 1)
            def _():
                z_copy(j).wait()

            @pl.when(it == (ROWS * j + 1) // STEPS)
            def _():
                for copy in o_copies(j - 1):
                    copy.start()

    for copy in o_copies(n - 1):
        copy.start()
    for j in range(n):
        for copy in o_copies(j):
            copy.wait()


def attend(static, sc, z_parts, biases, mask, norms, w_all, w_proj, out, mask_away=None):
    n, fresh, away = len(z_parts), out is None, mask_away is not None
    z_parts, biases = jax.tree.map(lambda v: pltpu.with_memory_space_constraint(v, pltpu.HBM), (list(z_parts), list(biases)))
    args = (sc, *z_parts, *biases, mask, norms, w_all, w_proj, *[mask_away] * away, *[out] * (not fresh))
    whole = SDS((mask.shape[0], ROWS, CH, COLS), F32)
    aways = [SDS((k, CH, COLS), F32) for k in (AWAY_FIRST, AWAY.shape[0] - AWAY_FIRST)] * away
    rows = sum(z.shape[0] for z in z_parts)
    pair, wide, square, line = [pltpu.VMEM((SLOTS, *shape), dtype) for shape, dtype in (
        ((CH, COLS), BF16), ((CH, COLS), F32), ((COLS, COLS), F32), ((8, COLS), F32))]
    each = [pltpu.VMEM((n, HEADS, COLS, COLS), dtype) for dtype in (BF16, F32)]
    sems = pltpu.SemaphoreType.DMA((n,))
    return pl.pallas_call(
        functools.partial(attention_kernel, static, fresh, away),
        out_shape=(whole, *aways),
        in_specs=[SM] + [HB] * (5 * n + 1) + [VM] * 3 + [HB] * (away + (not fresh)),
        out_specs=(HB,) * (1 + len(aways)),
        scratch_shapes=[
            pltpu.VMEM((rows, CH, COLS), F32), pltpu.VMEM((rows + STEPS, CH, COLS), F32), pltpu.VMEM((rows, COLS), jnp.int32),
            pltpu.VMEM((rows, COLS), F32), *each, pltpu.VMEM((SLOTS, HEADS, CH, COLS), BF16),
            pltpu.VMEM((SLOTS, COLS, CH), BF16), pair, wide, pair, wide, pltpu.VMEM((SLOTS, COLS, LANES), F32),
            square, square, pltpu.VMEM((COLS, COLS), BF16), line, line, wide, sems, sems, sems, sems,
        ],
        compiler_params=pltpu.CompilerParams(vmem_limit_bytes=48 * MIB),
        input_output_aliases={} if fresh else {len(args) - 1: 0},
        name="triangle_attention",
    )(*args)


FIRST = 8


def exchange(values, r):
    return lax.ppermute(values, 'dap', [(i, i ^ r) for i in range(4)])


def update_weights(params):
    norm_gain, norm_bias, w_a, w_agate, w_b, w_bgate, w_gate, x_gain, x_bias, w_proj = params
    half = jnp.bfloat16(0.5)
    wide = lambda v: jnp.broadcast_to(v[:, None], (CH, COLS))
    deep = lambda v: jnp.broadcast_to(v[:, None, None], (CH, 8, 128))
    return ([wide(norm_gain), wide(norm_bias)], [deep(x_gain), deep(x_bias)],
            half * jnp.concatenate([w_a.T, w_agate.T, w_b.T, w_bgate.T]), [half * w_gate.T, half * w_proj.T])


def solution(mesh):
    def local_block(pair_z, pair_mask, *weights):
        me = lax.axis_index('dap')
        zt = jnp.transpose(pair_z, (0, 1, 3, 2))
        n_own = zt.shape[0] // 4
        mask_bf = pair_mask.astype(BF16)
        arrived, layouts, before = [], [], ()
        for t in range(n_own):
            pieces = [(2, 0, FIRST), (2, FIRST, ROWS)] if t == 0 else [(2, 0, ROWS)]
            pieces += [(3, 0, ROWS), (1, 0, ROWS)]
            got = []
            for r, start, stop in pieces:
                where = (n_own * (me ^ r) + t, start, 0, 0)
                send = lax.dynamic_slice(lax.optimization_barrier((zt, *before))[0], where, (1, stop - start, CH, COLS))[0]
                if t == 0 or r == 1:
                    before = (send,)
                got.append(exchange(send, r))
                if t == 0 and stop == ROWS and r == 2:
                    mask_bf, weights = lax.optimization_barrier((mask_bf, weights, send))[:2]
                    masks = [lax.dynamic_slice_in_dim(mask_bf, n_own * (me ^ k), n_own) for k in range(4)]
                    before = (*before, *masks)
                    masks = [exchange(m, k) if k else m for k, m in enumerate(masks)]
            arrived.append([zt, *got])
            layouts.append(((0, 0), *((r, start) for r, start, _ in pieces)))

        out_n, out_x, out_ab, out_sq = update_weights(weights[:10])
        in_n, in_x, in_ab, in_sq = update_weights(weights[10:20])
        att_gain, att_shift, w_q, w_k, w_v, w_bias, w_gate, w_proj = weights[20:]
        att_n = [jnp.broadcast_to(v[:, None], (CH, COLS)) for v in (att_gain, att_shift)]
        norms = jnp.stack(out_n + in_n + att_n)
        xgs = jnp.stack(out_x + in_x)
        w_ab = jnp.stack([out_ab, in_ab])
        w_sq = jnp.stack(out_sq + in_sq)
        w_bias8 = jnp.concatenate([w_bias.T, jnp.zeros((4, CH), BF16)])
        w_all = jnp.concatenate([w_q.T * jnp.bfloat16(HEAD ** -0.5), w_k.T, w_v.T, w_gate.T])
        w_out = w_proj.T
        att_norms = norms[4:]

        token = [None]

        def ordered(call, sc, *args):
            sc = jnp.stack([jnp.asarray(v, jnp.int32) for v in sc])
            if token[0] is not None:
                sc = lax.optimization_barrier((sc, token[0]))[0]
            res = call(sc, *args)
            token[0] = jax.tree.leaves(res)[-1]
            return res

        def attention(jobs, out, mask_away=None):
            samples, orders, z_parts, biases, starts = zip(*jobs)
            static = tuple((start, z.shape[0], tuple(place for _, place in blocks))
                           for start, z, blocks in zip(starts, z_parts, biases))
            arrays = [array for blocks in biases for array, _ in blocks]
            return ordered(functools.partial(attend, static), samples + orders, z_parts, arrays, pair_mask, att_norms,
                           w_all, w_out, out, mask_away)

        far = [(t, r) for t in range(n_own) for r in (2, 3)]
        a_far, b_far = ordered(l1_call, [n_own * (me ^ r) + t for t, r in far], zt, pair_mask, norms, w_ab)
        b_par = exchange(b_far, 1)
        x_near = ordered(l2_call, [me], a_far, b_far, b_par, xgs)

        out = None
        held = []
        for t in range(n_own):
            last = t == n_own - 1
            z_own, z_par, bias, far2, *far3 = ordered(functools.partial(u_call, last, layouts[t]), [me, n_own * me + t],
                                                      arrived[t], [m[t] for m in masks], norms, xgs, w_ab, w_sq, w_bias8)
            here = lambda array: [(array, r) for r in range(4)]
            near = (n_own * (me ^ 1) + t, 0, exchange(z_par, 1), here(exchange(bias, 1)), 0)
            own = (n_own * me + t, 0, z_own, here(bias), 0)
            two = exchange(far2, 2)
            three = [exchange(v, 3) for v in far3[:2]]
            held.append((two, three))
            if last:
                out, *away = attention([own, (0, 0, far3[-1], here(bias), 0)], out,
                                       masks[3][t][None, SOME:].astype(jnp.int32))
                away = [exchange(v, 3) for v in away]
            else:
                out, = attention([own, near], out)

        def rows_of(t, r, blocks, x_far, xi):
            return ordered(functools.partial(r_call, blocks), [me, n_own * (me ^ r) + t, far.index((t, r))],
                           zt, x_near, x_far, xi, norms, w_sq, w_bias8)

        for t in range(n_own - 1):
            two, (three,) = held[t]
            z_two, mine_two = rows_of(t, 2, 1, two, two)
            z_three, mine_three = rows_of(t, 3, 1, three, three)
            par_two, par_three = exchange(mine_two, 1), exchange(mine_three, 1)
            jobs = [(n_own * (me ^ r) + t, me, z, [(mine, 0), (par, 0), (mine, 1), (par, 1)], 0)
                    for r, z, mine, par in ((2, z_two, mine_two, par_three), (3, z_three, mine_three, par_two))]
            out, = attention(([] if t else [near]) + jobs, out)
        two, three = held[t + 1]
        z_two, mine = rows_of(t + 1, 2, 3, two, two)
        par = exchange(mine, 1)
        out, = attention([(n_own * (me ^ 2) + t + 1, me, z_two, [(mine, k) for k in (0, 3, 1, 2)], 0)], out)
        z_three, = rows_of(t + 1, 3, 0, three[1], three[0])
        out, = attention([(n_own * (me ^ 3) + t + 1, me, z_three, [(par, k) for k in (3, 0, 2, 1)], 0)], out)
        for v, start in zip(away, (SOME, SOME + AWAY_FIRST)):
            out = lax.dynamic_update_slice(out, v[None], (n_own * (me ^ 3) + n_own - 1, start, 0, 0))
        return jnp.transpose(out, (0, 1, 3, 2))

    pair_spec = P('data', 'dap')
    return jax.shard_map(local_block, mesh=mesh, in_specs=(pair_spec, pair_spec) + (P(),) * 28,
                         out_specs=pair_spec, check_vma=False)
```

```python
import functools

import jax
import jax.numpy as jnp
from jax import lax
from jax.experimental import pallas as pl
from jax.experimental.pallas import tpu as pltpu
from jax.sharding import PartitionSpec as P


LN_EPS = 1e-5
F32, BF16 = jnp.float32, jnp.bfloat16
ROWS, CH, COLS = 64, 64, 256
TILE = 16
MIB = 1 << 20
OUT, IN, ATT = range(3)


def channel_stats(vals):
    ch_mean = jnp.mean(vals, axis=0, keepdims=True)
    ch_var = jnp.mean(jnp.square(vals - ch_mean), axis=0, keepdims=True)
    return ch_mean, lax.rsqrt(ch_var + LN_EPS)


def channel_norm(vals, norm, stats=None):
    gain, shift = norm
    ch_mean, scale = channel_stats(vals) if stats is None else stats
    return (vals - ch_mean) * scale * gain + shift


def sigmoid(vals):
    return 0.5 * jnp.tanh(0.5 * vals) + 0.5


def swap_major(vals):
    return jnp.swapaxes(vals, 0, 1)


def pair_of(ref, place):
    return ref.at[2 * place], ref.at[2 * place + 1]


def norm_of(ref, place):
    return [part[:] for part in pair_of(ref, place)]


def contract(lhs, rhs, axis_id):
    return lax.dot_general(lhs, rhs, (((axis_id,), (axis_id,)), ((), ())), preferred_element_type=F32)


def mm(lhs, rhs):
    return jnp.dot(lhs, rhs, preferred_element_type=F32)


def opened(gate, product):
    return (jnp.tanh(gate) + 1.0) * product


def row_at(base, i):
    return pl.ds(base + i, 1)


def ab_row(proj, tile_a, tile_b, slot):
    for n, tile in enumerate((tile_a, tile_b)):
        linear, gate = jnp.split(proj[2 * CH * n:2 * CH * n + 2 * CH], 2)
        tile[slot] = opened(gate, linear).astype(BF16)


def x_norm_tile(x_s, tile_x, base, xg, xb):
    parts = [(sub, half) for sub in range(2) for half in range(2)]

    def load(c, part):
        return x_s[c, pl.ds(pl.multiple_of(base + 8 * part[0], 8), 8), 128 * part[1]:128 * part[1] + 128]

    means = [sum(load(c, p) for c in range(CH)) * (1.0 / CH) for p in parts]
    scales = [lax.rsqrt(sum(jnp.square(load(c, p) - means[n]) for c in range(CH)) * (1.0 / CH) + LN_EPS)
              for n, p in enumerate(parts)]
    for c in range(CH):
        rows = []
        for sub in range(2):
            rows.append(jnp.concatenate(
                [(load(c, (sub, half)) - means[2 * sub + half]) * scales[2 * sub + half] * xg[c] + xb[c]
                 for half in range(2)], axis=1))
        tile_x[c] = jnp.concatenate(rows).astype(BF16)


LAG = 3


def staggered(count, *stages):
    held = [{} for _ in stages]
    for tick in range(count + LAG * (len(stages) - 1)):
        for k, stage in enumerate(stages):
            i = tick - LAG * k
            if 0 <= i < count:
                held[k][i] = stage(i, held[k - 1].pop(i) if k else None)


def u_kernel(last, layout, sc, *refs):
    z_refs = refs[:len(layout)]
    n_far = 3 if last else 1
    (mask0, mask1, mask2, mask3, norms, xgs, w_ab, w_sq, w_bias, z2_own, z2_par, bias_out, far2, *far3) = refs[len(layout):][:13 + n_far]
    (z_s, a_s, b_s, x_s, mask, stats, tile_a, tile_b, tile_x, tile_c, tile_d, tile_z, in_sem, z_sem, x_sem) = refs[len(layout) + 13 + n_far:]
    me, sample = sc[0], sc[1]
    lanes = pl.ds(pl.multiple_of(LANES * (me // 2), LANES), LANES)
    out_norm = norm_of(norms, OUT)
    in_norm = norm_of(norms, IN)
    att_norm = norm_of(norms, ATT)
    n_tiles = COLS // TILE

    for ref, (r, start) in zip(z_refs, layout):
        src = ref if r else ref.at[sample]
        rows = pl.ds(pl.multiple_of(ROWS * (me ^ r) + start, 8), src.shape[0])
        pltpu.make_async_copy(src, z_s.at[rows], in_sem.at[r]).start()
    for r, part in enumerate((mask0, mask1, mask2, mask3)):
        mask[pl.ds(pl.multiple_of(ROWS * (me ^ r), ROWS), ROWS), :] = part[:].astype(F32)

    def gate_and_product(place, normed, product):
        gate, proj = pair_of(w_sq, place)
        return mm(gate[:], normed), mm(proj[:], product)

    def mask_row(base, i):
        return mask[row_at(base, i), :]

    def measure(base, i, vals=None):
        found = channel_stats(z_s[base + i] if vals is None else vals)
        for n in range(2):
            stats[n if vals is None else n + 2, row_at(base, i), :] = found[n]
        return found

    def recall(base, i, first):
        return [stats[first + n, row_at(base, i), :] for n in range(2)]

    def flush(base):
        a_s[:, pl.ds(base, TILE), :] = swap_major(tile_a[:])
        b_s[:, pl.ds(base, TILE), :] = swap_major(tile_b[:])

    def export(t, start, outgoing, sem):
        r = (t * TILE // ROWS) ^ me
        q = t % (ROWS // TILE)
        rows = pl.ds(pl.multiple_of(TILE * q, TILE), TILE)
        half = pl.ds(pl.multiple_of(ROWS + TILE * (q % 2), TILE), TILE)
        side = pl.ds(pl.multiple_of(LANES * (q // 2), LANES), LANES)
        act = (lambda cp: cp.start()) if start else (lambda cp: cp.wait())
        wide, z_tile = tile_c.at[t % 2], tile_z.at[t % 2]
        narrow = tile_c.at[t % 2, :, :, lanes]
        jobs = [(r == 2, narrow, far2.at[half, :, side])] if outgoing else [
            (r == 0, z_tile, z2_own.at[rows]), (r == 1, z_tile, z2_par.at[rows]), (r == 2, wide, far2.at[rows])]
        if last:
            near_rows, away_rows = (pl.ds(pl.multiple_of(TILE * row, TILE), TILE)
                                    for row in (jnp.minimum(q, CHUNKS - 1), jnp.maximum(q - CHUNKS, 0)))
            jobs += [((r == 3) & (q < CHUNKS), *((narrow, far3[1].at[near_rows]) if outgoing else (wide, far3[0].at[near_rows])))]
            if not outgoing:
                jobs += [((r == 3) & (q >= CHUNKS), z_tile, far3[-1].at[away_rows])]
        else:
            jobs += [(r == 3, narrow, far3[0].at[half, :, side]) if outgoing else (r == 3, wide, far3[0].at[rows])]
        for when, src, dst in jobs:
            @pl.when(when)
            def _():
                act(pltpu.make_async_copy(src, dst, sem.at[t % 2]))

    @pl.loop(0, n_tiles)
    def _(v):
        r = v * TILE // ROWS

        @pl.when(v * TILE % ROWS == 0)
        def _():
            pltpu.make_async_copy(z_refs[0].at[sample], z_s.at[pl.ds(0, ROWS)], in_sem.at[r]).wait()

        base = pl.multiple_of(ROWS * (me ^ r) + v * TILE % ROWS, TILE)
        staggered(
            TILE,
            lambda i, _: mm(w_ab[OUT], (mask_row(base, i) * channel_norm(z_s[base + i], out_norm, measure(base, i))).astype(BF16)),
            lambda i, proj: ab_row(proj, tile_a, tile_b, i))
        flush(base)

    @pl.loop(0, CH, unroll=16)
    def _(c):
        x_s[c] = contract(a_s[c], b_s[c], 1)

    @pl.loop(0, n_tiles)
    def _(t):
        base = pl.multiple_of(TILE * t, TILE)

        @pl.when(t >= 2)
        def _():
            export(t - 2, False, True, x_sem)

        x_norm_tile(x_s, tile_x, base, *pair_of(xgs, OUT))
        tile_c[t % 2] = swap_major(tile_x[:])

        def gate_and_update(i, _):
            normed = channel_norm(z_s[base + i], out_norm, recall(base, i, 0)).astype(BF16)
            return gate_and_product(OUT, normed, tile_c[t % 2, i])

        def next_norm(i, parts):
            z_one = z_s[base + i] + opened(*parts)
            tile_z[0, i] = z_one
            return (mask_row(base, i) * channel_norm(z_one, in_norm, measure(base, i, z_one))).astype(BF16)

        staggered(TILE, gate_and_update, next_norm, lambda i, normed: mm(w_ab[IN], normed),
                  lambda i, proj: ab_row(proj, tile_a, tile_b, i))
        flush(base)
        z_s[pl.ds(base, TILE)] = tile_z[0]
        export(t, True, True, x_sem)

    for t in (n_tiles - 2, n_tiles - 1):
        export(t, False, True, x_sem)

    @pl.loop(0, CH, unroll=16)
    def _(c):
        x_s[c] = contract(a_s[c], b_s[c], 0)

    @pl.loop(0, n_tiles)
    def _(t):
        base = pl.multiple_of(TILE * t, TILE)

        @pl.when(t >= 2)
        def _():
            export(t - 2, False, False, z_sem)

        x_norm_tile(x_s, tile_x, base, *pair_of(xgs, IN))
        tile_c[t % 2] = swap_major(tile_x[:])

        def gate_and_update(i, _):
            normed = channel_norm(z_s[base + i], in_norm, recall(base, i, 2)).astype(BF16)
            return gate_and_product(IN, normed, tile_c[t % 2, i])

        def next_norm(i, parts):
            z_two = z_s[base + i] + opened(*parts)
            tile_z[t % 2, i] = z_two
            return channel_norm(z_two, att_norm).astype(BF16)

        def bias_row(i, normed):
            tile_d[i] = mm(w_bias[:], normed)

        staggered(TILE, gate_and_update, next_norm, bias_row)
        rows = pl.ds(pl.multiple_of(t * TILE % ROWS, TILE), TILE)
        bias_out[t * TILE // ROWS, :, rows, :] = swap_major(tile_d[:])[:4].astype(BF16)
        export(t, True, False, z_sem)

    bias_to = ((far2, 0, 0), (far2, 1, 1), (far2, 3, 2)) if last else ((far2, 0, 0), (far3[0], 1, 0))

    def bias_copy(n):
        dst, block, place = bias_to[n]
        return pltpu.make_async_copy(bias_out.at[me ^ block], dst.at[pl.ds(FAR_BIAS + 4 * place, 4)], in_sem.at[n])

    for n in range(len(bias_to)):
        bias_copy(n).start()
    for t in (n_tiles - 2, n_tiles - 1):
        export(t, False, False, z_sem)
    for n in range(len(bias_to)):
        bias_copy(n).wait()


LANES = 128
VM = pl.BlockSpec(memory_space=pltpu.VMEM)
HB = pl.BlockSpec(memory_space=pltpu.HBM)
SDS = jax.ShapeDtypeStruct
AT_FIRST = lambda i, *_: (i, 0, 0, 0)
SM = pl.BlockSpec(memory_space=pltpu.SMEM)
PARAMS = pltpu.CompilerParams(vmem_limit_bytes=40 * MIB, dimension_semantics=("arbitrary",))
AB_TILE = pltpu.VMEM((TILE, CH, COLS), BF16)
DMA2 = pltpu.SemaphoreType.DMA((2,))
FAR_BIAS = ROWS + ROWS // 2
FAR = SDS((FAR_BIAS + 4, CH, COLS), BF16)
CHUNKS = 2
SOME = CHUNKS * TILE
AWAY = SDS((ROWS - SOME, CH, COLS), F32)
SOME_FULL = SDS((SOME, CH, COLS), BF16)
SOME_HALF = SDS((SOME, CH, LANES), BF16)
FAR_LAST = SDS((FAR_BIAS + 12, CH, COLS), BF16)
ROW_WIDE = SDS((ROWS, CH, COLS), F32)
SAMPLE_BF = pltpu.VMEM((CH, COLS, COLS), BF16)


def u_call(last, layout, sc, z_parts, masks, norms, xgs, w_ab, w_sq, w_bias):
    return pl.pallas_call(
        functools.partial(u_kernel, last, layout),
        out_shape=(ROW_WIDE, ROW_WIDE, SDS((4, 4, ROWS, COLS), BF16), *((FAR_LAST, SOME_FULL, SOME_HALF, AWAY) if last else (FAR, FAR))),
        in_specs=[SM] + [HB] * len(layout) + [VM] * 9,
        out_specs=(HB, HB, VM) + (HB,) * (4 if last else 2),
        scratch_shapes=[
            pltpu.VMEM((COLS, CH, COLS), F32), SAMPLE_BF, SAMPLE_BF,
            pltpu.VMEM((CH, COLS, COLS), F32), pltpu.VMEM((COLS, COLS), F32), pltpu.VMEM((4, COLS, COLS), F32), AB_TILE, AB_TILE, pltpu.VMEM((CH, TILE, COLS), BF16), pltpu.VMEM((2, TILE, CH, COLS), BF16),
            pltpu.VMEM((TILE, 8, COLS), F32), pltpu.VMEM((2, TILE, CH, COLS), F32),
            pltpu.SemaphoreType.DMA((4,)), DMA2, DMA2,
        ],
        compiler_params=pltpu.CompilerParams(vmem_limit_bytes=62 * MIB),
        name="pair_updates",
    )(sc, *z_parts, *masks, norms, xgs, w_ab, w_sq, w_bias)


def l1_kernel(ids, z_in, mask_in, norms, w_ab, a_out, b_out, mask, tile_a, tile_b):
    out_norm = norm_of(norms, OUT)
    mask[:] = mask_in[0].astype(F32)

    @pl.loop(0, ROWS // TILE)
    def _(t):
        base = pl.multiple_of(TILE * t, TILE)
        staggered(
            TILE,
            lambda i, _: mm(w_ab[OUT], (mask[row_at(base, i), :] * channel_norm(z_in[0, base + i], out_norm)).astype(BF16)),
            lambda i, proj: ab_row(proj, tile_a, tile_b, i))
        a_out[0, :, pl.ds(base, TILE), :] = swap_major(tile_a[:])
        b_out[0, :, pl.ds(base, TILE), :] = swap_major(tile_b[:])


def l1_call(ids, zt, mask, norms, w_ab):
    n = ids.shape[0]
    ab = SDS((n, CH, ROWS, COLS), BF16)
    ab_spec = pl.BlockSpec((1, CH, ROWS, COLS), AT_FIRST)
    return pl.pallas_call(
        l1_kernel,
        out_shape=(ab, ab),
        grid_spec=pltpu.PrefetchScalarGridSpec(
            num_scalar_prefetch=1, grid=(n,),
            in_specs=[pl.BlockSpec((1, ROWS, CH, COLS), lambda i, ids: (ids[i], 0, 0, 0)),
                      pl.BlockSpec((1, ROWS, COLS), lambda i, ids: (ids[i], 0, 0)), VM, VM],
            out_specs=(ab_spec, ab_spec),
            scratch_shapes=[pltpu.VMEM((ROWS, COLS), F32), AB_TILE, AB_TILE]),
        compiler_params=PARAMS,
        name="near_projections",
    )(ids, zt, mask, norms, w_ab)


def l2_kernel(sc, a_in, b_own, b_par, xgs, x_out, x_s, tile_x):
    odd = sc[0] % 2 == 1

    @pl.loop(0, CH, unroll=2)
    def _(c):
        for n in range(2):
            own, par = b_own[n, c].astype(F32), b_par[1 - n, c].astype(F32)
            pair = jnp.concatenate([jnp.where(odd, par, own), jnp.where(odd, own, par)]).astype(BF16)
            x_s[c, :, LANES * n:LANES * n + LANES] = contract(a_in[n, c], pair, 1)

    @pl.loop(0, ROWS // TILE)
    def _(t):
        base = pl.multiple_of(TILE * t, TILE)
        x_norm_tile(x_s, tile_x, base, *pair_of(xgs, OUT))
        both = swap_major(tile_x[:])
        for n in range(2):
            x_out[n, pl.ds(base, TILE)] = both[:, :, LANES * n:LANES * n + LANES]


def l2_call(sc, a_all, b_own, b_par, xgs):
    n = a_all.shape[0]
    ab_spec = pl.BlockSpec((2, CH, ROWS, COLS), AT_FIRST)
    return pl.pallas_call(
        l2_kernel,
        grid=(n // 2,),
        out_shape=SDS((n, ROWS, CH, LANES), BF16),
        in_specs=[SM, ab_spec, ab_spec, ab_spec, VM],
        out_specs=pl.BlockSpec((2, ROWS, CH, LANES), AT_FIRST),
        scratch_shapes=[pltpu.VMEM((CH, ROWS, COLS), F32), pltpu.VMEM((CH, TILE, COLS), BF16)],
        compiler_params=PARAMS,
        name="near_product",
    )(sc, a_all, b_own, b_par, xgs)


def r_kernel(blocks, sc, z_in, x_near, x_far, xi, *refs):
    bias_far, refs = (refs[0], refs[1:]) if blocks else (None, refs)
    norms, w_sq, w_bias, z_out, *refs = refs
    swap, refs = (refs[0], refs[1:]) if blocks else (None, refs)
    tile_d, tile_z, z_buf, sem = refs
    step, steps = pl.program_id(0), pl.num_programs(0)
    first = sc[0] < 2
    out_norm, in_norm, att_norm = [norm_of(norms, place) for place in (OUT, IN, ATT)]

    def z_copy(n):
        return pltpu.make_async_copy(z_buf.at[n % 2], z_out.at[pl.ds(pl.multiple_of(n * TILE, TILE), TILE)], sem.at[n % 2])

    @pl.when(step >= 2)
    def _():
        z_copy(step - 2).wait()

    def gate_and_product(place, normed, product):
        gate, proj = pair_of(w_sq, place)
        return mm(gate[:], normed), mm(proj[:], product)

    def outgoing(i, _):
        near, far = x_near[0, i].astype(F32), x_far[i].astype(F32)
        xn = jnp.concatenate([jnp.where(first, near, far), jnp.where(first, far, near)], axis=1).astype(BF16)
        return gate_and_product(OUT, channel_norm(z_in[0, i], out_norm).astype(BF16), xn)

    def norm_one(i, parts):
        z_one = z_in[0, i] + opened(*parts)
        tile_z[i] = z_one
        return channel_norm(z_one, in_norm).astype(BF16)

    def incoming(i, normed):
        return gate_and_product(IN, normed, xi[i])

    def norm_two(i, parts):
        z_two = tile_z[i] + opened(*parts)
        z_buf[step % 2, i] = z_two
        return channel_norm(z_two, att_norm).astype(BF16) if blocks else None

    def bias_row(i, normed):
        tile_d[i] = mm(w_bias[:], normed)

    staggered(TILE, outgoing, norm_one, incoming, norm_two, *([bias_row] if blocks else []))
    z_copy(step).start()
    if blocks:
        swap[0, :, pl.ds(pl.multiple_of(step * TILE, TILE), TILE), :] = swap_major(tile_d[:])[:4].astype(BF16)

        @pl.when(step == 0)
        def _():
            for n in range(blocks):
                swap[n + 1] = bias_far[4 * n:4 * n + 4]

    @pl.when(step == steps - 1)
    def _():
        z_copy(step - 1).wait()
        z_copy(step).wait()


def r_call(blocks, sc, zt, x_near, x_far, xi, norms, w_sq, w_bias):
    steps = ROWS // TILE if blocks else CHUNKS
    far_map = (lambda i, sc: (ROWS // TILE + i % 2, 0, i // 2)) if blocks else (lambda i, sc: (i, 0, 0))
    return pl.pallas_call(
        functools.partial(r_kernel, blocks),
        out_shape=[pltpu.HBM((steps * TILE, CH, COLS), F32)] + [pltpu.HBM((blocks + 1, 4, ROWS, COLS), BF16)] * (blocks > 0),
        grid_spec=pltpu.PrefetchScalarGridSpec(
            num_scalar_prefetch=1, grid=(steps,),
            in_specs=[pl.BlockSpec((1, TILE, CH, COLS), lambda i, sc: (sc[1], i, 0, 0)),
                      pl.BlockSpec((1, TILE, CH, LANES), lambda i, sc: (sc[2], i, 0, 0)),
                      pl.BlockSpec((TILE, CH, LANES), far_map), pl.BlockSpec((TILE, CH, COLS), lambda i, sc: (i, 0, 0)),
                      *[pl.BlockSpec((4 * blocks, CH, COLS), lambda i, sc: (FAR_BIAS // (4 * blocks), 0, 0))] * (blocks > 0),
                      VM, VM, VM],
            out_specs=[HB] + [pl.BlockSpec((blocks + 1, 4, ROWS, COLS), lambda i, sc: (0, 0, 0, 0))] * (blocks > 0),
            scratch_shapes=[pltpu.VMEM((TILE, 8, COLS), F32), pltpu.VMEM((TILE, CH, COLS), F32),
                            pltpu.VMEM((2, TILE, CH, COLS), F32), DMA2]),
        compiler_params=PARAMS,
        name="row_updates",
    )(sc, zt, x_near, x_far, xi, *[xi] * (blocks > 0), norms, w_sq, w_bias)


HEADS, HEAD = 4, 16
MASK_FILL = -1e9
CHUNK = 32
SLOTS = 2
STEPS = 6
AWAY_FIRST = 24
HEAD_ROWS = 8


def attention_kernel(parts, fresh, away, sc, *refs):
    n = len(parts)
    z_refs, bias_refs, (mask_in, norms, w_all, w_proj, *rest) = refs[:n], refs[n:5 * n], refs[5 * n:]
    mask_away, rest = (rest[0], rest[1:]) if away else (None, rest)
    out, *rest = rest if fresh else rest[1:]
    out_away, rest = (rest[:2], rest[2:]) if away else ((), rest)
    (z_in, z_out, mask_i, mask, bias_in, bias_t, q_s, k_s, v_s, g_s, vn_s, gn_s, keep_s, s_buf, e_buf, p_s,
     top_s, inv_s, o_s, m_sem, z_sem, o_sem, b_sem) = rest
    n_rows = sum(size for _, size, _ in parts)
    att_norm = norm_of(norms, 0)

    def rows_of(j):
        return pl.ds(ROWS * j, parts[j][1])

    def own(ref, j):
        return ref.at[sc[j], pl.ds(*parts[j][:2])]

    def z_copy(j):
        start = 0 if j else HEAD_ROWS
        size = parts[j][1] - start
        return pltpu.make_async_copy(z_refs[j].at[pl.ds(start, size)], z_in.at[pl.ds(ROWS * j + start, size)], z_sem.at[j])

    def head_copy():
        return pltpu.make_async_copy(z_refs[0].at[pl.ds(0, HEAD_ROWS)], z_in.at[pl.ds(0, HEAD_ROWS)], z_sem.at[n])

    def m_copy(j):
        src = mask_away.at[0] if away and j == n - 1 else own(mask_in, j)
        return pltpu.make_async_copy(src, mask_i.at[rows_of(j)], m_sem.at[j])

    def b_copy(j, r):
        rows = pl.ds(pl.multiple_of(ROWS * (sc[n + j] ^ r), ROWS), ROWS)
        return pltpu.make_async_copy(bias_refs[4 * j + r].at[parts[j][2][r]], bias_in.at[j, :, rows], b_sem.at[j])

    def o_copies(j):
        first, size, _ = parts[j]
        cuts = (0, size) if j < n - 1 else (0, AWAY_FIRST if away else size - TILE, size)
        pieces = []
        for k, (start, stop) in enumerate(zip(cuts, cuts[1:])):
            dst = out_away[k] if away and j == n - 1 else out.at[sc[j], pl.ds(first + start, stop - start)]
            src = z_out.at[pl.ds(ROWS * j + start, stop - start)]
            pieces.append((ROWS * j + stop, pltpu.make_async_copy(src, dst, o_sem.at[j])))
        return pieces

    starts = [f(j) for j in range(n) for f in (m_copy, *(functools.partial(b_copy, r=r) for r in range(4)))]
    for copy in starts + [head_copy()] + [z_copy(j) for j in range(n)]:
        copy.start()
    for copy in starts:
        copy.wait()
    mask[:] = mask_i[:].astype(F32)
    q_s[:] = jnp.zeros_like(q_s)

    @pl.loop(0, n * HEADS, unroll=4)
    def _(h):
        bias_t[h // HEADS, h % HEADS] = bias_in[h // HEADS, h % HEADS].astype(F32).T

    head_copy().wait()

    def project(row, slot):
        row = jnp.minimum(row, n_rows - 1)
        normed = channel_norm(z_in[row], att_norm).astype(BF16)
        proj = mm(w_all[:], normed)
        k_s[slot] = proj[CH:2 * CH].T.astype(BF16)
        q = proj[:CH].astype(BF16)
        for h in range(HEADS):
            q_s[slot, h, HEAD * h:HEAD * h + HEAD] = q[HEAD * h:HEAD * h + HEAD]
        vn_s[slot] = proj[2 * CH:3 * CH].astype(BF16)
        gn_s[slot] = sigmoid(proj[3 * CH:])

    def keep_mask(row, slot):
        row = jnp.minimum(row, n_rows - 1)
        keep_s[slot] = jnp.broadcast_to(mask[pl.ds(row, 1), :], (LANES, COLS)).T

    def tall(line):
        return jnp.concatenate([line] * (CHUNK // 8))

    def fold(part, op):
        out = part[:8]
        for n in range(1, part.shape[0] // 8):
            out = op(out, part[8 * n:8 * n + 8])
        return out

    def scores(slot, h):
        return mm(k_s[slot], q_s[slot, h])

    def weigh(slot, h, probs):
        heads = slice(HEAD * h, HEAD * h + HEAD)
        o_s[slot, heads] = mm(v_s[slot, heads], probs)

    def step(row, slot, h, logits, defer):
        buf, prev = h % 2, (h + 1) % 2
        sample = jnp.clip(row, 0, n_rows - 1) // ROWS
        top, total, probs = None, None, []
        for c in range(COLS // CHUNK):
            rows = slice(CHUNK * c, CHUNK * c + CHUNK)
            probs.append((e_buf[buf, rows] * tall(inv_s[buf])).astype(BF16))
            exps = jnp.exp(s_buf[prev, rows] - tall(top_s[prev]))
            e_buf[prev, rows] = exps
            part = fold(exps, jnp.add)
            total = part if total is None else total + part
            keep = keep_s[slot, rows]
            keep = jnp.concatenate([keep, keep], axis=1) > 0
            vals = jnp.where(keep, logits[rows] + bias_t[sample, h, rows], MASK_FILL)
            s_buf[buf, rows] = vals
            part = fold(vals, jnp.maximum)
            top = part if top is None else jnp.maximum(top, part)
        top_s[buf] = jnp.broadcast_to(jnp.max(top, axis=0, keepdims=True), (8, COLS))
        inv_s[prev] = jnp.broadcast_to(1.0 / jnp.sum(total, axis=0, keepdims=True), (8, COLS))
        if defer:
            p_s[:] = jnp.concatenate(probs)
        else:
            weigh(1 - slot if h < 2 else slot, (h - 2) % HEADS, jnp.concatenate(probs))

    def finish(row, slot):
        gated = (g_s[slot] * o_s[slot]).astype(BF16)
        z_out[jnp.maximum(row, 0)] = z_in[jnp.clip(row, 0, n_rows - 1)] + mm(w_proj[:], gated)

    project(0, 0)
    keep_mask(0, 0)
    n_steps = (n_rows + 2 + STEPS - 1) // STEPS

    @pl.loop(0, n_steps)
    def _(it):
        first = STEPS * it - 1
        lg = scores(1, 0)
        weigh(0, 1, p_s[:])
        for k in range(STEPS):
            row, slot, last = first + k, 1 - k % 2, k == STEPS - 1
            for h in range(HEADS):
                nxt = scores(slot, h + 1) if h < HEADS - 1 else (None if last else scores(1 - slot, 0))
                if h == 2:
                    project(row + 2, slot)
                step(row, slot, h, lg, last and h == HEADS - 1)
                lg = nxt
                if h == 3:
                    finish(row - 1, 1 - slot)
                    v_s[1 - slot] = vn_s[1 - slot]
                    g_s[1 - slot] = gn_s[1 - slot]
            keep_mask(row + 2, slot)
        for j in range(n):
            @pl.when(it == max((ROWS * j - 1) // STEPS - 1, 0))
            def _():
                z_copy(j).wait()

            for stop, copy in o_copies(j):
                if stop < n_rows:
                    @pl.when(it == (stop + 1) // STEPS)
                    def _():
                        copy.start()

    for stop, copy in o_copies(n - 1):
        if stop == n_rows:
            copy.start()
    for j in range(n):
        for _, copy in o_copies(j):
            copy.wait()


def attend(static, sc, z_parts, biases, mask, norms, w_all, w_proj, out, mask_away=None):
    n, fresh, away = len(z_parts), out is None, mask_away is not None
    z_parts, biases = jax.tree.map(lambda v: pltpu.with_memory_space_constraint(v, pltpu.HBM), (list(z_parts), list(biases)))
    args = (sc, *z_parts, *biases, mask, norms, w_all, w_proj, *[mask_away] * away, *[out] * (not fresh))
    whole = SDS((mask.shape[0], ROWS, CH, COLS), F32)
    aways = [SDS((k, CH, COLS), F32) for k in (AWAY_FIRST, AWAY.shape[0] - AWAY_FIRST)] * away
    rows = sum(z.shape[0] for z in z_parts)
    pair, wide, square, line = [pltpu.VMEM((SLOTS, *shape), dtype) for shape, dtype in (
        ((CH, COLS), BF16), ((CH, COLS), F32), ((COLS, COLS), F32), ((8, COLS), F32))]
    each = [pltpu.VMEM((n, HEADS, COLS, COLS), dtype) for dtype in (BF16, F32)]
    sems, more = pltpu.SemaphoreType.DMA((n,)), pltpu.SemaphoreType.DMA((n + 1,))
    return pl.pallas_call(
        functools.partial(attention_kernel, static, fresh, away),
        out_shape=(whole, *aways),
        in_specs=[SM] + [HB] * (5 * n + 1) + [VM] * 3 + [HB] * (away + (not fresh)),
        out_specs=(HB,) * (1 + len(aways)),
        scratch_shapes=[
            pltpu.VMEM((rows, CH, COLS), F32), pltpu.VMEM((rows + STEPS, CH, COLS), F32), pltpu.VMEM((rows, COLS), jnp.int32),
            pltpu.VMEM((rows, COLS), F32), *each, pltpu.VMEM((SLOTS, HEADS, CH, COLS), BF16),
            pltpu.VMEM((SLOTS, COLS, CH), BF16), pair, wide, pair, wide, pltpu.VMEM((SLOTS, COLS, LANES), F32),
            square, square, pltpu.VMEM((COLS, COLS), BF16), line, line, wide, sems, more, sems, sems,
        ],
        compiler_params=pltpu.CompilerParams(vmem_limit_bytes=48 * MIB),
        input_output_aliases={} if fresh else {len(args) - 1: 0},
        name="triangle_attention",
    )(*args)


FIRST = 8


def exchange(values, r):
    return lax.ppermute(values, 'dap', [(i, i ^ r) for i in range(4)])


def update_weights(params):
    norm_gain, norm_bias, w_a, w_agate, w_b, w_bgate, w_gate, x_gain, x_bias, w_proj = params
    half = jnp.bfloat16(0.5)
    wide = lambda v: jnp.broadcast_to(v[:, None], (CH, COLS))
    deep = lambda v: jnp.broadcast_to(v[:, None, None], (CH, 8, 128))
    return ([wide(norm_gain), wide(norm_bias)], [deep(x_gain), deep(x_bias)],
            half * jnp.concatenate([w_a.T, w_agate.T, w_b.T, w_bgate.T]), [half * w_gate.T, half * w_proj.T])


def solution(mesh):
    def local_block(pair_z, pair_mask, *weights):
        me = lax.axis_index('dap')
        zt = jnp.transpose(pair_z, (0, 1, 3, 2))
        n_own = zt.shape[0] // 4
        mask_bf = pair_mask.astype(BF16)
        arrived, layouts, before = [], [], ()
        for t in range(n_own):
            pieces = [(2, 0, FIRST), (2, FIRST, ROWS)] if t == 0 else [(2, 0, ROWS)]
            pieces += [(3, 0, ROWS), (1, 0, ROWS)]
            got = []
            for r, start, stop in pieces:
                where = (n_own * (me ^ r) + t, start, 0, 0)
                send = lax.dynamic_slice(lax.optimization_barrier((zt, *before))[0], where, (1, stop - start, CH, COLS))[0]
                if t == 0 or r == 1:
                    before = (send,)
                got.append(exchange(send, r))
                if t == 0 and stop == ROWS and r == 2:
                    mask_bf, weights = lax.optimization_barrier((mask_bf, weights, send))[:2]
                    masks = [lax.dynamic_slice_in_dim(mask_bf, n_own * (me ^ k), n_own) for k in range(4)]
                    before = (*before, *masks)
                    masks = [exchange(m, k) if k else m for k, m in enumerate(masks)]
            arrived.append([zt, *got])
            layouts.append(((0, 0), *((r, start) for r, start, _ in pieces)))

        out_n, out_x, out_ab, out_sq = update_weights(weights[:10])
        in_n, in_x, in_ab, in_sq = update_weights(weights[10:20])
        att_gain, att_shift, w_q, w_k, w_v, w_bias, w_gate, w_proj = weights[20:]
        att_n = [jnp.broadcast_to(v[:, None], (CH, COLS)) for v in (att_gain, att_shift)]
        norms = jnp.stack(out_n + in_n + att_n)
        xgs = jnp.stack(out_x + in_x)
        w_ab = jnp.stack([out_ab, in_ab])
        w_sq = jnp.stack(out_sq + in_sq)
        w_bias8 = jnp.concatenate([w_bias.T, jnp.zeros((4, CH), BF16)])
        w_all = jnp.concatenate([w_q.T * jnp.bfloat16(HEAD ** -0.5), w_k.T, w_v.T, w_gate.T])
        w_out = w_proj.T
        att_norms = norms[4:]

        token = [None]

        def ordered(call, sc, *args):
            sc = jnp.stack([jnp.asarray(v, jnp.int32) for v in sc])
            if token[0] is not None:
                sc = lax.optimization_barrier((sc, token[0]))[0]
            res = call(sc, *args)
            token[0] = jax.tree.leaves(res)[-1]
            return res

        def attention(jobs, out, mask_away=None):
            samples, orders, z_parts, biases, starts = zip(*jobs)
            static = tuple((start, z.shape[0], tuple(place for _, place in blocks))
                           for start, z, blocks in zip(starts, z_parts, biases))
            arrays = [array for blocks in biases for array, _ in blocks]
            return ordered(functools.partial(attend, static), samples + orders, z_parts, arrays, pair_mask, att_norms,
                           w_all, w_out, out, mask_away)

        far = [(t, r) for t in range(n_own) for r in (2, 3)]
        a_far, b_far = ordered(l1_call, [n_own * (me ^ r) + t for t, r in far], zt, pair_mask, norms, w_ab)
        b_par = exchange(b_far, 1)
        x_near = ordered(l2_call, [me], a_far, b_far, b_par, xgs)

        out = None
        held = []
        for t in range(n_own):
            last = t == n_own - 1
            z_own, z_par, bias, far2, *far3 = ordered(functools.partial(u_call, last, layouts[t]), [me, n_own * me + t],
                                                      arrived[t], [m[t] for m in masks], norms, xgs, w_ab, w_sq, w_bias8)
            here = lambda array: [(array, r) for r in range(4)]
            near = (n_own * (me ^ 1) + t, 0, exchange(z_par, 1), here(exchange(bias, 1)), 0)
            own = (n_own * me + t, 0, z_own, here(bias), 0)
            two = exchange(far2, 2)
            three = [exchange(v, 3) for v in far3[:2]]
            held.append((two, three))
            if last:
                out, *away = attention([own, (0, 0, far3[-1], here(bias), 0)], out,
                                       masks[3][t][None, SOME:].astype(jnp.int32))
                away = [exchange(v, 3) for v in away]
            else:
                out, = attention([own, near], out)

        def rows_of(t, r, blocks, x_far, xi):
            return ordered(functools.partial(r_call, blocks), [me, n_own * (me ^ r) + t, far.index((t, r))],
                           zt, x_near, x_far, xi, norms, w_sq, w_bias8)

        for t in range(n_own - 1):
            two, (three,) = held[t]
            z_two, mine_two = rows_of(t, 2, 1, two, two)
            z_three, mine_three = rows_of(t, 3, 1, three, three)
            par_two, par_three = exchange(mine_two, 1), exchange(mine_three, 1)
            jobs = [(n_own * (me ^ r) + t, me, z, [(mine, 0), (par, 0), (mine, 1), (par, 1)], 0)
                    for r, z, mine, par in ((2, z_two, mine_two, par_three), (3, z_three, mine_three, par_two))]
            out, = attention(([] if t else [near]) + jobs, out)
        two, three = held[t + 1]
        z_two, mine = rows_of(t + 1, 2, 3, two, two)
        par = exchange(mine, 1)
        out, = attention([(n_own * (me ^ 2) + t + 1, me, z_two, [(mine, k) for k in (0, 3, 1, 2)], 0)], out)
        z_three, = rows_of(t + 1, 3, 0, three[1], three[0])
        out, = attention([(n_own * (me ^ 3) + t + 1, me, z_three, [(par, k) for k in (3, 0, 2, 1)], 0)], out)
        for v, start in zip(away, (SOME, SOME + AWAY_FIRST)):
            out = lax.dynamic_update_slice(out, v[None], (n_own * (me ^ 3) + n_own - 1, start, 0, 0))
        return jnp.transpose(out, (0, 1, 3, 2))

    pair_spec = P('data', 'dap')
    return jax.shard_map(local_block, mesh=mesh, in_specs=(pair_spec, pair_spec) + (P(),) * 28,
                         out_specs=pair_spec, check_vma=False)
```

```python
import functools

import jax
import jax.numpy as jnp
from jax import lax
from jax.experimental import pallas as pl
from jax.experimental.pallas import tpu as pltpu
from jax.sharding import PartitionSpec as P


LN_EPS = 1e-5
F32, BF16 = jnp.float32, jnp.bfloat16
ROWS, CH, COLS = 64, 64, 256
TILE = 16
MIB = 1 << 20
OUT, IN, ATT = range(3)


def channel_stats(vals):
    ch_mean = jnp.mean(vals, axis=0, keepdims=True)
    ch_var = jnp.mean(jnp.square(vals - ch_mean), axis=0, keepdims=True)
    return ch_mean, lax.rsqrt(ch_var + LN_EPS)


def channel_norm(vals, norm, stats=None):
    gain, shift = norm
    ch_mean, scale = channel_stats(vals) if stats is None else stats
    return (vals - ch_mean) * scale * gain + shift


def sigmoid(vals):
    return 0.5 * jnp.tanh(0.5 * vals) + 0.5


def swap_major(vals):
    return jnp.swapaxes(vals, 0, 1)


def pair_of(ref, place):
    return ref.at[2 * place], ref.at[2 * place + 1]


def norm_of(ref, place):
    return [part[:] for part in pair_of(ref, place)]


def contract(lhs, rhs, axis_id):
    return lax.dot_general(lhs, rhs, (((axis_id,), (axis_id,)), ((), ())), preferred_element_type=F32)


def mm(lhs, rhs):
    return jnp.dot(lhs, rhs, preferred_element_type=F32)


def opened(gate, product):
    return (jnp.tanh(gate) + 1.0) * product


def row_at(base, i):
    return pl.ds(base + i, 1)


def ab_row(proj, tile_a, tile_b, slot):
    for n, tile in enumerate((tile_a, tile_b)):
        linear, gate = jnp.split(proj[2 * CH * n:2 * CH * n + 2 * CH], 2)
        tile[slot] = opened(gate, linear).astype(BF16)


def x_norm_tile(x_s, tile_x, base, xg, xb):
    parts = [(sub, half) for sub in range(2) for half in range(2)]

    def load(c, part):
        return x_s[c, pl.ds(pl.multiple_of(base + 8 * part[0], 8), 8), 128 * part[1]:128 * part[1] + 128]

    means = [sum(load(c, p) for c in range(CH)) * (1.0 / CH) for p in parts]
    scales = [lax.rsqrt(sum(jnp.square(load(c, p) - means[n]) for c in range(CH)) * (1.0 / CH) + LN_EPS)
              for n, p in enumerate(parts)]
    for c in range(CH):
        rows = []
        for sub in range(2):
            rows.append(jnp.concatenate(
                [(load(c, (sub, half)) - means[2 * sub + half]) * scales[2 * sub + half] * xg[c] + xb[c]
                 for half in range(2)], axis=1))
        tile_x[c] = jnp.concatenate(rows).astype(BF16)


LAG = 3


def staggered(count, *stages):
    held = [{} for _ in stages]
    for tick in range(count + LAG * (len(stages) - 1)):
        for k, stage in enumerate(stages):
            i = tick - LAG * k
            if 0 <= i < count:
                held[k][i] = stage(i, held[k - 1].pop(i) if k else None)


def u_kernel(last, layout, sc, *refs):
    z_refs = refs[:len(layout)]
    n_far = 3 if last else 1
    (mask0, mask1, mask2, mask3, norms, xgs, w_ab, w_sq, w_bias, z2_own, z2_par, bias_out, far2, *far3) = refs[len(layout):][:13 + n_far]
    (z_s, a_s, b_s, x_s, mask, stats, tile_a, tile_b, tile_x, tile_c, tile_d, tile_z, in_sem, z_sem, x_sem) = refs[len(layout) + 13 + n_far:]
    me, sample = sc[0], sc[1]
    lanes = pl.ds(pl.multiple_of(LANES * (me // 2), LANES), LANES)
    out_norm = norm_of(norms, OUT)
    in_norm = norm_of(norms, IN)
    att_norm = norm_of(norms, ATT)
    n_tiles = COLS // TILE

    for ref, (r, start) in zip(z_refs, layout):
        src = ref if r else ref.at[sample]
        rows = pl.ds(ROWS * (me ^ r) + start, src.shape[0])
        pltpu.make_async_copy(src, z_s.at[rows], in_sem.at[r]).start()
    for r, part in enumerate((mask0, mask1, mask2, mask3)):
        mask[pl.ds(pl.multiple_of(ROWS * (me ^ r), ROWS), ROWS), :] = part[:].astype(F32)

    def gate_and_product(place, normed, product):
        gate, proj = pair_of(w_sq, place)
        return mm(gate[:], normed), mm(proj[:], product)

    def mask_row(base, i):
        return mask[row_at(base, i), :]

    def measure(base, i, vals=None):
        found = channel_stats(z_s[base + i] if vals is None else vals)
        for n in range(2):
            stats[n if vals is None else n + 2, row_at(base, i), :] = found[n]
        return found

    def recall(base, i, first):
        return [stats[first + n, row_at(base, i), :] for n in range(2)]

    def flush(base):
        a_s[:, pl.ds(base, TILE), :] = swap_major(tile_a[:])
        b_s[:, pl.ds(base, TILE), :] = swap_major(tile_b[:])

    def export(t, start, outgoing, sem):
        r = (t * TILE // ROWS) ^ me
        q = t % (ROWS // TILE)
        rows = pl.ds(pl.multiple_of(TILE * q, TILE), TILE)
        half = pl.ds(pl.multiple_of(ROWS + TILE * (q % 2), TILE), TILE)
        side = pl.ds(pl.multiple_of(LANES * (q // 2), LANES), LANES)
        act = (lambda cp: cp.start()) if start else (lambda cp: cp.wait())
        wide, z_tile = tile_c.at[t % 2], tile_z.at[t % 2]
        narrow = tile_c.at[t % 2, :, :, lanes]
        jobs = [(r == 2, narrow, far2.at[half, :, side])] if outgoing else [
            (r == 0, z_tile, z2_own.at[rows]), (r == 1, z_tile, z2_par.at[rows]), (r == 2, wide, far2.at[rows])]
        if last:
            near_rows, away_rows = (pl.ds(pl.multiple_of(TILE * row, TILE), TILE)
                                    for row in (jnp.minimum(q, CHUNKS - 1), jnp.maximum(q - CHUNKS, 0)))
            jobs += [((r == 3) & (q < CHUNKS), *((narrow, far3[1].at[near_rows]) if outgoing else (wide, far3[0].at[near_rows])))]
            if not outgoing:
                jobs += [((r == 3) & (q >= CHUNKS), z_tile, far3[-1].at[away_rows])]
        else:
            jobs += [(r == 3, narrow, far3[0].at[half, :, side]) if outgoing else (r == 3, wide, far3[0].at[rows])]
        for when, src, dst in jobs:
            @pl.when(when)
            def _():
                act(pltpu.make_async_copy(src, dst, sem.at[t % 2]))

    @pl.loop(0, n_tiles)
    def _(v):
        r = v * TILE // ROWS

        @pl.when(v * TILE % ROWS == 0)
        def _():
            pltpu.make_async_copy(z_refs[0].at[sample], z_s.at[pl.ds(0, ROWS)], in_sem.at[r]).wait()

        base = pl.multiple_of(ROWS * (me ^ r) + v * TILE % ROWS, TILE)
        staggered(
            TILE,
            lambda i, _: mm(w_ab[OUT], (mask_row(base, i) * channel_norm(z_s[base + i], out_norm, measure(base, i))).astype(BF16)),
            lambda i, proj: ab_row(proj, tile_a, tile_b, i))
        flush(base)

    @pl.loop(0, CH, unroll=16)
    def _(c):
        x_s[c] = contract(a_s[c], b_s[c], 1)

    @pl.loop(0, n_tiles)
    def _(t):
        base = pl.multiple_of(TILE * t, TILE)

        @pl.when(t >= 2)
        def _():
            export(t - 2, False, True, x_sem)

        x_norm_tile(x_s, tile_x, base, *pair_of(xgs, OUT))
        tile_c[t % 2] = swap_major(tile_x[:])

        def gate_and_update(i, _):
            normed = channel_norm(z_s[base + i], out_norm, recall(base, i, 0)).astype(BF16)
            return gate_and_product(OUT, normed, tile_c[t % 2, i])

        def next_norm(i, parts):
            z_one = z_s[base + i] + opened(*parts)
            tile_z[0, i] = z_one
            return (mask_row(base, i) * channel_norm(z_one, in_norm, measure(base, i, z_one))).astype(BF16)

        staggered(TILE, gate_and_update, next_norm, lambda i, normed: mm(w_ab[IN], normed),
                  lambda i, proj: ab_row(proj, tile_a, tile_b, i))
        flush(base)
        z_s[pl.ds(base, TILE)] = tile_z[0]
        export(t, True, True, x_sem)

    for t in (n_tiles - 2, n_tiles - 1):
        export(t, False, True, x_sem)

    @pl.loop(0, CH, unroll=16)
    def _(c):
        x_s[c] = contract(a_s[c], b_s[c], 0)

    @pl.loop(0, n_tiles)
    def _(t):
        base = pl.multiple_of(TILE * t, TILE)

        @pl.when(t >= 2)
        def _():
            export(t - 2, False, False, z_sem)

        x_norm_tile(x_s, tile_x, base, *pair_of(xgs, IN))
        tile_c[t % 2] = swap_major(tile_x[:])

        def gate_and_update(i, _):
            normed = channel_norm(z_s[base + i], in_norm, recall(base, i, 2)).astype(BF16)
            return gate_and_product(IN, normed, tile_c[t % 2, i])

        def next_norm(i, parts):
            z_two = z_s[base + i] + opened(*parts)
            tile_z[t % 2, i] = z_two
            return channel_norm(z_two, att_norm).astype(BF16)

        def bias_row(i, normed):
            tile_d[i] = mm(w_bias[:], normed)

        staggered(TILE, gate_and_update, next_norm, bias_row)
        rows = pl.ds(pl.multiple_of(t * TILE % ROWS, TILE), TILE)
        bias_out[t * TILE // ROWS, :, rows, :] = swap_major(tile_d[:])[:4].astype(BF16)
        export(t, True, False, z_sem)

    bias_to = ((far2, 0, 0), (far2, 1, 1), (far2, 3, 2)) if last else ((far2, 0, 0), (far3[0], 1, 0))

    def bias_copy(n):
        dst, block, place = bias_to[n]
        return pltpu.make_async_copy(bias_out.at[me ^ block], dst.at[pl.ds(FAR_BIAS + 4 * place, 4)], in_sem.at[n])

    for n in range(len(bias_to)):
        bias_copy(n).start()
    for t in (n_tiles - 2, n_tiles - 1):
        export(t, False, False, z_sem)
    for n in range(len(bias_to)):
        bias_copy(n).wait()


LANES = 128
VM = pl.BlockSpec(memory_space=pltpu.VMEM)
HB = pl.BlockSpec(memory_space=pltpu.HBM)
SDS = jax.ShapeDtypeStruct
AT_FIRST = lambda i, *_: (i, 0, 0, 0)
SM = pl.BlockSpec(memory_space=pltpu.SMEM)
PARAMS = pltpu.CompilerParams(vmem_limit_bytes=40 * MIB, dimension_semantics=("arbitrary",))
AB_TILE = pltpu.VMEM((TILE, CH, COLS), BF16)
DMA2 = pltpu.SemaphoreType.DMA((2,))
FAR_BIAS = ROWS + ROWS // 2
FAR = SDS((FAR_BIAS + 4, CH, COLS), BF16)
CHUNKS = 2
SOME = CHUNKS * TILE
AWAY = SDS((ROWS - SOME, CH, COLS), F32)
SOME_FULL = SDS((SOME, CH, COLS), BF16)
SOME_HALF = SDS((SOME, CH, LANES), BF16)
FAR_LAST = SDS((FAR_BIAS + 12, CH, COLS), BF16)
ROW_WIDE = SDS((ROWS, CH, COLS), F32)
SAMPLE_BF = pltpu.VMEM((CH, COLS, COLS), BF16)


def u_call(last, layout, sc, z_parts, masks, norms, xgs, w_ab, w_sq, w_bias):
    return pl.pallas_call(
        functools.partial(u_kernel, last, layout),
        out_shape=(ROW_WIDE, ROW_WIDE, SDS((4, 4, ROWS, COLS), BF16), *((FAR_LAST, SOME_FULL, SOME_HALF, AWAY) if last else (FAR, FAR))),
        in_specs=[SM] + [HB] * len(layout) + [VM] * 9,
        out_specs=(HB, HB, VM) + (HB,) * (4 if last else 2),
        scratch_shapes=[
            pltpu.VMEM((COLS, CH, COLS), F32), SAMPLE_BF, SAMPLE_BF,
            pltpu.VMEM((CH, COLS, COLS), F32), pltpu.VMEM((COLS, COLS), F32), pltpu.VMEM((4, COLS, COLS), F32), AB_TILE, AB_TILE, pltpu.VMEM((CH, TILE, COLS), BF16), pltpu.VMEM((2, TILE, CH, COLS), BF16),
            pltpu.VMEM((TILE, 8, COLS), F32), pltpu.VMEM((2, TILE, CH, COLS), F32),
            pltpu.SemaphoreType.DMA((4,)), DMA2, DMA2,
        ],
        compiler_params=pltpu.CompilerParams(vmem_limit_bytes=62 * MIB),
        name="pair_updates",
    )(sc, *z_parts, *masks, norms, xgs, w_ab, w_sq, w_bias)


def l1_kernel(ids, z_in, mask_in, norms, w_ab, a_out, b_out, mask, tile_a, tile_b):
    out_norm = norm_of(norms, OUT)
    mask[:] = mask_in[0].astype(F32)

    @pl.loop(0, ROWS // TILE)
    def _(t):
        base = pl.multiple_of(TILE * t, TILE)
        staggered(
            TILE,
            lambda i, _: mm(w_ab[OUT], (mask[row_at(base, i), :] * channel_norm(z_in[0, base + i], out_norm)).astype(BF16)),
            lambda i, proj: ab_row(proj, tile_a, tile_b, i))
        a_out[0, :, pl.ds(base, TILE), :] = swap_major(tile_a[:])
        b_out[0, :, pl.ds(base, TILE), :] = swap_major(tile_b[:])


def l1_call(ids, zt, mask, norms, w_ab):
    n = ids.shape[0]
    ab = SDS((n, CH, ROWS, COLS), BF16)
    ab_spec = pl.BlockSpec((1, CH, ROWS, COLS), AT_FIRST)
    return pl.pallas_call(
        l1_kernel,
        out_shape=(ab, ab),
        grid_spec=pltpu.PrefetchScalarGridSpec(
            num_scalar_prefetch=1, grid=(n,),
            in_specs=[pl.BlockSpec((1, ROWS, CH, COLS), lambda i, ids: (ids[i], 0, 0, 0)),
                      pl.BlockSpec((1, ROWS, COLS), lambda i, ids: (ids[i], 0, 0)), VM, VM],
            out_specs=(ab_spec, ab_spec),
            scratch_shapes=[pltpu.VMEM((ROWS, COLS), F32), AB_TILE, AB_TILE]),
        compiler_params=PARAMS,
        name="near_projections",
    )(ids, zt, mask, norms, w_ab)


def l2_kernel(sc, a_in, b_own, b_par, xgs, x_out, x_s, tile_x):
    odd = sc[0] % 2 == 1

    @pl.loop(0, CH, unroll=2)
    def _(c):
        for n in range(2):
            own, par = b_own[n, c].astype(F32), b_par[1 - n, c].astype(F32)
            pair = jnp.concatenate([jnp.where(odd, par, own), jnp.where(odd, own, par)]).astype(BF16)
            x_s[c, :, LANES * n:LANES * n + LANES] = contract(a_in[n, c], pair, 1)

    @pl.loop(0, ROWS // TILE)
    def _(t):
        base = pl.multiple_of(TILE * t, TILE)
        x_norm_tile(x_s, tile_x, base, *pair_of(xgs, OUT))
        both = swap_major(tile_x[:])
        for n in range(2):
            x_out[n, pl.ds(base, TILE)] = both[:, :, LANES * n:LANES * n + LANES]


def l2_call(sc, a_all, b_own, b_par, xgs):
    n = a_all.shape[0]
    ab_spec = pl.BlockSpec((2, CH, ROWS, COLS), AT_FIRST)
    return pl.pallas_call(
        l2_kernel,
        grid=(n // 2,),
        out_shape=SDS((n, ROWS, CH, LANES), BF16),
        in_specs=[SM, ab_spec, ab_spec, ab_spec, VM],
        out_specs=pl.BlockSpec((2, ROWS, CH, LANES), AT_FIRST),
        scratch_shapes=[pltpu.VMEM((CH, ROWS, COLS), F32), pltpu.VMEM((CH, TILE, COLS), BF16)],
        compiler_params=PARAMS,
        name="near_product",
    )(sc, a_all, b_own, b_par, xgs)


def r_kernel(blocks, sc, z_in, x_near, x_far, xi, *refs):
    bias_far, refs = (refs[0], refs[1:]) if blocks else (None, refs)
    norms, w_sq, w_bias, z_out, *refs = refs
    swap, refs = (refs[0], refs[1:]) if blocks else (None, refs)
    tile_d, tile_z, z_buf, sem = refs
    step, steps = pl.program_id(0), pl.num_programs(0)
    first = sc[0] < 2
    out_norm, in_norm, att_norm = [norm_of(norms, place) for place in (OUT, IN, ATT)]

    def z_copy(n):
        return pltpu.make_async_copy(z_buf.at[n % 2], z_out.at[pl.ds(pl.multiple_of(n * TILE, TILE), TILE)], sem.at[n % 2])

    @pl.when(step >= 2)
    def _():
        z_copy(step - 2).wait()

    def gate_and_product(place, normed, product):
        gate, proj = pair_of(w_sq, place)
        return mm(gate[:], normed), mm(proj[:], product)

    def outgoing(i, _):
        near, far = x_near[0, i].astype(F32), x_far[i].astype(F32)
        xn = jnp.concatenate([jnp.where(first, near, far), jnp.where(first, far, near)], axis=1).astype(BF16)
        return gate_and_product(OUT, channel_norm(z_in[0, i], out_norm).astype(BF16), xn)

    def norm_one(i, parts):
        z_one = z_in[0, i] + opened(*parts)
        tile_z[i] = z_one
        return channel_norm(z_one, in_norm).astype(BF16)

    def incoming(i, normed):
        return gate_and_product(IN, normed, xi[i])

    def norm_two(i, parts):
        z_two = tile_z[i] + opened(*parts)
        z_buf[step % 2, i] = z_two
        return channel_norm(z_two, att_norm).astype(BF16) if blocks else None

    def bias_row(i, normed):
        tile_d[i] = mm(w_bias[:], normed)

    staggered(TILE, outgoing, norm_one, incoming, norm_two, *([bias_row] if blocks else []))
    z_copy(step).start()
    if blocks:
        swap[0, :, pl.ds(pl.multiple_of(step * TILE, TILE), TILE), :] = swap_major(tile_d[:])[:4].astype(BF16)

        @pl.when(step == 0)
        def _():
            for n in range(blocks):
                swap[n + 1] = bias_far[4 * n:4 * n + 4]

    @pl.when(step == steps - 1)
    def _():
        z_copy(step - 1).wait()
        z_copy(step).wait()


def r_call(blocks, sc, zt, x_near, x_far, xi, norms, w_sq, w_bias):
    steps = ROWS // TILE if blocks else CHUNKS
    far_map = (lambda i, sc: (ROWS // TILE + i % 2, 0, i // 2)) if blocks else (lambda i, sc: (i, 0, 0))
    return pl.pallas_call(
        functools.partial(r_kernel, blocks),
        out_shape=[pltpu.HBM((steps * TILE, CH, COLS), F32)] + [pltpu.HBM((blocks + 1, 4, ROWS, COLS), BF16)] * (blocks > 0),
        grid_spec=pltpu.PrefetchScalarGridSpec(
            num_scalar_prefetch=1, grid=(steps,),
            in_specs=[pl.BlockSpec((1, TILE, CH, COLS), lambda i, sc: (sc[1], i, 0, 0)),
                      pl.BlockSpec((1, TILE, CH, LANES), lambda i, sc: (sc[2], i, 0, 0)),
                      pl.BlockSpec((TILE, CH, LANES), far_map), pl.BlockSpec((TILE, CH, COLS), lambda i, sc: (i, 0, 0)),
                      *[pl.BlockSpec((4 * blocks, CH, COLS), lambda i, sc: (FAR_BIAS // (4 * blocks), 0, 0))] * (blocks > 0),
                      VM, VM, VM],
            out_specs=[HB] + [pl.BlockSpec((blocks + 1, 4, ROWS, COLS), lambda i, sc: (0, 0, 0, 0))] * (blocks > 0),
            scratch_shapes=[pltpu.VMEM((TILE, 8, COLS), F32), pltpu.VMEM((TILE, CH, COLS), F32),
                            pltpu.VMEM((2, TILE, CH, COLS), F32), DMA2]),
        compiler_params=PARAMS,
        name="row_updates",
    )(sc, zt, x_near, x_far, xi, *[xi] * (blocks > 0), norms, w_sq, w_bias)


HEADS, HEAD = 4, 16
MASK_FILL = -1e9
CHUNK = 32
SLOTS = 2
STEPS = 6
AWAY_FIRST = 28
HEAD_ROWS = 8


def attention_kernel(parts, fresh, away, sc, *refs):
    n = len(parts)
    z_refs, bias_refs, (mask_in, norms, w_all, w_proj, *rest) = refs[:n], refs[n:5 * n], refs[5 * n:]
    mask_away, rest = (rest[0], rest[1:]) if away else (None, rest)
    out, *rest = rest if fresh else rest[1:]
    out_away, rest = (rest[:2], rest[2:]) if away else ((), rest)
    (z_in, z_out, mask_i, mask, bias_in, bias_t, q_s, k_s, v_s, g_s, vn_s, gn_s, keep_s, s_buf, e_buf, p_s,
     top_s, inv_s, o_s, m_sem, z_sem, o_sem, b_sem) = rest
    n_rows = sum(size for _, size, _ in parts)
    att_norm = norm_of(norms, 0)

    def rows_of(j):
        return pl.ds(ROWS * j, parts[j][1])

    def own(ref, j):
        return ref.at[sc[j], pl.ds(*parts[j][:2])]

    def z_copy(j):
        start = 0 if j else HEAD_ROWS
        size = parts[j][1] - start
        return pltpu.make_async_copy(z_refs[j].at[pl.ds(start, size)], z_in.at[pl.ds(ROWS * j + start, size)], z_sem.at[j])

    def head_copy():
        return pltpu.make_async_copy(z_refs[0].at[pl.ds(0, HEAD_ROWS)], z_in.at[pl.ds(0, HEAD_ROWS)], z_sem.at[n])

    def m_copy(j):
        src = mask_away.at[0] if away and j == n - 1 else own(mask_in, j)
        return pltpu.make_async_copy(src, mask_i.at[rows_of(j)], m_sem.at[j])

    def b_copy(j, r):
        rows = pl.ds(pl.multiple_of(ROWS * (sc[n + j] ^ r), ROWS), ROWS)
        return pltpu.make_async_copy(bias_refs[4 * j + r].at[parts[j][2][r]], bias_in.at[j, :, rows], b_sem.at[j])

    def o_copies(j):
        first, size, _ = parts[j]
        cuts = (0, size) if j < n - 1 else (0, AWAY_FIRST if away else size - TILE, size)
        pieces = []
        for k, (start, stop) in enumerate(zip(cuts, cuts[1:])):
            dst = out_away[k] if away and j == n - 1 else out.at[sc[j], pl.ds(first + start, stop - start)]
            src = z_out.at[pl.ds(ROWS * j + start, stop - start)]
            pieces.append((ROWS * j + stop, pltpu.make_async_copy(src, dst, o_sem.at[j])))
        return pieces

    starts = [f(j) for j in range(n) for f in (m_copy, *(functools.partial(b_copy, r=r) for r in range(4)))]
    for copy in starts + [head_copy()] + [z_copy(j) for j in range(n)]:
        copy.start()
    for copy in starts:
        copy.wait()
    mask[:] = mask_i[:].astype(F32)
    q_s[:] = jnp.zeros_like(q_s)

    @pl.loop(0, n * HEADS, unroll=4)
    def _(h):
        bias_t[h // HEADS, h % HEADS] = bias_in[h // HEADS, h % HEADS].astype(F32).T

    head_copy().wait()

    def project(row, slot):
        row = jnp.minimum(row, n_rows - 1)
        normed = channel_norm(z_in[row], att_norm).astype(BF16)
        proj = mm(w_all[:], normed)
        k_s[slot] = proj[CH:2 * CH].T.astype(BF16)
        q = proj[:CH].astype(BF16)
        for h in range(HEADS):
            q_s[slot, h, HEAD * h:HEAD * h + HEAD] = q[HEAD * h:HEAD * h + HEAD]
        vn_s[slot] = proj[2 * CH:3 * CH].astype(BF16)
        gn_s[slot] = sigmoid(proj[3 * CH:])

    def keep_mask(row, slot):
        row = jnp.minimum(row, n_rows - 1)
        keep_s[slot] = jnp.broadcast_to(mask[pl.ds(row, 1), :], (LANES, COLS)).T

    def tall(line):
        return jnp.concatenate([line] * (CHUNK // 8))

    def fold(part, op):
        out = part[:8]
        for n in range(1, part.shape[0] // 8):
            out = op(out, part[8 * n:8 * n + 8])
        return out

    def scores(slot, h):
        return mm(k_s[slot], q_s[slot, h])

    def weigh(slot, h, probs):
        heads = slice(HEAD * h, HEAD * h + HEAD)
        o_s[slot, heads] = mm(v_s[slot, heads], probs)

    def step(row, slot, h, logits, defer):
        buf, prev = h % 2, (h + 1) % 2
        sample = jnp.clip(row, 0, n_rows - 1) // ROWS
        top, total, probs = None, None, []
        for c in range(COLS // CHUNK):
            rows = slice(CHUNK * c, CHUNK * c + CHUNK)
            probs.append((e_buf[buf, rows] * tall(inv_s[buf])).astype(BF16))
            exps = jnp.exp(s_buf[prev, rows] - tall(top_s[prev]))
            e_buf[prev, rows] = exps
            part = fold(exps, jnp.add)
            total = part if total is None else total + part
            keep = keep_s[slot, rows]
            keep = jnp.concatenate([keep, keep], axis=1) > 0
            vals = jnp.where(keep, logits[rows] + bias_t[sample, h, rows], MASK_FILL)
            s_buf[buf, rows] = vals
            part = fold(vals, jnp.maximum)
            top = part if top is None else jnp.maximum(top, part)
        top_s[buf] = jnp.broadcast_to(jnp.max(top, axis=0, keepdims=True), (8, COLS))
        inv_s[prev] = jnp.broadcast_to(1.0 / jnp.sum(total, axis=0, keepdims=True), (8, COLS))
        if defer:
            p_s[:] = jnp.concatenate(probs)
        else:
            weigh(1 - slot if h < 2 else slot, (h - 2) % HEADS, jnp.concatenate(probs))

    def finish(row, slot):
        gated = (g_s[slot] * o_s[slot]).astype(BF16)
        z_out[jnp.maximum(row, 0)] = z_in[jnp.clip(row, 0, n_rows - 1)] + mm(w_proj[:], gated)

    project(0, 0)
    keep_mask(0, 0)
    n_steps = (n_rows + 2 + STEPS - 1) // STEPS

    @pl.loop(0, n_steps)
    def _(it):
        first = STEPS * it - 1
        lg = scores(1, 0)
        weigh(0, 1, p_s[:])
        for k in range(STEPS):
            row, slot, last = first + k, 1 - k % 2, k == STEPS - 1
            for h in range(HEADS):
                nxt = scores(slot, h + 1) if h < HEADS - 1 else (None if last else scores(1 - slot, 0))
                if h == 2:
                    project(row + 2, slot)
                step(row, slot, h, lg, last and h == HEADS - 1)
                lg = nxt
                if h == 3:
                    finish(row - 1, 1 - slot)
                    v_s[1 - slot] = vn_s[1 - slot]
                    g_s[1 - slot] = gn_s[1 - slot]
            keep_mask(row + 2, slot)
        for j in range(n):
            @pl.when(it == max((ROWS * j - 1) // STEPS - 1, 0))
            def _():
                z_copy(j).wait()

            for stop, copy in o_copies(j):
                if stop < n_rows:
                    @pl.when(it == (stop + 1) // STEPS)
                    def _():
                        copy.start()

    for stop, copy in o_copies(n - 1):
        if stop == n_rows:
            copy.start()
    for j in range(n):
        for _, copy in o_copies(j):
            copy.wait()


def attend(static, sc, z_parts, biases, mask, norms, w_all, w_proj, out, mask_away=None):
    n, fresh, away = len(z_parts), out is None, mask_away is not None
    z_parts, biases = jax.tree.map(lambda v: pltpu.with_memory_space_constraint(v, pltpu.HBM), (list(z_parts), list(biases)))
    args = (sc, *z_parts, *biases, mask, norms, w_all, w_proj, *[mask_away] * away, *[out] * (not fresh))
    whole = SDS((mask.shape[0], ROWS, CH, COLS), F32)
    aways = [SDS((k, CH, COLS), F32) for k in (AWAY_FIRST, AWAY.shape[0] - AWAY_FIRST)] * away
    rows = sum(z.shape[0] for z in z_parts)
    pair, wide, square, line = [pltpu.VMEM((SLOTS, *shape), dtype) for shape, dtype in (
        ((CH, COLS), BF16), ((CH, COLS), F32), ((COLS, COLS), F32), ((8, COLS), F32))]
    each = [pltpu.VMEM((n, HEADS, COLS, COLS), dtype) for dtype in (BF16, F32)]
    sems, more = pltpu.SemaphoreType.DMA((n,)), pltpu.SemaphoreType.DMA((n + 1,))
    return pl.pallas_call(
        functools.partial(attention_kernel, static, fresh, away),
        out_shape=(whole, *aways),
        in_specs=[SM] + [HB] * (5 * n + 1) + [VM] * 3 + [HB] * (away + (not fresh)),
        out_specs=(HB,) * (1 + len(aways)),
        scratch_shapes=[
            pltpu.VMEM((rows, CH, COLS), F32), pltpu.VMEM((rows + STEPS, CH, COLS), F32), pltpu.VMEM((rows, COLS), jnp.int32),
            pltpu.VMEM((rows, COLS), F32), *each, pltpu.VMEM((SLOTS, HEADS, CH, COLS), BF16),
            pltpu.VMEM((SLOTS, COLS, CH), BF16), pair, wide, pair, wide, pltpu.VMEM((SLOTS, COLS, LANES), F32),
            square, square, pltpu.VMEM((COLS, COLS), BF16), line, line, wide, sems, more, sems, sems,
        ],
        compiler_params=pltpu.CompilerParams(vmem_limit_bytes=48 * MIB),
        input_output_aliases={} if fresh else {len(args) - 1: 0},
        name="triangle_attention",
    )(*args)


FIRST = 4


def exchange(values, r):
    return lax.ppermute(values, 'dap', [(i, i ^ r) for i in range(4)])


def update_weights(params):
    norm_gain, norm_bias, w_a, w_agate, w_b, w_bgate, w_gate, x_gain, x_bias, w_proj = params
    half = jnp.bfloat16(0.5)
    wide = lambda v: jnp.broadcast_to(v[:, None], (CH, COLS))
    deep = lambda v: jnp.broadcast_to(v[:, None, None], (CH, 8, 128))
    return ([wide(norm_gain), wide(norm_bias)], [deep(x_gain), deep(x_bias)],
            half * jnp.concatenate([w_a.T, w_agate.T, w_b.T, w_bgate.T]), [half * w_gate.T, half * w_proj.T])


def solution(mesh):
    def local_block(pair_z, pair_mask, *weights):
        me = lax.axis_index('dap')
        zt = jnp.transpose(pair_z, (0, 1, 3, 2))
        n_own = zt.shape[0] // 4
        mask_bf = pair_mask.astype(BF16)
        arrived, layouts, before = [], [], ()
        for t in range(n_own):
            pieces = [(2, 0, FIRST), (2, FIRST, ROWS)] if t == 0 else [(2, 0, ROWS)]
            pieces += [(3, 0, ROWS), (1, 0, ROWS)]
            got = []
            for r, start, stop in pieces:
                where = (n_own * (me ^ r) + t, start, 0, 0)
                send = lax.dynamic_slice(lax.optimization_barrier((zt, *before))[0], where, (1, stop - start, CH, COLS))[0]
                if t == 0 or r == 1:
                    before = (send,)
                got.append(exchange(send, r))
                if t == 0 and stop == ROWS and r == 2:
                    mask_bf, weights = lax.optimization_barrier((mask_bf, weights, send))[:2]
                    masks = [lax.dynamic_slice_in_dim(mask_bf, n_own * (me ^ k), n_own) for k in range(4)]
                    before = (*before, *masks)
                    masks = [exchange(m, k) if k else m for k, m in enumerate(masks)]
            arrived.append([zt, *got])
            layouts.append(((0, 0), *((r, start) for r, start, _ in pieces)))

        out_n, out_x, out_ab, out_sq = update_weights(weights[:10])
        in_n, in_x, in_ab, in_sq = update_weights(weights[10:20])
        att_gain, att_shift, w_q, w_k, w_v, w_bias, w_gate, w_proj = weights[20:]
        att_n = [jnp.broadcast_to(v[:, None], (CH, COLS)) for v in (att_gain, att_shift)]
        norms = jnp.stack(out_n + in_n + att_n)
        xgs = jnp.stack(out_x + in_x)
        w_ab = jnp.stack([out_ab, in_ab])
        w_sq = jnp.stack(out_sq + in_sq)
        w_bias8 = jnp.concatenate([w_bias.T, jnp.zeros((4, CH), BF16)])
        w_all = jnp.concatenate([w_q.T * jnp.bfloat16(HEAD ** -0.5), w_k.T, w_v.T, w_gate.T])
        w_out = w_proj.T
        att_norms = norms[4:]

        token = [None]

        def ordered(call, sc, *args):
            sc = jnp.stack([jnp.asarray(v, jnp.int32) for v in sc])
            if token[0] is not None:
                sc = lax.optimization_barrier((sc, token[0]))[0]
            res = call(sc, *args)
            token[0] = jax.tree.leaves(res)[-1]
            return res

        def attention(jobs, out, mask_away=None):
            samples, orders, z_parts, biases, starts = zip(*jobs)
            static = tuple((start, z.shape[0], tuple(place for _, place in blocks))
                           for start, z, blocks in zip(starts, z_parts, biases))
            arrays = [array for blocks in biases for array, _ in blocks]
            return ordered(functools.partial(attend, static), samples + orders, z_parts, arrays, pair_mask, att_norms,
                           w_all, w_out, out, mask_away)

        far = [(t, r) for t in range(n_own) for r in (2, 3)]
        a_far, b_far = ordered(l1_call, [n_own * (me ^ r) + t for t, r in far], zt, pair_mask, norms, w_ab)
        b_par = exchange(b_far, 1)
        x_near = ordered(l2_call, [me], a_far, b_far, b_par, xgs)

        out = None
        held = []
        for t in range(n_own):
            last = t == n_own - 1
            z_own, z_par, bias, far2, *far3 = ordered(functools.partial(u_call, last, layouts[t]), [me, n_own * me + t],
                                                      arrived[t], [m[t] for m in masks], norms, xgs, w_ab, w_sq, w_bias8)
            here = lambda array: [(array, r) for r in range(4)]
            near = (n_own * (me ^ 1) + t, 0, exchange(z_par, 1), here(exchange(bias, 1)), 0)
            own = (n_own * me + t, 0, z_own, here(bias), 0)
            two = exchange(far2, 2)
            three = [exchange(v, 3) for v in far3[:2]]
            held.append((two, three))
            if last:
                out, *away = attention([own, (0, 0, far3[-1], here(bias), 0)], out,
                                       masks[3][t][None, SOME:].astype(jnp.int32))
                away = [exchange(v, 3) for v in away]
            else:
                out, = attention([own, near], out)

        def rows_of(t, r, blocks, x_far, xi):
            return ordered(functools.partial(r_call, blocks), [me, n_own * (me ^ r) + t, far.index((t, r))],
                           zt, x_near, x_far, xi, norms, w_sq, w_bias8)

        for t in range(n_own - 1):
            two, (three,) = held[t]
            z_two, mine_two = rows_of(t, 2, 1, two, two)
            z_three, mine_three = rows_of(t, 3, 1, three, three)
            par_two, par_three = exchange(mine_two, 1), exchange(mine_three, 1)
            jobs = [(n_own * (me ^ r) + t, me, z, [(mine, 0), (par, 0), (mine, 1), (par, 1)], 0)
                    for r, z, mine, par in ((2, z_two, mine_two, par_three), (3, z_three, mine_three, par_two))]
            out, = attention(([] if t else [near]) + jobs, out)
        two, three = held[t + 1]
        z_two, mine = rows_of(t + 1, 2, 3, two, two)
        par = exchange(mine, 1)
        out, = attention([(n_own * (me ^ 2) + t + 1, me, z_two, [(mine, k) for k in (0, 3, 1, 2)], 0)], out)
        z_three, = rows_of(t + 1, 3, 0, three[1], three[0])
        out, = attention([(n_own * (me ^ 3) + t + 1, me, z_three, [(par, k) for k in (3, 0, 2, 1)], 0)], out)
        for v, start in zip(away, (SOME, SOME + AWAY_FIRST)):
            out = lax.dynamic_update_slice(out, v[None], (n_own * (me ^ 3) + n_own - 1, start, 0, 0))
        return jnp.transpose(out, (0, 1, 3, 2))

    pair_spec = P('data', 'dap')
    return jax.shard_map(local_block, mesh=mesh, in_specs=(pair_spec, pair_spec) + (P(),) * 28,
                         out_specs=pair_spec, check_vma=False)
```

```python
import functools

import jax
import jax.numpy as jnp
from jax import lax
from jax.experimental import pallas as pl
from jax.experimental.pallas import tpu as pltpu
from jax.sharding import PartitionSpec as P


LN_EPS = 1e-5
F32, BF16 = jnp.float32, jnp.bfloat16
ROWS, CH, COLS = 64, 64, 256
TILE = 16
SUB = 8
MIB = 1 << 20
OUT, IN, ATT = range(3)


def channel_stats(vals):
    ch_mean = jnp.mean(vals, axis=0, keepdims=True)
    ch_var = jnp.mean(jnp.square(vals - ch_mean), axis=0, keepdims=True)
    return ch_mean, lax.rsqrt(ch_var + LN_EPS)


def channel_norm(vals, norm, stats=None):
    gain, shift = norm
    ch_mean, scale = channel_stats(vals) if stats is None else stats
    return (vals - ch_mean) * scale * gain + shift


def sigmoid(vals):
    return 0.5 * jnp.tanh(0.5 * vals) + 0.5


def swap_major(vals):
    return jnp.swapaxes(vals, 0, 1)


def pair_of(ref, place):
    return ref.at[2 * place], ref.at[2 * place + 1]


def norm_of(ref, place):
    return [part[:] for part in pair_of(ref, place)]


def contract(lhs, rhs, axis_id):
    return lax.dot_general(lhs, rhs, (((axis_id,), (axis_id,)), ((), ())), preferred_element_type=F32)


def mm(lhs, rhs):
    return jnp.dot(lhs, rhs, preferred_element_type=F32)


def opened(gate, product):
    return (jnp.tanh(gate) + 1.0) * product


def row_at(base, i):
    return pl.ds(base + i, 1)


def ab_row(proj, tile_a, tile_b, slot):
    for n, tile in enumerate((tile_a, tile_b)):
        linear, gate = jnp.split(proj[2 * CH * n:2 * CH * n + 2 * CH], 2)
        tile[slot] = opened(gate, linear).astype(BF16)


def x_norm_tile(x_s, tile_x, base, xg, xb):
    parts = [(sub, half) for sub in range(2) for half in range(2)]

    def load(c, part):
        return x_s[c, pl.ds(pl.multiple_of(base + 8 * part[0], 8), 8), 128 * part[1]:128 * part[1] + 128]

    means = [sum(load(c, p) for c in range(CH)) * (1.0 / CH) for p in parts]
    scales = [lax.rsqrt(sum(jnp.square(load(c, p) - means[n]) for c in range(CH)) * (1.0 / CH) + LN_EPS)
              for n, p in enumerate(parts)]
    for c in range(CH):
        rows = []
        for sub in range(2):
            rows.append(jnp.concatenate(
                [(load(c, (sub, half)) - means[2 * sub + half]) * scales[2 * sub + half] * xg[c] + xb[c]
                 for half in range(2)], axis=1))
        tile_x[c] = jnp.concatenate(rows).astype(BF16)


LAG = 3


def staggered(count, *stages):
    held = [{} for _ in stages]
    for tick in range(count + LAG * (len(stages) - 1)):
        for k, stage in enumerate(stages):
            i = tick - LAG * k
            if 0 <= i < count:
                held[k][i] = stage(i, held[k - 1].pop(i) if k else None)


def u_kernel(last, layout, sc, *refs):
    z_refs = refs[:len(layout)]
    n_far = 3 if last else 1
    (mask0, mask1, mask2, mask3, norms, xgs, w_ab, w_sq, w_bias, z2_own, z2_par, bias_out, far2, *far3) = refs[len(layout):][:13 + n_far]
    (z_s, a_s, b_s, x_s, mask, stats, tile_a, tile_b, tile_x, tile_c, tile_d, tile_z, in_sem, z_sem, x_sem) = refs[len(layout) + 13 + n_far:]
    me, sample = sc[0], sc[1]
    lanes = pl.ds(pl.multiple_of(LANES * (me // 2), LANES), LANES)
    out_norm = norm_of(norms, OUT)
    in_norm = norm_of(norms, IN)
    att_norm = norm_of(norms, ATT)
    n_tiles = COLS // TILE

    for ref, (r, start) in zip(z_refs, layout):
        src = ref if r else ref.at[sample]
        rows = pl.ds(ROWS * (me ^ r) + start, src.shape[0])
        pltpu.make_async_copy(src, z_s.at[rows], in_sem.at[r]).start()
    for r, part in enumerate((mask0, mask1, mask2, mask3)):
        mask[pl.ds(pl.multiple_of(ROWS * (me ^ r), ROWS), ROWS), :] = part[:].astype(F32)

    def gate_and_product(place, normed, product):
        gate, proj = pair_of(w_sq, place)
        return mm(gate[:], normed), mm(proj[:], product)

    def mask_row(base, i):
        return mask[row_at(base, i), :]

    def measure(base, i, vals=None):
        found = channel_stats(z_s[base + i] if vals is None else vals)
        for n in range(2):
            stats[n if vals is None else n + 2, row_at(base, i), :] = found[n]
        return found

    def recall(base, i, first):
        return [stats[first + n, row_at(base, i), :] for n in range(2)]

    def flush(base):
        a_s[:, pl.ds(base, TILE), :] = swap_major(tile_a[:])
        b_s[:, pl.ds(base, TILE), :] = swap_major(tile_b[:])

    def export(t, start, outgoing, sem):
        r = (t * TILE // ROWS) ^ me
        q = t % (ROWS // TILE)
        rows = pl.ds(pl.multiple_of(TILE * q, TILE), TILE)
        half = pl.ds(pl.multiple_of(ROWS + TILE * (q % 2), TILE), TILE)
        side = pl.ds(pl.multiple_of(LANES * (q // 2), LANES), LANES)
        act = (lambda cp: cp.start()) if start else (lambda cp: cp.wait())
        wide, z_tile = tile_c.at[t % 2], tile_z.at[t % 2]
        narrow = tile_c.at[t % 2, :, :, lanes]
        jobs = [(r == 2, narrow, far2.at[half, :, side])] if outgoing else [
            (r == 0, z_tile, z2_own.at[rows]), (r == 1, z_tile, z2_par.at[rows]), (r == 2, wide, far2.at[rows])]
        if last:
            whole = pl.ds(pl.multiple_of(TILE * jnp.minimum(q, CHUNKS - 1), TILE), TILE)
            src, dst = (narrow, far3[1]) if outgoing else (wide, far3[0])
            jobs += [((r == 3) & (q < CHUNKS), src, dst.at[whole]),
                     ((r == 3) & (q == CHUNKS), src.at[pl.ds(0, SPLIT)], dst.at[pl.ds(CHUNKS * TILE, SPLIT)])]
            if not outgoing:
                rest = TILE - SPLIT
                jobs += [((r == 3) & (q == CHUNKS), z_tile.at[pl.ds(SPLIT, rest)], far3[-1].at[pl.ds(0, rest)]),
                         ((r == 3) & (q > CHUNKS), z_tile, far3[-1].at[pl.ds(rest, TILE)])]
        else:
            jobs += [(r == 3, narrow, far3[0].at[half, :, side]) if outgoing else (r == 3, wide, far3[0].at[rows])]
        for when, src, dst in jobs:
            @pl.when(when)
            def _():
                act(pltpu.make_async_copy(src, dst, sem.at[t % 2]))

    @pl.loop(0, n_tiles)
    def _(v):
        r = v * TILE // ROWS

        @pl.when(v * TILE % ROWS == 0)
        def _():
            pltpu.make_async_copy(z_refs[0].at[sample], z_s.at[pl.ds(0, ROWS)], in_sem.at[r]).wait()

        base = pl.multiple_of(ROWS * (me ^ r) + v * TILE % ROWS, TILE)
        staggered(
            TILE,
            lambda i, _: mm(w_ab[OUT], (mask_row(base, i) * channel_norm(z_s[base + i], out_norm, measure(base, i))).astype(BF16)),
            lambda i, proj: ab_row(proj, tile_a, tile_b, i))
        flush(base)

    @pl.loop(0, CH, unroll=16)
    def _(c):
        x_s[c] = contract(a_s[c], b_s[c], 1)

    @pl.loop(0, n_tiles)
    def _(t):
        base = pl.multiple_of(TILE * t, TILE)

        @pl.when(t >= 2)
        def _():
            export(t - 2, False, True, x_sem)

        x_norm_tile(x_s, tile_x, base, *pair_of(xgs, OUT))
        tile_c[t % 2] = swap_major(tile_x[:])

        def gate_and_update(i, _):
            normed = channel_norm(z_s[base + i], out_norm, recall(base, i, 0)).astype(BF16)
            return gate_and_product(OUT, normed, tile_c[t % 2, i])

        def next_norm(i, parts):
            z_one = z_s[base + i] + opened(*parts)
            tile_z[0, i] = z_one
            return (mask_row(base, i) * channel_norm(z_one, in_norm, measure(base, i, z_one))).astype(BF16)

        staggered(TILE, gate_and_update, next_norm, lambda i, normed: mm(w_ab[IN], normed),
                  lambda i, proj: ab_row(proj, tile_a, tile_b, i))
        flush(base)
        z_s[pl.ds(base, TILE)] = tile_z[0]
        export(t, True, True, x_sem)

    for t in (n_tiles - 2, n_tiles - 1):
        export(t, False, True, x_sem)

    @pl.loop(0, CH, unroll=16)
    def _(c):
        x_s[c] = contract(a_s[c], b_s[c], 0)

    @pl.loop(0, n_tiles)
    def _(t):
        base = pl.multiple_of(TILE * t, TILE)

        @pl.when(t >= 2)
        def _():
            export(t - 2, False, False, z_sem)

        x_norm_tile(x_s, tile_x, base, *pair_of(xgs, IN))
        tile_c[t % 2] = swap_major(tile_x[:])

        def gate_and_update(i, _):
            normed = channel_norm(z_s[base + i], in_norm, recall(base, i, 2)).astype(BF16)
            return gate_and_product(IN, normed, tile_c[t % 2, i])

        def next_norm(i, parts):
            z_two = z_s[base + i] + opened(*parts)
            tile_z[t % 2, i] = z_two
            return channel_norm(z_two, att_norm).astype(BF16)

        def bias_row(i, normed):
            tile_d[i] = mm(w_bias[:], normed)

        staggered(TILE, gate_and_update, next_norm, bias_row)
        rows = pl.ds(pl.multiple_of(t * TILE % ROWS, TILE), TILE)
        bias_out[t * TILE // ROWS, :, rows, :] = swap_major(tile_d[:])[:4].astype(BF16)
        export(t, True, False, z_sem)

    bias_to = ((far2, 0, 0), (far2, 1, 1), (far2, 3, 2)) if last else ((far2, 0, 0), (far3[0], 1, 0))

    def bias_copy(n):
        dst, block, place = bias_to[n]
        return pltpu.make_async_copy(bias_out.at[me ^ block], dst.at[pl.ds(FAR_BIAS + 4 * place, 4)], in_sem.at[n])

    for n in range(len(bias_to)):
        bias_copy(n).start()
    for t in (n_tiles - 2, n_tiles - 1):
        export(t, False, False, z_sem)
    for n in range(len(bias_to)):
        bias_copy(n).wait()


LANES = 128
VM = pl.BlockSpec(memory_space=pltpu.VMEM)
HB = pl.BlockSpec(memory_space=pltpu.HBM)
SDS = jax.ShapeDtypeStruct
AT_FIRST = lambda i, *_: (i, 0, 0, 0)
SM = pl.BlockSpec(memory_space=pltpu.SMEM)
PARAMS = pltpu.CompilerParams(vmem_limit_bytes=40 * MIB, dimension_semantics=("arbitrary",))
AB_TILE = pltpu.VMEM((TILE, CH, COLS), BF16)
DMA2 = pltpu.SemaphoreType.DMA((2,))
FAR_BIAS = ROWS + ROWS // 2
FAR = SDS((FAR_BIAS + 4, CH, COLS), BF16)
CHUNKS = 2
SOME = 34
SPLIT = SOME - CHUNKS * TILE
AWAY = SDS((ROWS - SOME, CH, COLS), F32)
SOME_FULL = SDS((SOME, CH, COLS), BF16)
SOME_HALF = SDS((SOME, CH, LANES), BF16)
FAR_LAST = SDS((FAR_BIAS + 12, CH, COLS), BF16)
ROW_WIDE = SDS((ROWS, CH, COLS), F32)
SAMPLE_BF = pltpu.VMEM((CH, COLS, COLS), BF16)


def u_call(last, layout, sc, z_parts, masks, norms, xgs, w_ab, w_sq, w_bias):
    return pl.pallas_call(
        functools.partial(u_kernel, last, layout),
        out_shape=(ROW_WIDE, ROW_WIDE, SDS((4, 4, ROWS, COLS), BF16), *((FAR_LAST, SOME_FULL, SOME_HALF, AWAY) if last else (FAR, FAR))),
        in_specs=[SM] + [HB] * len(layout) + [VM] * 9,
        out_specs=(HB, HB, VM) + (HB,) * (4 if last else 2),
        scratch_shapes=[
            pltpu.VMEM((COLS, CH, COLS), F32), SAMPLE_BF, SAMPLE_BF,
            pltpu.VMEM((CH, COLS, COLS), F32), pltpu.VMEM((COLS, COLS), F32), pltpu.VMEM((4, COLS, COLS), F32), AB_TILE, AB_TILE, pltpu.VMEM((CH, TILE, COLS), BF16), pltpu.VMEM((2, TILE, CH, COLS), BF16),
            pltpu.VMEM((TILE, 8, COLS), F32), pltpu.VMEM((2, TILE, CH, COLS), F32),
            pltpu.SemaphoreType.DMA((4,)), DMA2, DMA2,
        ],
        compiler_params=pltpu.CompilerParams(vmem_limit_bytes=62 * MIB),
        name="pair_updates",
    )(sc, *z_parts, *masks, norms, xgs, w_ab, w_sq, w_bias)


def l1_kernel(ids, z_in, mask_in, norms, w_ab, a_out, b_out, mask, tile_a, tile_b):
    out_norm = norm_of(norms, OUT)
    mask[:] = mask_in[0].astype(F32)

    @pl.loop(0, ROWS // TILE)
    def _(t):
        base = pl.multiple_of(TILE * t, TILE)
        staggered(
            TILE,
            lambda i, _: mm(w_ab[OUT], (mask[row_at(base, i), :] * channel_norm(z_in[0, base + i], out_norm)).astype(BF16)),
            lambda i, proj: ab_row(proj, tile_a, tile_b, i))
        a_out[0, :, pl.ds(base, TILE), :] = swap_major(tile_a[:])
        b_out[0, :, pl.ds(base, TILE), :] = swap_major(tile_b[:])


def l1_call(ids, zt, mask, norms, w_ab):
    n = ids.shape[0]
    ab = SDS((n, CH, ROWS, COLS), BF16)
    ab_spec = pl.BlockSpec((1, CH, ROWS, COLS), AT_FIRST)
    return pl.pallas_call(
        l1_kernel,
        out_shape=(ab, ab),
        grid_spec=pltpu.PrefetchScalarGridSpec(
            num_scalar_prefetch=1, grid=(n,),
            in_specs=[pl.BlockSpec((1, ROWS, CH, COLS), lambda i, ids: (ids[i], 0, 0, 0)),
                      pl.BlockSpec((1, ROWS, COLS), lambda i, ids: (ids[i], 0, 0)), VM, VM],
            out_specs=(ab_spec, ab_spec),
            scratch_shapes=[pltpu.VMEM((ROWS, COLS), F32), AB_TILE, AB_TILE]),
        compiler_params=PARAMS,
        name="near_projections",
    )(ids, zt, mask, norms, w_ab)


def l2_kernel(sc, a_in, b_own, b_par, xgs, x_out, x_s, tile_x):
    odd = sc[0] % 2 == 1

    @pl.loop(0, CH, unroll=2)
    def _(c):
        for n in range(2):
            own, par = b_own[n, c].astype(F32), b_par[1 - n, c].astype(F32)
            pair = jnp.concatenate([jnp.where(odd, par, own), jnp.where(odd, own, par)]).astype(BF16)
            x_s[c, :, LANES * n:LANES * n + LANES] = contract(a_in[n, c], pair, 1)

    @pl.loop(0, ROWS // TILE)
    def _(t):
        base = pl.multiple_of(TILE * t, TILE)
        x_norm_tile(x_s, tile_x, base, *pair_of(xgs, OUT))
        both = swap_major(tile_x[:])
        for n in range(2):
            x_out[n, pl.ds(base, TILE)] = both[:, :, LANES * n:LANES * n + LANES]


def l2_call(sc, a_all, b_own, b_par, xgs):
    n = a_all.shape[0]
    ab_spec = pl.BlockSpec((2, CH, ROWS, COLS), AT_FIRST)
    return pl.pallas_call(
        l2_kernel,
        grid=(n // 2,),
        out_shape=SDS((n, ROWS, CH, LANES), BF16),
        in_specs=[SM, ab_spec, ab_spec, ab_spec, VM],
        out_specs=pl.BlockSpec((2, ROWS, CH, LANES), AT_FIRST),
        scratch_shapes=[pltpu.VMEM((CH, ROWS, COLS), F32), pltpu.VMEM((CH, TILE, COLS), BF16)],
        compiler_params=PARAMS,
        name="near_product",
    )(sc, a_all, b_own, b_par, xgs)


def r_kernel(blocks, sc, z_in, x_near, x_far, xi, *refs):
    bias_far, refs = (refs[0], refs[1:]) if blocks else (None, refs)
    norms, w_sq, w_bias, z_out, *refs = refs
    swap, refs = (refs[0], refs[1:]) if blocks else (None, refs)
    tile_d, tile_z, z_buf, sem = refs
    step, steps, tile = pl.program_id(0), pl.num_programs(0), xi.shape[0]
    first = sc[0] < 2
    out_norm, in_norm, att_norm = [norm_of(norms, place) for place in (OUT, IN, ATT)]

    def z_copy(n):
        return pltpu.make_async_copy(z_buf.at[n % 2], z_out.at[pl.ds(n * tile, tile)], sem.at[n % 2])

    @pl.when(step >= 2)
    def _():
        z_copy(step - 2).wait()

    def gate_and_product(place, normed, product):
        gate, proj = pair_of(w_sq, place)
        return mm(gate[:], normed), mm(proj[:], product)

    def outgoing(i, _):
        near, far = x_near[0, i].astype(F32), x_far[i].astype(F32)
        xn = jnp.concatenate([jnp.where(first, near, far), jnp.where(first, far, near)], axis=1).astype(BF16)
        return gate_and_product(OUT, channel_norm(z_in[0, i], out_norm).astype(BF16), xn)

    def norm_one(i, parts):
        z_one = z_in[0, i] + opened(*parts)
        tile_z[i] = z_one
        return channel_norm(z_one, in_norm).astype(BF16)

    def incoming(i, normed):
        return gate_and_product(IN, normed, xi[i])

    def norm_two(i, parts):
        z_two = tile_z[i] + opened(*parts)
        z_buf[step % 2, i] = z_two
        return channel_norm(z_two, att_norm).astype(BF16) if blocks else None

    def bias_row(i, normed):
        tile_d[i] = mm(w_bias[:], normed)

    staggered(tile, outgoing, norm_one, incoming, norm_two, *([bias_row] if blocks else []))
    z_copy(step).start()
    if blocks:
        swap[0, :, pl.ds(pl.multiple_of(step * TILE, TILE), TILE), :] = swap_major(tile_d[:])[:4].astype(BF16)

        @pl.when(step == 0)
        def _():
            for n in range(blocks):
                swap[n + 1] = bias_far[4 * n:4 * n + 4]

    @pl.when(step == steps - 1)
    def _():
        z_copy(step - 1).wait()
        z_copy(step).wait()


def r_call(blocks, sc, zt, x_near, x_far, xi, norms, w_sq, w_bias):
    steps = ROWS // TILE if blocks else CHUNKS
    tile = TILE if blocks else SOME // steps
    far_map = (lambda i, sc: (ROWS // TILE + i % 2, 0, i // 2)) if blocks else (lambda i, sc: (i, 0, 0))
    return pl.pallas_call(
        functools.partial(r_kernel, blocks),
        out_shape=[pltpu.HBM((steps * tile, CH, COLS), F32)] + [pltpu.HBM((blocks + 1, 4, ROWS, COLS), BF16)] * (blocks > 0),
        grid_spec=pltpu.PrefetchScalarGridSpec(
            num_scalar_prefetch=1, grid=(steps,),
            in_specs=[pl.BlockSpec((1, tile, CH, COLS), lambda i, sc: (sc[1], i, 0, 0)),
                      pl.BlockSpec((1, tile, CH, LANES), lambda i, sc: (sc[2], i, 0, 0)),
                      pl.BlockSpec((tile, CH, LANES), far_map), pl.BlockSpec((tile, CH, COLS), lambda i, sc: (i, 0, 0)),
                      *[pl.BlockSpec((4 * blocks, CH, COLS), lambda i, sc: (FAR_BIAS // (4 * blocks), 0, 0))] * (blocks > 0),
                      VM, VM, VM],
            out_specs=[HB] + [pl.BlockSpec((blocks + 1, 4, ROWS, COLS), lambda i, sc: (0, 0, 0, 0))] * (blocks > 0),
            scratch_shapes=[pltpu.VMEM((tile, 8, COLS), F32), pltpu.VMEM((tile, CH, COLS), F32),
                            pltpu.VMEM((2, tile, CH, COLS), F32), DMA2]),
        compiler_params=PARAMS,
        name="row_updates",
    )(sc, zt, x_near, x_far, xi, *[xi] * (blocks > 0), norms, w_sq, w_bias)


HEADS, HEAD = 4, 16
MASK_FILL = -1e9
CHUNK = 32
SLOTS = 2
STEPS = 6
AWAY_FIRST = 26
HEAD_ROWS = 8


def mask_rows(size):
    return pl.cdiv(size, SUB) * SUB


def attention_kernel(parts, fresh, away, sc, *refs):
    n = len(parts)
    z_refs, bias_refs, (mask_in, norms, w_all, w_proj, *rest) = refs[:n], refs[n:5 * n], refs[5 * n:]
    mask_away, rest = (rest[0], rest[1:]) if away else (None, rest)
    out, *rest = rest if fresh else rest[1:]
    out_away, rest = (rest[:2], rest[2:]) if away else ((), rest)
    (z_in, z_out, mask_i, mask, bias_in, bias_t, q_s, k_s, v_s, g_s, vn_s, gn_s, keep_s, s_buf, e_buf, p_s,
     top_s, inv_s, o_s, m_sem, z_sem, o_sem, b_sem) = rest
    n_rows = sum(size for _, size, _ in parts)
    att_norm = norm_of(norms, 0)

    def z_copy(j):
        start = 0 if j else HEAD_ROWS
        size = parts[j][1] - start
        return pltpu.make_async_copy(z_refs[j].at[pl.ds(start, size)], z_in.at[pl.ds(ROWS * j + start, size)], z_sem.at[j])

    def head_copy():
        return pltpu.make_async_copy(z_refs[0].at[pl.ds(0, HEAD_ROWS)], z_in.at[pl.ds(0, HEAD_ROWS)], z_sem.at[n])

    def m_copy(j):
        size = mask_rows(parts[j][1])
        src = mask_away.at[0] if away and j == n - 1 else mask_in.at[sc[j], pl.ds(parts[j][0], size)]
        return pltpu.make_async_copy(src, mask_i.at[pl.ds(ROWS * j, size)], m_sem.at[j])

    def b_copy(j, r):
        rows = pl.ds(pl.multiple_of(ROWS * (sc[n + j] ^ r), ROWS), ROWS)
        return pltpu.make_async_copy(bias_refs[4 * j + r].at[parts[j][2][r]], bias_in.at[j, :, rows], b_sem.at[j])

    def o_copies(j):
        first, size, _ = parts[j]
        cuts = (0, size) if j < n - 1 else (0, AWAY_FIRST if away else size - TILE, size)
        pieces = []
        for k, (start, stop) in enumerate(zip(cuts, cuts[1:])):
            dst = out_away[k] if away and j == n - 1 else out.at[sc[j], pl.ds(first + start, stop - start)]
            src = z_out.at[pl.ds(ROWS * j + start, stop - start)]
            pieces.append((ROWS * j + stop, pltpu.make_async_copy(src, dst, o_sem.at[j])))
        return pieces

    starts = [f(j) for j in range(n) for f in (m_copy, *(functools.partial(b_copy, r=r) for r in range(4)))]
    for copy in starts + [head_copy()] + [z_copy(j) for j in range(n)]:
        copy.start()
    for copy in starts:
        copy.wait()
    mask[:] = mask_i[:].astype(F32)
    q_s[:] = jnp.zeros_like(q_s)

    @pl.loop(0, n * HEADS, unroll=4)
    def _(h):
        bias_t[h // HEADS, h % HEADS] = bias_in[h // HEADS, h % HEADS].astype(F32).T

    head_copy().wait()

    def project(row, slot):
        row = jnp.minimum(row, n_rows - 1)
        normed = channel_norm(z_in[row], att_norm).astype(BF16)
        proj = mm(w_all[:], normed)
        k_s[slot] = proj[CH:2 * CH].T.astype(BF16)
        q = proj[:CH].astype(BF16)
        for h in range(HEADS):
            q_s[slot, h, HEAD * h:HEAD * h + HEAD] = q[HEAD * h:HEAD * h + HEAD]
        vn_s[slot] = proj[2 * CH:3 * CH].astype(BF16)
        gn_s[slot] = sigmoid(proj[3 * CH:])

    def keep_mask(row, slot):
        row = jnp.minimum(row, n_rows - 1)
        keep_s[slot] = jnp.broadcast_to(mask[pl.ds(row, 1), :], (LANES, COLS)).T

    def tall(line):
        return jnp.concatenate([line] * (CHUNK // SUB))

    def fold(part, op):
        out = part[:SUB]
        for n in range(1, part.shape[0] // SUB):
            out = op(out, part[SUB * n:SUB * n + SUB])
        return out

    def scores(slot, h):
        return mm(k_s[slot], q_s[slot, h])

    def weigh(slot, h, probs):
        heads = slice(HEAD * h, HEAD * h + HEAD)
        o_s[slot, heads] = mm(v_s[slot, heads], probs)

    def step(row, slot, h, logits, defer):
        buf, prev = h % 2, (h + 1) % 2
        sample = jnp.clip(row, 0, n_rows - 1) // ROWS
        top, total, probs = None, None, []
        for c in range(COLS // CHUNK):
            rows = slice(CHUNK * c, CHUNK * c + CHUNK)
            probs.append((e_buf[buf, rows] * tall(inv_s[buf])).astype(BF16))
            exps = jnp.exp(s_buf[prev, rows] - tall(top_s[prev]))
            e_buf[prev, rows] = exps
            part = fold(exps, jnp.add)
            total = part if total is None else total + part
            keep = keep_s[slot, rows]
            keep = jnp.concatenate([keep, keep], axis=1) > 0
            vals = jnp.where(keep, logits[rows] + bias_t[sample, h, rows], MASK_FILL)
            s_buf[buf, rows] = vals
            part = fold(vals, jnp.maximum)
            top = part if top is None else jnp.maximum(top, part)
        top_s[buf] = jnp.broadcast_to(jnp.max(top, axis=0, keepdims=True), (SUB, COLS))
        inv_s[prev] = jnp.broadcast_to(1.0 / jnp.sum(total, axis=0, keepdims=True), (SUB, COLS))
        if defer:
            p_s[:] = jnp.concatenate(probs)
        else:
            weigh(1 - slot if h < 2 else slot, (h - 2) % HEADS, jnp.concatenate(probs))

    def finish(row, slot):
        gated = (g_s[slot] * o_s[slot]).astype(BF16)
        z_out[jnp.maximum(row, 0)] = z_in[jnp.clip(row, 0, n_rows - 1)] + mm(w_proj[:], gated)

    project(0, 0)
    keep_mask(0, 0)
    n_steps = (n_rows + 2 + STEPS - 1) // STEPS

    @pl.loop(0, n_steps)
    def _(it):
        first = STEPS * it - 1
        lg = scores(1, 0)
        weigh(0, 1, p_s[:])
        for k in range(STEPS):
            row, slot, last = first + k, 1 - k % 2, k == STEPS - 1
            for h in range(HEADS):
                nxt = scores(slot, h + 1) if h < HEADS - 1 else (None if last else scores(1 - slot, 0))
                if h == 2:
                    project(row + 2, slot)
                step(row, slot, h, lg, last and h == HEADS - 1)
                lg = nxt
                if h == 3:
                    finish(row - 1, 1 - slot)
                    v_s[1 - slot] = vn_s[1 - slot]
                    g_s[1 - slot] = gn_s[1 - slot]
            keep_mask(row + 2, slot)
        for j in range(n):
            @pl.when(it == max((ROWS * j - 1) // STEPS - 1, 0))
            def _():
                z_copy(j).wait()

            for stop, copy in o_copies(j):
                if stop < n_rows:
                    @pl.when(it == (stop + 1) // STEPS)
                    def _():
                        copy.start()

    for stop, copy in o_copies(n - 1):
        if stop == n_rows:
            copy.start()
    for j in range(n):
        for _, copy in o_copies(j):
            copy.wait()


def attend(static, sc, z_parts, biases, mask, norms, w_all, w_proj, out, mask_away=None):
    n, fresh, away = len(z_parts), out is None, mask_away is not None
    z_parts, biases = jax.tree.map(lambda v: pltpu.with_memory_space_constraint(v, pltpu.HBM), (list(z_parts), list(biases)))
    args = (sc, *z_parts, *biases, mask, norms, w_all, w_proj, *[mask_away] * away, *[out] * (not fresh))
    whole = SDS((mask.shape[0], ROWS, CH, COLS), F32)
    aways = [SDS((k, CH, COLS), F32) for k in (AWAY_FIRST, AWAY.shape[0] - AWAY_FIRST)] * away
    rows = sum(z.shape[0] for z in z_parts)
    pair, wide, square, line = [pltpu.VMEM((SLOTS, *shape), dtype) for shape, dtype in (
        ((CH, COLS), BF16), ((CH, COLS), F32), ((COLS, COLS), F32), ((SUB, COLS), F32))]
    each = [pltpu.VMEM((n, HEADS, COLS, COLS), dtype) for dtype in (BF16, F32)]
    sems, more = pltpu.SemaphoreType.DMA((n,)), pltpu.SemaphoreType.DMA((n + 1,))
    return pl.pallas_call(
        functools.partial(attention_kernel, static, fresh, away),
        out_shape=(whole, *aways),
        in_specs=[SM] + [HB] * (5 * n + 1) + [VM] * 3 + [HB] * (away + (not fresh)),
        out_specs=(HB,) * (1 + len(aways)),
        scratch_shapes=[
            pltpu.VMEM((rows, CH, COLS), F32), pltpu.VMEM((rows + STEPS, CH, COLS), F32), pltpu.VMEM((mask_rows(rows), COLS), jnp.int32),
            pltpu.VMEM((mask_rows(rows), COLS), F32), *each, pltpu.VMEM((SLOTS, HEADS, CH, COLS), BF16),
            pltpu.VMEM((SLOTS, COLS, CH), BF16), pair, wide, pair, wide, pltpu.VMEM((SLOTS, COLS, LANES), F32),
            square, square, pltpu.VMEM((COLS, COLS), BF16), line, line, wide, sems, more, sems, sems,
        ],
        compiler_params=pltpu.CompilerParams(vmem_limit_bytes=48 * MIB),
        input_output_aliases={} if fresh else {len(args) - 1: 0},
        name="triangle_attention",
    )(*args)


FIRST = 4


def exchange(values, r):
    return lax.ppermute(values, 'dap', [(i, i ^ r) for i in range(4)])


def update_weights(params):
    norm_gain, norm_bias, w_a, w_agate, w_b, w_bgate, w_gate, x_gain, x_bias, w_proj = params
    half = jnp.bfloat16(0.5)
    wide = lambda v: jnp.broadcast_to(v[:, None], (CH, COLS))
    deep = lambda v: jnp.broadcast_to(v[:, None, None], (CH, 8, 128))
    return ([wide(norm_gain), wide(norm_bias)], [deep(x_gain), deep(x_bias)],
            half * jnp.concatenate([w_a.T, w_agate.T, w_b.T, w_bgate.T]), [half * w_gate.T, half * w_proj.T])


def solution(mesh):
    def local_block(pair_z, pair_mask, *weights):
        me = lax.axis_index('dap')
        zt = jnp.transpose(pair_z, (0, 1, 3, 2))
        n_own = zt.shape[0] // 4
        mask_bf = pair_mask.astype(BF16)
        arrived, layouts, before = [], [], ()
        for t in range(n_own):
            pieces = [(2, 0, FIRST), (2, FIRST, ROWS)] if t == 0 else [(2, 0, ROWS)]
            pieces += [(3, 0, ROWS), (1, 0, ROWS)]
            got = []
            for r, start, stop in pieces:
                where = (n_own * (me ^ r) + t, start, 0, 0)
                send = lax.dynamic_slice(lax.optimization_barrier((zt, *before))[0], where, (1, stop - start, CH, COLS))[0]
                if t == 0 or r == 1:
                    before = (send,)
                got.append(exchange(send, r))
                if t == 0 and stop == ROWS and r == 2:
                    mask_bf, weights = lax.optimization_barrier((mask_bf, weights, send))[:2]
                    masks = [lax.dynamic_slice_in_dim(mask_bf, n_own * (me ^ k), n_own) for k in range(4)]
                    before = (*before, *masks)
                    masks = [exchange(m, k) if k else m for k, m in enumerate(masks)]
            arrived.append([zt, *got])
            layouts.append(((0, 0), *((r, start) for r, start, _ in pieces)))

        out_n, out_x, out_ab, out_sq = update_weights(weights[:10])
        in_n, in_x, in_ab, in_sq = update_weights(weights[10:20])
        att_gain, att_shift, w_q, w_k, w_v, w_bias, w_gate, w_proj = weights[20:]
        att_n = [jnp.broadcast_to(v[:, None], (CH, COLS)) for v in (att_gain, att_shift)]
        norms = jnp.stack(out_n + in_n + att_n)
        xgs = jnp.stack(out_x + in_x)
        w_ab = jnp.stack([out_ab, in_ab])
        w_sq = jnp.stack(out_sq + in_sq)
        w_bias8 = jnp.concatenate([w_bias.T, jnp.zeros((4, CH), BF16)])
        w_all = jnp.concatenate([w_q.T * jnp.bfloat16(HEAD ** -0.5), w_k.T, w_v.T, w_gate.T])
        w_out = w_proj.T
        att_norms = norms[4:]

        token = [None]

        def ordered(call, sc, *args):
            sc = jnp.stack([jnp.asarray(v, jnp.int32) for v in sc])
            if token[0] is not None:
                sc = lax.optimization_barrier((sc, token[0]))[0]
            res = call(sc, *args)
            token[0] = jax.tree.leaves(res)[-1]
            return res

        def attention(jobs, out, mask_away=None):
            samples, orders, z_parts, biases, starts = zip(*jobs)
            static = tuple((start, z.shape[0], tuple(place for _, place in blocks))
                           for start, z, blocks in zip(starts, z_parts, biases))
            arrays = [array for blocks in biases for array, _ in blocks]
            return ordered(functools.partial(attend, static), samples + orders, z_parts, arrays, pair_mask, att_norms,
                           w_all, w_out, out, mask_away)

        far = [(t, r) for t in range(n_own) for r in (2, 3)]
        a_far, b_far = ordered(l1_call, [n_own * (me ^ r) + t for t, r in far], zt, pair_mask, norms, w_ab)
        b_par = exchange(b_far, 1)
        x_near = ordered(l2_call, [me], a_far, b_far, b_par, xgs)

        out = None
        held = []
        for t in range(n_own):
            last = t == n_own - 1
            z_own, z_par, bias, far2, *far3 = ordered(functools.partial(u_call, last, layouts[t]), [me, n_own * me + t],
                                                      arrived[t], [m[t] for m in masks], norms, xgs, w_ab, w_sq, w_bias8)
            here = lambda array: [(array, r) for r in range(4)]
            near = (n_own * (me ^ 1) + t, 0, exchange(z_par, 1), here(exchange(bias, 1)), 0)
            own = (n_own * me + t, 0, z_own, here(bias), 0)
            two = exchange(far2, 2)
            three = [exchange(v, 3) for v in far3[:2]]
            held.append((two, three))
            if last:
                out, *away = attention([own, (0, 0, far3[-1], here(bias), 0)], out,
                                       jnp.roll(masks[3][t], -SOME, axis=0)[None, :mask_rows(ROWS - SOME)].astype(jnp.int32))
                away = [exchange(v, 3) for v in away]
            else:
                out, = attention([own, near], out)

        def rows_of(t, r, blocks, x_far, xi):
            return ordered(functools.partial(r_call, blocks), [me, n_own * (me ^ r) + t, far.index((t, r))],
                           zt, x_near, x_far, xi, norms, w_sq, w_bias8)

        for t in range(n_own - 1):
            two, (three,) = held[t]
            z_two, mine_two = rows_of(t, 2, 1, two, two)
            z_three, mine_three = rows_of(t, 3, 1, three, three)
            par_two, par_three = exchange(mine_two, 1), exchange(mine_three, 1)
            jobs = [(n_own * (me ^ r) + t, me, z, [(mine, 0), (par, 0), (mine, 1), (par, 1)], 0)
                    for r, z, mine, par in ((2, z_two, mine_two, par_three), (3, z_three, mine_three, par_two))]
            out, = attention(([] if t else [near]) + jobs, out)
        two, three = held[t + 1]
        z_two, mine = rows_of(t + 1, 2, 3, two, two)
        par = exchange(mine, 1)
        out, = attention([(n_own * (me ^ 2) + t + 1, me, z_two, [(mine, k) for k in (0, 3, 1, 2)], 0)], out)
        z_three, = rows_of(t + 1, 3, 0, three[1], three[0])
        out, = attention([(n_own * (me ^ 3) + t + 1, me, z_three, [(par, k) for k in (3, 0, 2, 1)], 0)], out)
        for v, start in zip(away, (SOME, SOME + AWAY_FIRST)):
            out = lax.dynamic_update_slice(out, v[None], (n_own * (me ^ 3) + n_own - 1, start, 0, 0))
        return jnp.transpose(out, (0, 1, 3, 2))

    pair_spec = P('data', 'dap')
    return jax.shard_map(local_block, mesh=mesh, in_specs=(pair_spec, pair_spec) + (P(),) * 28,
                         out_specs=pair_spec, check_vma=False)
```
